8 devices in a mesh: dp: 1 (over z), row: 2 (over y), col: 4 (over x, core).
Axes of the slice: x: 2, y: 2, z: 1, core: 2. Of those that a mesh axis runs over, the one named last changes fastest.
Arguments:
- x: bfloat16 [2048, 896], P(('dp', 'row', 'col'))
- route_idx: int32 [2048, 8], P(('dp', 'row', 'col'))
- gates: float32 [2048, 8], P(('dp', 'row', 'col'))
- w1: bfloat16 [384, 896, 256], P(('row', 'col'))
- w3: bfloat16 [384, 896, 256], P(('row', 'col'))
- w2: bfloat16 [384, 256, 896], P(('row', 'col'))
- dy: bfloat16 [2048, 896], P(('dp', 'row', 'col'))
Outputs:
- output 1: bfloat16 [2048, 896], P(('dp', 'row', 'col'))
- output 2: bfloat16 [2048, 896], P(('dp', 'row', 'col'))
- output 3: float32 [2048, 8], P(('dp', 'row', 'col'))
- output 4: float32 [384, 896, 256], P(('dp', 'row', 'col'))
- output 5: float32 [384, 896, 256], P(('dp', 'row', 'col'))
- output 6: float32 [384, 256, 896], P(('dp', 'row', 'col'))
All inputs are finite; a program needn't handle non-finite values.
Results may differ from the reference program's by a relative error of at most 0.00783231.
Values are sent between devices in bfloat16 or wider.
A program may use at most 1 GiB of HBM per device.

```python
import jax
import jax.numpy as jnp
from jax import lax

TOK = 256
NDEV = 8
D = 896
FF = 256
EXPERTS = 384
TOP = 8

TG = NDEV * TOK
CAP = (4 * TOK * TOP + EXPERTS - 1) // EXPERTS
CG = NDEV * CAP
NH = max(1, min(TOP // 2, (8 * TOP) // NDEV))
HOT = 2 * EXPERTS // NDEV
NCOLD = EXPERTS - HOT


def setup_inputs(seed: int = 0, part: int = 0) -> dict:
    kw = jax.random.split(jax.random.key(seed), 3)
    kp = jax.random.split(jax.random.fold_in(jax.random.key(seed + 1), part), 8)
    w1 = (jax.random.normal(kw[0], (EXPERTS, D, FF), jnp.float32) * D ** -0.5).astype(jnp.bfloat16)
    w3 = (jax.random.normal(kw[1], (EXPERTS, D, FF), jnp.float32) * D ** -0.5).astype(jnp.bfloat16)
    w2 = (jax.random.normal(kw[2], (EXPERTS, FF, D), jnp.float32) * FF ** -0.5).astype(jnp.bfloat16)
    dmax = min(NH, HOT - NH, TOP - NH)
    sh = jax.random.randint(kp[2], (), 0, HOT)
    sc = jax.random.randint(kp[3], (), 0, NCOLD)
    dd = jax.random.randint(kp[0], (NDEV, TOK // 2), 0, dmax + 1)
    nh = jnp.stack([NH + dd, NH - dd], axis=-1).reshape(NDEV, TOK)
    nc = TOP - nh
    sth = jnp.cumsum(nh, axis=1) - nh
    stc = jnp.cumsum(nc, axis=1) - nc
    dev = jnp.arange(NDEV)[:, None, None]
    j = jnp.arange(TOP)[None, None, :]
    hot_ids = (sh + dev * (TOK * NH) + sth[:, :, None] + j) % HOT
    cold_ids = HOT + (sc + dev * (TOK * (TOP - NH)) + stc[:, :, None] + j - nh[:, :, None]) % NCOLD
    ids = jnp.where(j < nh[:, :, None], hot_ids, cold_ids).reshape(TG, TOP)
    ids = jax.random.permutation(kp[4], ids, axis=1, independent=True).astype(jnp.int32)
    gu = jax.random.uniform(kp[5], (TG, TOP), jnp.float32, 0.5, 1.5)
    gates = gu / jnp.sum(gu, axis=1, keepdims=True)
    x = jax.random.normal(kp[6], (TG, D), jnp.float32).astype(jnp.bfloat16)
    dy = jax.random.normal(kp[7], (TG, D), jnp.float32).astype(jnp.bfloat16)
    return {'x': x, 'route_idx': ids, 'gates': gates, 'w1': w1, 'w3': w3, 'w2': w2, 'dy': dy}


def reference(x, route_idx, gates, w1, w3, w2, dy):
    n = TG * TOP
    ef = route_idx.reshape(n)
    order = jnp.argsort(ef, stable=True).astype(jnp.int32)
    es = ef[order]
    first = jnp.searchsorted(es, es, side='left').astype(jnp.int32)
    rank = jnp.arange(n, dtype=jnp.int32) - first
    tab = jnp.full((EXPERTS, CG), n, jnp.int32).at[es, rank].set(order)
    gf = gates.reshape(n)

    def body(carry, inp):
        y_acc, dx_acc, dg = carry
        te, a1, a3, a2 = inp
        valid = te < n
        ai = jnp.minimum(te, n - 1)
        tk = ai // TOP
        xr = x[tk]
        xs = jnp.where(valid[:, None], xr, jnp.zeros_like(xr))
        u = jnp.dot(xs, a1, preferred_element_type=jnp.float32).astype(jnp.bfloat16).astype(jnp.float32)
        v = jnp.dot(xs, a3, preferred_element_type=jnp.float32).astype(jnp.bfloat16).astype(jnp.float32)
        sg = jax.nn.sigmoid(u)
        a = (u * sg * v).astype(jnp.bfloat16)
        o = jnp.dot(a, a2, preferred_element_type=jnp.float32).astype(jnp.bfloat16).astype(jnp.float32)
        g = jnp.where(valid, gf[ai], 0.0)
        y_acc = y_acc.at[tk].add(g[:, None] * o)
        dys = dy[tk].astype(jnp.float32)
        dg = dg.at[ai].add(jnp.where(valid, jnp.sum(dys * o, axis=1), 0.0))
        do = (g[:, None] * dys).astype(jnp.bfloat16)
        gw2 = jnp.dot(a.T, do, preferred_element_type=jnp.float32)
        da = jnp.dot(do, a2.T, preferred_element_type=jnp.float32)
        du = (da * v * sg * (1.0 + u * (1.0 - sg))).astype(jnp.bfloat16)
        dv = (da * u * sg).astype(jnp.bfloat16)
        gw1 = jnp.dot(xs.T, du, preferred_element_type=jnp.float32)
        gw3 = jnp.dot(xs.T, dv, preferred_element_type=jnp.float32)
        dxs = jnp.dot(du, a1.T, preferred_element_type=jnp.float32) + jnp.dot(dv, a3.T, preferred_element_type=jnp.float32)
        dx_acc = dx_acc.at[tk].add(dxs.astype(jnp.bfloat16).astype(jnp.float32))
        return (y_acc, dx_acc, dg), (gw1, gw3, gw2)

    init = (jnp.zeros((TG, D), jnp.float32), jnp.zeros((TG, D), jnp.float32), jnp.zeros((n,), jnp.float32))
    (y_acc, dx_acc, dg), (gw1, gw3, gw2) = lax.scan(body, init, (tab, w1, w3, w2))
    return (y_acc.astype(jnp.bfloat16), dx_acc.astype(jnp.bfloat16), dg.reshape(TG, TOP), gw1, gw3, gw2)
```

```python
import functools

import jax
import jax.numpy as jnp
from jax import lax
from jax.experimental import pallas as pl
from jax.experimental.pallas import tpu as pltpu
from jax.sharding import PartitionSpec as P

F32 = jnp.float32
BF16 = jnp.bfloat16
NP = 8
TOK = 256
CAP = 24
PAD = 32
GRP = 8
NROW = NP * CAP


def nt(a, b):
    return lax.dot_general(a, b, (((1,), (1,)), ((), ())), preferred_element_type=F32)


def nn(a, b):
    return lax.dot_general(a, b, (((1,), (0,)), ((), ())), preferred_element_type=F32)


def tn(a, b):
    return lax.dot_general(a, b, (((0,), (0,)), ((), ())), preferred_element_type=F32)


def onehot(rows, cap):
    n = rows.shape[0]
    it = lax.broadcasted_iota(jnp.int32, (cap, TOK), 0).astype(F32)
    return [jnp.broadcast_to(rows[k:k + 1], (cap, TOK)) == it for k in range(n)]


def kernel(ne, el, x_hbm, dy_hbm, rt_ref, gt_ref, w1_ref, w3_ref, w2_ref,
           y_hbm, dx_hbm, dg_ref, gw1_ref, gw3_ref, gw2_ref,
           xs, dys, xe_s, dye_s, o_s, d_s, yacc, dxacc, cm, gm, dgm, sem):
    s = pl.program_id(0)
    ng = el // GRP
    steps = pl.num_programs(0)
    e0 = (lax.axis_index('row') * 4 + lax.axis_index('col')) * el

    @pl.when(s == 0)
    def _():
        cx = pltpu.make_async_copy(x_hbm, xs, sem.at[0])
        cd = pltpu.make_async_copy(dy_hbm, dys, sem.at[1])
        cx.start()
        cd.start()
        o_s[...] = jnp.zeros_like(o_s)
        d_s[...] = jnp.zeros_like(d_s)
        yacc[...] = jnp.zeros_like(yacc)
        dxacc[...] = jnp.zeros_like(dxacc)
        tr = lax.broadcasted_iota(jnp.int32, (TOK, TOK), 0)
        tc = lax.broadcasted_iota(jnp.int32, (TOK, TOK), 1)
        tri = jnp.where(tr < tc, 1.0, 0.0).astype(BF16)
        ee = lax.broadcasted_iota(jnp.int32, (el, TOK), 0) + e0

        def prep(p, _):
            r = rt_ref[p]
            g = gt_ref[p]
            m = jnp.zeros((el, TOK), F32)
            gs = jnp.zeros((el, TOK), F32)
            for j in range(r.shape[0]):
                hit = jnp.broadcast_to(r[j:j + 1], (el, TOK)) == ee
                m = jnp.where(hit, 1.0, m)
                gs = jnp.where(hit, jnp.broadcast_to(g[j:j + 1], (el, TOK)), gs)
            rank = nn(m.astype(BF16), tri)
            cm[p] = jnp.where(m > 0.0, rank, -1.0)
            gm[p] = gs
            return 0

        lax.fori_loop(0, NP, prep, 0)
        cx.wait()
        cd.wait()

    def gather(g, i):
        base = pl.multiple_of(g * GRP, GRP)
        slot = lax.rem(g, 2)
        q = lax.rem(i, 4)

        def pair(src, dst):
            res = []
            for h in range(2):
                p = q * 2 + h
                oh = onehot(cm[p, pl.ds(base, GRP), :], CAP)
                oh = jnp.concatenate([jnp.where(m, 1.0, 0.0) for m in oh], axis=0).astype(BF16)
                res.append(nn(oh, src[p]))
            for k in range(GRP):
                blk = jnp.concatenate([r[k * CAP:(k + 1) * CAP] for r in res], axis=0)
                dst[slot, k, pl.ds(pl.multiple_of(q * 2 * CAP, 2 * CAP), 2 * CAP), :] = blk.astype(BF16)

        @pl.when(i < 4)
        def _():
            pair(xs, xe_s)

        @pl.when(i >= 4)
        def _():
            pair(dys, dye_s)

    def scatter(g, p):
        base = pl.multiple_of(g * GRP, GRP)
        slot = lax.rem(g, 2)
        oh = onehot(cm[p, pl.ds(base, GRP), :], PAD)
        gr = gm[p, pl.ds(base, GRP), :]
        g1 = gr.astype(BF16).astype(F32)
        r1 = gr - g1
        g2 = r1.astype(BF16).astype(F32)
        g3 = r1 - g2
        sl = pl.ds(pl.multiple_of(p * PAD, PAD), PAD)
        ob = jnp.concatenate([o_s[slot, k, sl, :] for k in range(GRP)], axis=0)
        db = jnp.concatenate([d_s[slot, k, sl, :] for k in range(GRP)], axis=0)

        def spread(part):
            return jnp.concatenate(
                [jnp.where(oh[k], jnp.broadcast_to(part[k:k + 1], (PAD, TOK)), 0.0) for k in range(GRP)],
                axis=0).astype(BF16)

        gs = jnp.concatenate([spread(g1), spread(g2), spread(g3)], axis=0)
        yacc[p] += tn(gs, jnp.concatenate([ob, ob, ob], axis=0))
        one = jnp.concatenate([jnp.where(m, 1.0, 0.0) for m in oh], axis=0).astype(BF16)
        dxacc[p] += tn(one, db)

    def core(g, i):
        slot = lax.rem(g, 2)
        e = g * GRP + i
        xe = xe_s[slot, i]
        dye = dye_s[slot, i]
        w13 = jnp.concatenate([w1_ref[0], w3_ref[0]], axis=1)
        w2 = w2_ref[0]
        ff = w2.shape[0]
        uv = nn(xe, w13).astype(BF16).astype(F32)
        u, v = uv[:, :ff], uv[:, ff:]
        sg = jax.nn.sigmoid(u)
        us = u * sg
        a = (us * v).astype(BF16)
        o = nn(a, w2).astype(BF16)
        of = o.astype(F32)
        dyf = dye.astype(F32)
        dgc = jnp.sum(dyf * of, axis=1, keepdims=True)
        it = lax.broadcasted_iota(jnp.int32, (CAP, TOK), 0).astype(F32)
        gcol = []
        for p in range(NP):
            m = jnp.broadcast_to(cm[p, pl.ds(e, 1), :], (CAP, TOK)) == it
            gb = jnp.broadcast_to(gm[p, pl.ds(e, 1), :], (CAP, TOK))
            gcol.append(jnp.sum(jnp.where(m, gb, 0.0), axis=1, keepdims=True))
            db = jnp.broadcast_to(dgc[p * CAP:(p + 1) * CAP], (CAP, TOK))
            dgm[p, pl.ds(e, 1), :] = jnp.sum(jnp.where(m, db, 0.0), axis=0, keepdims=True)
        do = (jnp.concatenate(gcol, axis=0) * dyf).astype(BF16)
        da = nt(do, w2)
        du = (da * v * sg * (1.0 + u * (1.0 - sg))).astype(BF16)
        dv = (da * u * sg).astype(BF16)
        duv = jnp.concatenate([du, dv], axis=1)
        dx = nt(duv, w13)
        gw2_ref[0] = tn(a, do)
        g13 = tn(xe, duv)
        gw1_ref[0] = g13[:, :ff]
        gw3_ref[0] = g13[:, ff:]
        zero = jnp.zeros((PAD - CAP, o.shape[1]), F32)
        for p in range(NP):
            rows = slice(p * CAP, (p + 1) * CAP)
            o_s[slot, i, p * PAD:(p + 1) * PAD, :] = jnp.concatenate([of[rows], zero], axis=0).astype(BF16)
            d_s[slot, i, p * PAD:(p + 1) * PAD, :] = jnp.concatenate([dx[rows], zero], axis=0).astype(BF16)

    t = s - GRP
    g = lax.div(t, GRP)
    i = lax.rem(s, GRP)

    @pl.when(s < ng * GRP)
    def _():
        gather(lax.div(s, GRP), i)

    @pl.when(jnp.logical_and(s >= GRP, s < GRP + el))
    def _():
        core(g, i)

    @pl.when(s >= 2 * GRP)
    def _():
        scatter(lax.div(s, GRP) - 2, i)

    @pl.when(s == steps - 1)
    def _():
        cy = pltpu.make_async_copy(yacc, y_hbm, sem.at[0])
        cd = pltpu.make_async_copy(dxacc, dx_hbm, sem.at[1])
        cy.start()
        cd.start()

        def fin(p, _):
            r = rt_ref[p]
            acc = jnp.zeros(r.shape, F32)
            for e in range(el):
                acc = acc + jnp.where(r == e + e0, jnp.broadcast_to(dgm[p, e:e + 1, :], r.shape), 0.0)
            dg_ref[p] = acc
            return 0

        lax.fori_loop(0, NP, fin, 0)
        cy.wait()
        cd.wait()


def solution(mesh):
    grp = ('row', 'col')
    tspec = P(('dp', 'row', 'col'), None)
    wspec = P(grp, None, None)
    gspec = P(('dp', 'row', 'col'), None, None)

    def local(x, ridx, gates, w1, w3, w2, dy):
        tok, d = x.shape
        top = ridx.shape[1]
        el, _, ff = w1.shape
        ne = el * NP
        xa = lax.all_gather(x, grp)
        dya = lax.all_gather(dy, grp)
        rt = lax.all_gather(ridx.T, grp)
        gt = lax.all_gather(gates.T, grp)
        steps = el + 2 * GRP

        def eidx(s):
            return (jnp.clip(s - GRP, 0, el - 1), 0, 0)

        wide = pl.BlockSpec((1, d, ff), eidx)
        tall = pl.BlockSpec((1, ff, d), eidx)
        anyspec = pl.BlockSpec(memory_space=pl.ANY)
        vm = pl.BlockSpec(memory_space=pltpu.VMEM)
        yp, dxp, dgp, gw1, gw3, gw2 = pl.pallas_call(
            functools.partial(kernel, ne, el),
            grid=(steps,),
            in_specs=[anyspec, anyspec, vm, vm, wide, wide, tall],
            out_specs=[anyspec, anyspec, vm, wide, wide, tall],
            out_shape=[
                jax.ShapeDtypeStruct((NP, tok, d), F32),
                jax.ShapeDtypeStruct((NP, tok, d), F32),
                jax.ShapeDtypeStruct((NP, top, tok), F32),
                jax.ShapeDtypeStruct((el, d, ff), F32),
                jax.ShapeDtypeStruct((el, d, ff), F32),
                jax.ShapeDtypeStruct((el, ff, d), F32),
            ],
            scratch_shapes=[
                pltpu.VMEM((NP, tok, d), BF16),
                pltpu.VMEM((NP, tok, d), BF16),
                pltpu.VMEM((2, GRP, NROW, d), BF16),
                pltpu.VMEM((2, GRP, NROW, d), BF16),
                pltpu.VMEM((2, GRP, NP * PAD, d), BF16),
                pltpu.VMEM((2, GRP, NP * PAD, d), BF16),
                pltpu.VMEM((NP, tok, d), F32),
                pltpu.VMEM((NP, tok, d), F32),
                pltpu.VMEM((NP, el, tok), F32),
                pltpu.VMEM((NP, el, tok), F32),
                pltpu.VMEM((NP, el, tok), F32),
                pltpu.SemaphoreType.DMA((2,)),
            ],
            compiler_params=pltpu.CompilerParams(
                dimension_semantics=('arbitrary',), vmem_limit_bytes=67_000_000),
            cost_estimate=pl.CostEstimate(flops=60_000_000_000, bytes_accessed=200_000_000, transcendentals=0),
        )(xa, dya, rt, gt, w1, w3, w2)
        y = lax.psum_scatter(yp, grp, scatter_dimension=0, tiled=False).astype(BF16)
        dx = lax.psum_scatter(dxp, grp, scatter_dimension=0, tiled=False).astype(BF16)
        dg = lax.psum_scatter(dgp, grp, scatter_dimension=0, tiled=False).T
        return y, dx, dg, gw1, gw3, gw2

    return jax.shard_map(local, mesh=mesh, in_specs=(tspec, tspec, tspec, wspec, wspec, wspec, tspec), out_specs=(tspec, tspec, tspec, gspec, gspec, gspec), check_vma=False)
```

```python
import functools

import jax
import jax.numpy as jnp
from jax import lax
from jax.experimental import pallas as pl
from jax.experimental.pallas import tpu as pltpu
from jax.sharding import PartitionSpec as P

F32 = jnp.float32
BF16 = jnp.bfloat16
MESH = pl.DeviceIdType.MESH
NP = 8
TOK = 256
HALF = TOK // 2
CAP = 24
PAD = 32
GRP = 8
NROW = NP * CAP
NBUF = 4


def nt(a, b):
    return lax.dot_general(a, b, (((1,), (1,)), ((), ())), preferred_element_type=F32)


def nn(a, b):
    return lax.dot_general(a, b, (((1,), (0,)), ((), ())), preferred_element_type=F32)


def tn(a, b):
    return lax.dot_general(a, b, (((0,), (0,)), ((), ())), preferred_element_type=F32)


def onehot(rows, cap):
    n = rows.shape[0]
    it = lax.broadcasted_iota(jnp.int32, (cap, TOK), 0).astype(F32)
    return [jnp.broadcast_to(rows[k:k + 1], (cap, TOK)) == it for k in range(n)]


def ds(i, n):
    return pl.ds(pl.multiple_of(i * n, n), n)


def gather_pair(cm, g, q, src, store):
    res = []
    for h in range(2):
        p = q * 2 + h
        oh = onehot(cm[p, ds(g, GRP), :], CAP)
        oh = jnp.concatenate([jnp.where(m, 1.0, 0.0) for m in oh], axis=0).astype(BF16)
        res.append(nn(oh, src[p]))
    for k in range(GRP):
        blk = jnp.concatenate([r[k * CAP:(k + 1) * CAP] for r in res], axis=0)
        store(k, ds(q, 2 * CAP), blk.astype(BF16))


def gate_column(cm, gm, e):
    it = lax.broadcasted_iota(jnp.int32, (CAP, TOK), 0).astype(F32)
    cols = []
    for p in range(NP):
        m = jnp.broadcast_to(cm[p, pl.ds(e, 1), :], (CAP, TOK)) == it
        gb = jnp.broadcast_to(gm[p, pl.ds(e, 1), :], (CAP, TOK))
        cols.append(jnp.sum(jnp.where(m, gb, 0.0), axis=1, keepdims=True))
    return jnp.concatenate(cols, axis=0)


def main_kernel(el, x_hbm, dy_hbm, rg_ref, w1_hbm, w3_hbm, w2_hbm,
                y_ref, dx_ref, dg_ref, xa_hbm, dya_hbm, cm_hbm, gm_hbm, duv_hbm, a_hbm,
                xs, dys, rgs, xe_s, o_s, uv_s, a_s, yacc, dxacc, cm, gm, dgm, dgo, dgr,
                w1b, w3b, w2b, rd, r1, r2,
                wsem, lsem, osem, rg_ss, rg_rs, ag_ss, ag_rs, dd_ss, dd_rs, s1_ss, s1_rs, s2_ss, s2_rs, dg_ss, dg_rs):
    ng = el // GRP
    ff = w2b.shape[1]
    Z = lax.axis_index('dp')
    Y = lax.axis_index('row')
    col = lax.axis_index('col')
    X = lax.div(col, 2)
    C = lax.rem(col, 2)
    me = Y * 4 + col
    e0 = me * el

    def pos(fy, fx, fc):
        return (1 - Y if fy else Y), (1 - X if fx else X), (1 - C if fc else C)

    def blk(fy, fx, fc):
        yy, xx, cc = pos(fy, fx, fc)
        return yy * 4 + xx * 2 + cc

    def dev(fy, fx, fc):
        yy, xx, cc = pos(fy, fx, fc)
        return (Z, yy, xx * 2 + cc)

    peers = [(a, b, c) for a in range(2) for b in range(2) for c in range(2)][1:]

    def remote(src, dst, ss, rs, to):
        return pltpu.make_async_remote_copy(src_ref=src, dst_ref=dst, send_sem=ss, recv_sem=rs,
                                            device_id=dev(*to), device_id_type=MESH)

    lx = pltpu.make_async_copy(x_hbm, xs.at[me], lsem.at[0])
    ld = pltpu.make_async_copy(dy_hbm, dys.at[me], lsem.at[1])
    lx.start()
    ld.start()

    def wcopies(e):
        b = lax.rem(e, NBUF)
        k = lax.rem(e, el)
        return [pltpu.make_async_copy(h.at[k], v.at[b], wsem.at[n, b])
                for n, (h, v) in enumerate(((w1_hbm, w1b), (w3_hbm, w3b), (w2_hbm, w2b)))]

    for e in range(NBUF - 1):
        for c in wcopies(e):
            c.start()

    barrier = pltpu.get_barrier_semaphore()
    for to in peers:
        pl.semaphore_signal(barrier, inc=1, device_id=dev(*to), device_id_type=MESH)
    pl.semaphore_wait(barrier, len(peers))

    rgs[me] = rg_ref[...]
    rg_copies = [remote(rg_ref, rgs.at[me], rg_ss.at[n], rg_rs.at[n], to) for n, to in enumerate(peers)]
    for c in rg_copies:
        c.start()

    def half(buf, b, h):
        return buf.at[b, pl.ds(h * HALF, HALF), :]

    XN, YN, DN, PN = (0, 1, 0), (1, 0, 0), (1, 1, 0), (0, 0, 1)
    FIRST = [(0, (0, 0, 0), 0, XN), (1, (0, 0, 0), 1, YN), (2, (0, 0, 0), 1, XN), (3, (0, 0, 0), 0, YN)]
    OWN2 = [(6, (0, 0, 0), 0, PN), (7, (0, 0, 0), 1, PN)]
    FWD = [(4, XN, 0, YN), (5, YN, 1, XN)]
    ARR = {0: (XN, 0), 1: (YN, 1), 2: (XN, 1), 3: (YN, 0), 4: (DN, 0), 5: (DN, 1)}
    ONWARD = {0: 8, 1: 9, 2: 10, 3: 11, 4: 12, 5: 13}

    def ag_copy(t, buf, n, f, h, to):
        r = half(buf, blk(*f), h)
        return remote(r, r, ag_ss.at[t, n], ag_rs.at[t, n], to)

    def ag_recv(t, buf, n, f, h):
        r = half(buf, blk(*f), h)
        remote(r, r, ag_ss.at[t, n], ag_rs.at[t, n], PN).wait_recv()

    def ag_start(t, buf):
        for n, f, h, to in FIRST + OWN2:
            ag_copy(t, buf, n, f, h, to).start()

    def ag_relay(t, buf, ns):
        for n in ns:
            f, h = ARR[n]
            ag_recv(t, buf, n, f, h)
            if n < 2:
                k, ff_, hh, to = FWD[n]
                ag_copy(t, buf, k, ff_, hh, to).start()
            ag_copy(t, buf, ONWARD[n], f, h, PN).start()

    def ag_finish(t, buf):
        for n, h in ((6, 0), (7, 1)):
            ag_recv(t, buf, n, PN, h)
        for n, k in ONWARD.items():
            f, h = ARR[n]
            ag_recv(t, buf, k, (f[0], f[1], 1), h)

    def ag_drain(t, buf):
        for n, f, h, to in FIRST + OWN2 + FWD:
            ag_copy(t, buf, n, f, h, to).wait_send()
        for n, k in ONWARD.items():
            f, h = ARR[n]
            ag_copy(t, buf, k, f, h, PN).wait_send()

    lx.wait()
    ld.wait()
    ag_start(0, xs)

    def zero(p, _):
        yacc[p] = jnp.zeros(yacc.shape[1:], F32)
        dxacc[p] = jnp.zeros(dxacc.shape[1:], F32)
        return 0

    lax.fori_loop(0, NP, zero, 0)

    for n, to in enumerate(peers):
        remote(rgs.at[blk(*to)], rgs.at[blk(*to)], rg_ss.at[n], rg_rs.at[n], to).wait_recv()
    top = rgs.shape[1] // 2
    tr = lax.broadcasted_iota(jnp.int32, (TOK, TOK), 0)
    tc = lax.broadcasted_iota(jnp.int32, (TOK, TOK), 1)
    tri = jnp.where(tr < tc, 1.0, 0.0).astype(BF16)
    ee = (lax.broadcasted_iota(jnp.int32, (el, TOK), 0) + e0).astype(F32)

    def prep(p, _):
        rg = rgs[p]
        m = jnp.zeros((el, TOK), F32)
        gs = jnp.zeros((el, TOK), F32)
        for j in range(top):
            hit = jnp.broadcast_to(rg[j:j + 1], (el, TOK)) == ee
            m = jnp.where(hit, 1.0, m)
            gs = jnp.where(hit, jnp.broadcast_to(rg[top + j:top + j + 1], (el, TOK)), gs)
        rank = nn(m.astype(BF16), tri)
        cm[p] = jnp.where(m > 0.0, rank, -1.0)
        gm[p] = gs
        return 0

    lax.fori_loop(0, NP, prep, 0)

    ag_relay(0, xs, (0, 1, 2, 3))
    ag_start(1, dys)
    ag_relay(0, xs, (4, 5))
    ag_finish(0, xs)
    out_copies = [pltpu.make_async_copy(xs, xa_hbm, osem.at[0]),
                  pltpu.make_async_copy(cm, cm_hbm, osem.at[1]),
                  pltpu.make_async_copy(gm, gm_hbm, osem.at[2]),
                  pltpu.make_async_copy(dys, dya_hbm, osem.at[3])]
    for c in out_copies[:3]:
        c.start()

    def gather_all(g, src):
        def step(q, _):
            def store(k, rows, val):
                xe_s[k, rows, :] = val
            gather_pair(cm, g, q, src, store)
            return 0
        lax.fori_loop(0, NP // 2, step, 0)

    def put_rows(i, val):
        zero = jnp.zeros((PAD - CAP, val.shape[1]), F32)
        for p in range(NP):
            o_s[i, p * PAD:(p + 1) * PAD, :] = jnp.concatenate([val[p * CAP:(p + 1) * CAP], zero], axis=0).astype(BF16)

    def take_rows(p):
        return jnp.concatenate([o_s[k, ds(p, PAD), :] for k in range(GRP)], axis=0)

    def combine_y(g):
        def step(p, _):
            oh = onehot(cm[p, ds(g, GRP), :], PAD)
            gr = gm[p, ds(g, GRP), :]
            g1 = gr.astype(BF16).astype(F32)
            rest = gr - g1
            g2 = rest.astype(BF16).astype(F32)
            g3 = rest - g2
            ob = take_rows(p)

            def spread(part):
                return jnp.concatenate(
                    [jnp.where(oh[k], jnp.broadcast_to(part[k:k + 1], (PAD, TOK)), 0.0) for k in range(GRP)],
                    axis=0).astype(BF16)

            gs = jnp.concatenate([spread(g1), spread(g2), spread(g3)], axis=0)
            yacc[p] += tn(gs, jnp.concatenate([ob, ob, ob], axis=0))
            return 0
        lax.fori_loop(0, NP, step, 0)

    def combine_dx(g):
        def step(p, _):
            oh = onehot(cm[p, ds(g, GRP), :], PAD)
            one = jnp.concatenate([jnp.where(m, 1.0, 0.0) for m in oh], axis=0).astype(BF16)
            dxacc[p] += tn(one, take_rows(p))
            return 0
        lax.fori_loop(0, NP, step, 0)

    def weights(n):
        for c in wcopies(n):
            c.wait()

        @pl.when(n + NBUF - 1 < 2 * el)
        def _():
            for c in wcopies(n + NBUF - 1):
                c.start()
        b = lax.rem(n, NBUF)
        return jnp.concatenate([w1b[b], w3b[b]], axis=1), w2b[b]

    def act(uv):
        u, v = uv[:, :ff], uv[:, ff:]
        sg = jax.nn.sigmoid(u)
        return u, v, sg, (u * sg * v).astype(BF16)

    ORDER = [(1, 1), (0, 1), (1, 0), (0, 0)]
    S1 = [((1, 1), 0, XN), ((1, 1), 1, YN), ((0, 1), 0, XN), ((1, 0), 1, YN)]
    IN1 = [((1, 0), 0), ((0, 1), 1), ((0, 0), 0), ((0, 0), 1)]
    S2 = [YN, XN]

    def dd_copy(t, acc, n):
        fy, fx = ORDER[n]
        return remote(acc.at[blk(fy, fx, 1)], rd.at[t, n], dd_ss.at[t, n], dd_rs.at[t, n], PN)

    def s1_copy(t, acc, n):
        (fy, fx), h, to = S1[n]
        return remote(half(acc, blk(fy, fx, 0), h), r1.at[t, n], s1_ss.at[t, n], s1_rs.at[t, n], to)

    def s2_copy(t, acc, n):
        (fy, fx), h = IN1[n]
        return remote(half(acc, blk(fy, fx, 0), h), r2.at[t, n], s2_ss.at[t, n], s2_rs.at[t, n], S2[n])

    def rs_start(t, acc):
        for n in range(4):
            dd_copy(t, acc, n).start()

    def rs_mid1(t, acc):
        for n in range(4):
            dd_copy(t, acc, n).wait_recv()
            fy, fx = ORDER[n]
            acc[blk(fy, fx, 0)] += rd[t, n]
            for k in ((0, 1), (2,), (3,), ())[n]:
                s1_copy(t, acc, k).start()

    def rs_mid2(t, acc):
        for n in range(4):
            s1_copy(t, acc, n).wait_recv()
            (fy, fx), h = IN1[n]
            acc[blk(fy, fx, 0), h * HALF:(h + 1) * HALF, :] += r1[t, n]
            if n < 2:
                s2_copy(t, acc, n).start()

    def rs_fin(t, acc, out):
        for n in range(2):
            s2_copy(t, acc, n).wait_recv()
            rows = slice(n * HALF, (n + 1) * HALF)
            out[rows, :] = (acc[me, rows, :] + r2[t, n]).astype(BF16)

    def rs_drain(t, acc):
        for n in range(4):
            dd_copy(t, acc, n).wait_send()
            s1_copy(t, acc, n).wait_send()
        for n in range(2):
            s2_copy(t, acc, n).wait_send()

    def fwd_group(g, _):
        gather_all(g, xs)

        def fwd(i, _):
            n = g * GRP + i
            w13, w2 = weights(n)
            uv = nn(xe_s[i], w13).astype(BF16)
            uv_s[n] = uv
            a = act(uv.astype(F32))[3]
            put_rows(i, nn(a, w2))
            return 0

        lax.fori_loop(0, GRP, fwd, 0)
        combine_y(g)

        @pl.when(g == 0)
        def _():
            ag_relay(1, dys, (0, 1, 2, 3))

        @pl.when(g == 1)
        def _():
            ag_relay(1, dys, (4, 5))

        @pl.when(g == 2)
        def _():
            ag_finish(1, dys)
            out_copies[3].start()
        return 0

    lax.fori_loop(0, ng, fwd_group, 0)

    def duv_copy(g):
        return pltpu.make_async_copy(uv_s.at[ds(g, GRP)], duv_hbm.at[ds(g, GRP)], osem.at[4])

    def a_copy(g):
        return pltpu.make_async_copy(a_s.at[lax.rem(g, 2)], a_hbm.at[ds(g, GRP)], osem.at[5])

    def bwd_group(g, _):
        gather_all(g, dys)
        slot = lax.rem(g, 2)

        @pl.when(g == 0)
        def _():
            rs_start(0, yacc)

        def bwd(i, _):
            e = g * GRP + i
            w13, w2 = weights(el + e)
            u, v, sg, a = act(uv_s[e].astype(F32))
            a_s[slot, i] = a
            of = nn(a, w2).astype(BF16).astype(F32)
            dyf = xe_s[i].astype(F32)
            dgc = jnp.sum(dyf * of, axis=1, keepdims=True)
            it = lax.broadcasted_iota(jnp.int32, (CAP, TOK), 0).astype(F32)
            for p in range(NP):
                m = jnp.broadcast_to(cm[p, pl.ds(e, 1), :], (CAP, TOK)) == it
                db = jnp.broadcast_to(dgc[p * CAP:(p + 1) * CAP], (CAP, TOK))
                dgm[p, pl.ds(e, 1), :] = jnp.sum(jnp.where(m, db, 0.0), axis=0, keepdims=True)
            do = (gate_column(cm, gm, e) * dyf).astype(BF16)
            da = nt(do, w2)
            du = (da * v * sg * (1.0 + u * (1.0 - sg))).astype(BF16)
            dv = (da * u * sg).astype(BF16)
            duv = jnp.concatenate([du, dv], axis=1)
            uv_s[e] = duv
            put_rows(i, nt(duv, w13))
            return 0

        @pl.when(g > 0)
        def _():
            a_copy(g - 1).wait()
            duv_copy(g - 1).wait()

        lax.fori_loop(0, GRP, bwd, 0)
        a_copy(g).start()
        duv_copy(g).start()
        combine_dx(g)

        @pl.when(g == 1)
        def _():
            rs_mid1(0, yacc)

        @pl.when(g == ng - 1)
        def _():
            rs_mid2(0, yacc)
        return 0

    lax.fori_loop(0, ng, bwd_group, 0)

    def spread_dg(p, _):
        rg = rgs[p]
        acc = jnp.zeros((top, TOK), F32)
        for e in range(el):
            ef = (e0 + e).astype(F32)
            acc = acc + jnp.where(rg[:top] == ef, jnp.broadcast_to(dgm[p, e:e + 1, :], (top, TOK)), 0.0)
        dgo[p] = acc
        return 0

    lax.fori_loop(0, NP, spread_dg, 0)
    rs_start(1, dxacc)
    rs_fin(0, yacc, y_ref)
    dg_copies = [remote(dgo.at[blk(*to)], dgr.at[n], dg_ss.at[n], dg_rs.at[n], to) for n, to in enumerate(peers)]
    for c in dg_copies:
        c.start()
    rs_mid1(1, dxacc)
    rs_mid2(1, dxacc)
    total = dgo[me]
    for n, c in enumerate(dg_copies):
        c.wait_recv()
        total = total + dgr[n]
    dg_ref[...] = total
    rs_fin(1, dxacc, dx_ref)

    ag_drain(0, xs)
    ag_drain(1, dys)
    rs_drain(0, yacc)
    rs_drain(1, dxacc)
    for c in rg_copies + dg_copies:
        c.wait_send()
    for c in out_copies:
        c.wait()
    a_copy(ng - 1).wait()
    duv_copy(ng - 1).wait()


def grad_kernel(el, eb, xa_hbm, dya_hbm, cm, gm, a_ref, duv_ref, gw1_ref, gw3_ref, gw2_ref, xs, dys, xe_s, dye_s, sem):
    s = pl.program_id(0)
    per = GRP // eb
    ff = a_ref.shape[2]

    @pl.when(s == 0)
    def _():
        cx = pltpu.make_async_copy(xa_hbm, xs, sem.at[0])
        cd = pltpu.make_async_copy(dya_hbm, dys, sem.at[1])
        cx.start()
        cd.start()
        cx.wait()
        cd.wait()

    @pl.when(s < el // eb)
    def _():
        g = lax.div(s, per)
        slot = lax.rem(g, 2)
        for k in range(NP // 2 // per):
            q = lax.rem(s, per) * (NP // 2 // per) + k
            for src, dst in ((xs, xe_s), (dys, dye_s)):
                def store(j, rows, val):
                    dst[slot, j, rows, :] = val
                gather_pair(cm, g, q, src, store)

    @pl.when(s >= per)
    def _():
        t = s - per
        g = lax.div(t, per)
        slot = lax.rem(g, 2)
        for k in range(eb):
            i = lax.rem(t, per) * eb + k
            e = g * GRP + i
            do = (gate_column(cm, gm, e) * dye_s[slot, i].astype(F32)).astype(BF16)
            gw2_ref[k] = tn(a_ref[k], do)
            g13 = tn(xe_s[slot, i], duv_ref[k])
            gw1_ref[k] = g13[:, :ff]
            gw3_ref[k] = g13[:, ff:]


def solution(mesh):
    grp = ('row', 'col')
    tspec = P(('dp', 'row', 'col'), None)
    wspec = P(grp, None, None)
    gspec = P(('dp', 'row', 'col'), None, None)

    def local(x, ridx, gates, w1, w3, w2, dy):
        tok, d = x.shape
        top = ridx.shape[1]
        el, _, ff = w1.shape
        anyspec = pl.BlockSpec(memory_space=pl.ANY)
        vm = pl.BlockSpec(memory_space=pltpu.VMEM)
        sds = jax.ShapeDtypeStruct
        rg = jnp.concatenate([ridx.T.astype(F32), gates.T], axis=0)
        dma = pltpu.SemaphoreType.DMA
        y, dx, dg, xa, dya, cm, gm, duv, a = pl.pallas_call(
            functools.partial(main_kernel, el),
            in_specs=[anyspec, anyspec, vm, anyspec, anyspec, anyspec],
            out_specs=[vm, vm, vm] + [anyspec] * 6,
            out_shape=[
                sds((tok, d), BF16), sds((tok, d), BF16), sds((top, tok), F32),
                sds((NP, tok, d), BF16), sds((NP, tok, d), BF16),
                sds((NP, el, tok), F32), sds((NP, el, tok), F32),
                sds((el, NROW, 2 * ff), BF16), sds((el, NROW, ff), BF16),
            ],
            scratch_shapes=[
                pltpu.VMEM((NP, tok, d), BF16),
                pltpu.VMEM((NP, tok, d), BF16),
                pltpu.VMEM((NP, 2 * top, tok), F32),
                pltpu.VMEM((GRP, NROW, d), BF16),
                pltpu.VMEM((GRP, NP * PAD, d), BF16),
                pltpu.VMEM((el, NROW, 2 * ff), BF16),
                pltpu.VMEM((2, GRP, NROW, ff), BF16),
                pltpu.VMEM((NP, tok, d), F32),
                pltpu.VMEM((NP, tok, d), F32),
                pltpu.VMEM((NP, el, tok), F32),
                pltpu.VMEM((NP, el, tok), F32),
                pltpu.VMEM((NP, el, tok), F32),
                pltpu.VMEM((NP, top, tok), F32),
                pltpu.VMEM((NP - 1, top, tok), F32),
                pltpu.VMEM((NBUF, d, ff), BF16),
                pltpu.VMEM((NBUF, d, ff), BF16),
                pltpu.VMEM((NBUF, ff, d), BF16),
                pltpu.VMEM((2, 4, tok, d), F32),
                pltpu.VMEM((2, 4, tok // 2, d), F32),
                pltpu.VMEM((2, 2, tok // 2, d), F32),
                dma((3, NBUF)), dma((2,)), dma((6,)),
                dma((NP - 1,)), dma((NP - 1,)),
                dma((2, 14)), dma((2, 14)),
                dma((2, 4)), dma((2, 4)),
                dma((2, 4)), dma((2, 4)),
                dma((2, 2)), dma((2, 2)),
                dma((NP - 1,)), dma((NP - 1,)),
            ],
            compiler_params=pltpu.CompilerParams(
                collective_id=0, has_side_effects=True, vmem_limit_bytes=67_000_000),
            cost_estimate=pl.CostEstimate(flops=40_000_000_000, bytes_accessed=160_000_000, transcendentals=0),
        )(x, dy, rg, w1, w3, w2)

        eb = 2
        per = GRP // eb
        steps = el // eb + per

        def eidx(s):
            return (jnp.clip(s - per, 0, el // eb - 1), 0, 0)

        gw1, gw3, gw2 = pl.pallas_call(
            functools.partial(grad_kernel, el, eb),
            grid=(steps,),
            in_specs=[anyspec, anyspec, vm, vm, pl.BlockSpec((eb, NROW, ff), eidx), pl.BlockSpec((eb, NROW, 2 * ff), eidx)],
            out_specs=[pl.BlockSpec((eb, d, ff), eidx), pl.BlockSpec((eb, d, ff), eidx), pl.BlockSpec((eb, ff, d), eidx)],
            out_shape=[sds((el, d, ff), F32), sds((el, d, ff), F32), sds((el, ff, d), F32)],
            scratch_shapes=[
                pltpu.VMEM((NP, tok, d), BF16),
                pltpu.VMEM((NP, tok, d), BF16),
                pltpu.VMEM((2, GRP, NROW, d), BF16),
                pltpu.VMEM((2, GRP, NROW, d), BF16),
                pltpu.SemaphoreType.DMA((2,)),
            ],
            compiler_params=pltpu.CompilerParams(
                dimension_semantics=('arbitrary',), vmem_limit_bytes=60_000_000),
            cost_estimate=pl.CostEstimate(flops=20_000_000_000, bytes_accessed=150_000_000, transcendentals=0),
        )(xa, dya, cm, gm, a, duv)
        return y, dx, dg.T, gw1, gw3, gw2

    return jax.shard_map(local, mesh=mesh, in_specs=(tspec, tspec, tspec, wspec, wspec, wspec, tspec), out_specs=(tspec, tspec, tspec, gspec, gspec, gspec), check_vma=False)
```

```python
import functools

import jax
import jax.numpy as jnp
from jax import lax
from jax.experimental import pallas as pl
from jax.experimental.pallas import tpu as pltpu
from jax.sharding import PartitionSpec as P

F32 = jnp.float32
BF16 = jnp.bfloat16
MESH = pl.DeviceIdType.MESH
NP = 8
TOK = 256
HALF = TOK // 2
CAP = 24
PAD = 32
GRP = 8
NROW = NP * CAP
NBUF = 6
PAIR = 2
SPLIT = 24


def nt(a, b):
    return lax.dot_general(a, b, (((1,), (1,)), ((), ())), preferred_element_type=F32)


def nn(a, b):
    return lax.dot_general(a, b, (((1,), (0,)), ((), ())), preferred_element_type=F32)


def tn(a, b):
    return lax.dot_general(a, b, (((0,), (0,)), ((), ())), preferred_element_type=F32)


def onehot(rows, cap):
    n = rows.shape[0]
    it = lax.broadcasted_iota(jnp.int32, (cap, TOK), 0).astype(F32)
    return [jnp.broadcast_to(rows[k:k + 1], (cap, TOK)) == it for k in range(n)]


def ds(i, n):
    return pl.ds(pl.multiple_of(i * n, n), n)


def gather_pair(cm, g, q, src, store):
    res = []
    for h in range(2):
        p = q * 2 + h
        oh = onehot(cm[p, ds(g, GRP), :], CAP)
        oh = jnp.concatenate([jnp.where(m, 1.0, 0.0) for m in oh], axis=0).astype(BF16)
        res.append(nn(oh, src[p]))
    for k in range(GRP):
        blk = jnp.concatenate([r[k * CAP:(k + 1) * CAP] for r in res], axis=0)
        store(k, ds(q, 2 * CAP), blk.astype(BF16))


def gate_column(cm, gm, e):
    it = lax.broadcasted_iota(jnp.int32, (CAP, TOK), 0).astype(F32)
    cols = []
    for p in range(NP):
        m = jnp.broadcast_to(cm[p, pl.ds(e, 1), :], (CAP, TOK)) == it
        gb = jnp.broadcast_to(gm[p, pl.ds(e, 1), :], (CAP, TOK))
        cols.append(jnp.sum(jnp.where(m, gb, 0.0), axis=1, keepdims=True))
    return jnp.concatenate(cols, axis=0)


def main_kernel(el, x_hbm, dy_hbm, rg_ref, w1_hbm, w3_hbm, w2_hbm,
                y_ref, dg_ref, sx_hbm, sy_hbm, ka_hbm, kb_hbm, xa_hbm, dya_hbm, cm_hbm, gm_hbm, duv_hbm, a_hbm,
                xs, dys, rgs, xe_s, o_s, uv_s, a_s, yacc, dxacc, cm, gm, dgm, dgo, dgr,
                w1b, w3b, w2b, rd, r1, r2,
                wsem, lsem, osem, psem, rg_ss, rg_rs, ag_ss, ag_rs, dd_ss, dd_rs, s1_ss, s1_rs, s2_ss, s2_rs, dg_ss, dg_rs):
    ng = el // GRP
    ff = w2b.shape[1]
    Z = lax.axis_index('dp')
    Y = lax.axis_index('row')
    col = lax.axis_index('col')
    X = lax.div(col, 2)
    C = lax.rem(col, 2)
    me = Y * 4 + col
    e0 = me * el

    def pos(fy, fx, fc):
        return (1 - Y if fy else Y), (1 - X if fx else X), (1 - C if fc else C)

    def blk(fy, fx, fc):
        yy, xx, cc = pos(fy, fx, fc)
        return yy * 4 + xx * 2 + cc

    def dev(fy, fx, fc):
        yy, xx, cc = pos(fy, fx, fc)
        return (Z, yy, xx * 2 + cc)

    peers = [(a, b, c) for a in range(2) for b in range(2) for c in range(2)][1:]

    def remote(src, dst, ss, rs, to):
        return pltpu.make_async_remote_copy(src_ref=src, dst_ref=dst, send_sem=ss, recv_sem=rs,
                                            device_id=dev(*to), device_id_type=MESH)

    lx = pltpu.make_async_copy(x_hbm, xs.at[me], lsem.at[0])
    ld = pltpu.make_async_copy(dy_hbm, dys.at[me], lsem.at[1])
    lx.start()
    ld.start()

    def wcopies(e):
        b = lax.rem(e, NBUF)
        k = lax.rem(e, el)
        return [pltpu.make_async_copy(h.at[k], v.at[b], wsem.at[n, b])
                for n, (h, v) in enumerate(((w1_hbm, w1b), (w3_hbm, w3b), (w2_hbm, w2b)))]

    for e in range(NBUF - PAIR):
        for c in wcopies(e):
            c.start()

    barrier = pltpu.get_barrier_semaphore()
    for to in peers:
        pl.semaphore_signal(barrier, inc=1, device_id=dev(*to), device_id_type=MESH)
    pl.semaphore_wait(barrier, len(peers))

    rgs[me] = rg_ref[...]
    rg_copies = [remote(rg_ref, rgs.at[me], rg_ss.at[n], rg_rs.at[n], to) for n, to in enumerate(peers)]
    for c in rg_copies:
        c.start()

    def half(buf, b, h):
        return buf.at[b, pl.ds(h * HALF, HALF), :]

    XN, YN, DN, PN = (0, 1, 0), (1, 0, 0), (1, 1, 0), (0, 0, 1)
    FIRST = [(0, (0, 0, 0), 0, XN), (1, (0, 0, 0), 1, YN), (2, (0, 0, 0), 1, XN), (3, (0, 0, 0), 0, YN)]
    OWN2 = [(6, (0, 0, 0), 0, PN), (7, (0, 0, 0), 1, PN)]
    FWD = [(4, XN, 0, YN), (5, YN, 1, XN)]
    ARR = {0: (XN, 0), 1: (YN, 1), 2: (XN, 1), 3: (YN, 0), 4: (DN, 0), 5: (DN, 1)}
    ONWARD = {0: 8, 1: 9, 2: 10, 3: 11, 4: 12, 5: 13}

    def ag_copy(t, buf, n, f, h, to):
        r = half(buf, blk(*f), h)
        return remote(r, r, ag_ss.at[t, n], ag_rs.at[t, n], to)

    def ag_recv(t, buf, n, f, h):
        r = half(buf, blk(*f), h)
        remote(r, r, ag_ss.at[t, n], ag_rs.at[t, n], PN).wait_recv()

    def ag_start(t, buf):
        for n, f, h, to in FIRST + OWN2:
            ag_copy(t, buf, n, f, h, to).start()

    def ag_relay(t, buf, ns):
        for n in ns:
            f, h = ARR[n]
            ag_recv(t, buf, n, f, h)
            if n < 2:
                k, ff_, hh, to = FWD[n]
                ag_copy(t, buf, k, ff_, hh, to).start()
            ag_copy(t, buf, ONWARD[n], f, h, PN).start()

    def ag_finish(t, buf):
        for n, h in ((6, 0), (7, 1)):
            ag_recv(t, buf, n, PN, h)
        for n, k in ONWARD.items():
            f, h = ARR[n]
            ag_recv(t, buf, k, (f[0], f[1], 1), h)

    def ag_drain(t, buf):
        for n, f, h, to in FIRST + OWN2 + FWD:
            ag_copy(t, buf, n, f, h, to).wait_send()
        for n, k in ONWARD.items():
            f, h = ARR[n]
            ag_copy(t, buf, k, f, h, PN).wait_send()

    lx.wait()
    ld.wait()
    ag_start(0, xs)

    def zero(p, _):
        yacc[p] = jnp.zeros(yacc.shape[1:], F32)
        dxacc[p] = jnp.zeros(dxacc.shape[1:], F32)
        return 0

    lax.fori_loop(0, NP, zero, 0)

    for n, to in enumerate(peers):
        remote(rgs.at[blk(*to)], rgs.at[blk(*to)], rg_ss.at[n], rg_rs.at[n], to).wait_recv()
    top = rgs.shape[1] // 2
    tr = lax.broadcasted_iota(jnp.int32, (TOK, TOK), 0)
    tc = lax.broadcasted_iota(jnp.int32, (TOK, TOK), 1)
    tri = jnp.where(tr < tc, 1.0, 0.0).astype(BF16)
    ee = (lax.broadcasted_iota(jnp.int32, (el, TOK), 0) + e0).astype(F32)

    def prep(p, _):
        rg = rgs[p]
        m = jnp.zeros((el, TOK), F32)
        gs = jnp.zeros((el, TOK), F32)
        for j in range(top):
            hit = jnp.broadcast_to(rg[j:j + 1], (el, TOK)) == ee
            m = jnp.where(hit, 1.0, m)
            gs = jnp.where(hit, jnp.broadcast_to(rg[top + j:top + j + 1], (el, TOK)), gs)
        rank = nn(m.astype(BF16), tri)
        cm[p] = jnp.where(m > 0.0, rank, -1.0)
        gm[p] = gs
        return 0

    lax.fori_loop(0, NP, prep, 0)

    ag_relay(0, xs, (0, 1, 2, 3))
    ag_start(1, dys)
    ag_relay(0, xs, (4, 5))
    ag_finish(0, xs)
    out_copies = [pltpu.make_async_copy(xs, xa_hbm, osem.at[0]),
                  pltpu.make_async_copy(cm, cm_hbm, osem.at[1]),
                  pltpu.make_async_copy(gm, gm_hbm, osem.at[2]),
                  pltpu.make_async_copy(dys, dya_hbm, osem.at[3])]
    for c in out_copies[:3]:
        c.start()

    def gather_all(g, src):
        def step(q, _):
            def store(k, rows, val):
                xe_s[k, rows, :] = val
            gather_pair(cm, g, q, src, store)
            return 0
        lax.fori_loop(0, NP // 2, step, 0, unroll=2)

    def put_rows(i, val):
        zero = jnp.zeros((PAD - CAP, val.shape[1]), F32)
        for p in range(NP):
            o_s[i, p * PAD:(p + 1) * PAD, :] = jnp.concatenate([val[p * CAP:(p + 1) * CAP], zero], axis=0).astype(BF16)

    def take_rows(p):
        return jnp.concatenate([o_s[k, ds(p, PAD), :] for k in range(GRP)], axis=0)

    def combine_y(g):
        def step(p, _):
            oh = onehot(cm[p, ds(g, GRP), :], PAD)
            gr = gm[p, ds(g, GRP), :]
            g1 = gr.astype(BF16).astype(F32)
            rest = gr - g1
            g2 = rest.astype(BF16).astype(F32)
            g3 = rest - g2
            ob = take_rows(p)

            def spread(part):
                return jnp.concatenate(
                    [jnp.where(oh[k], jnp.broadcast_to(part[k:k + 1], (PAD, TOK)), 0.0) for k in range(GRP)],
                    axis=0).astype(BF16)

            gs = jnp.concatenate([spread(g1), spread(g2), spread(g3)], axis=0)
            yacc[p] += tn(gs, jnp.concatenate([ob, ob, ob], axis=0))
            return 0
        lax.fori_loop(0, NP, step, 0, unroll=2)

    def combine_dx(g):
        def step(p, _):
            oh = onehot(cm[p, ds(g, GRP), :], PAD)
            one = jnp.concatenate([jnp.where(m, 1.0, 0.0) for m in oh], axis=0).astype(BF16)
            dxacc[p] += tn(one, take_rows(p))
            return 0
        lax.fori_loop(0, NP, step, 0, unroll=2)

    def weights(n):
        for k in range(PAIR):
            for c in wcopies(n + k):
                c.wait()

        @pl.when(n + NBUF - PAIR < 2 * el)
        def _():
            for k in range(PAIR):
                for c in wcopies(n + NBUF - PAIR + k):
                    c.start()
        bufs = [lax.rem(n + k, NBUF) for k in range(PAIR)]
        return [(jnp.concatenate([w1b[b], w3b[b]], axis=1), w2b[b]) for b in bufs]

    def act(uv):
        u, v = uv[:, :ff], uv[:, ff:]
        sg = jax.nn.sigmoid(u)
        return u, v, sg, (u * sg * v).astype(BF16)

    ORDER = [(1, 1), (0, 1), (1, 0), (0, 0)]
    S1 = [((1, 1), 0, XN), ((1, 1), 1, YN), ((0, 1), 0, XN), ((1, 0), 1, YN)]
    IN1 = [((1, 0), 0), ((0, 1), 1), ((0, 0), 0), ((0, 0), 1)]
    S2 = [YN, XN]

    def dd_copy(t, acc, n):
        fy, fx = ORDER[n]
        return remote(acc.at[blk(fy, fx, 1)], rd.at[t, n], dd_ss.at[t, n], dd_rs.at[t, n], PN)

    def s1_copy(t, acc, n):
        (fy, fx), h, to = S1[n]
        return remote(half(acc, blk(fy, fx, 0), h), r1.at[t, n], s1_ss.at[t, n], s1_rs.at[t, n], to)

    def s2_copy(t, acc, n):
        (fy, fx), h = IN1[n]
        return remote(half(acc, blk(fy, fx, 0), h), r2.at[t, n], s2_ss.at[t, n], s2_rs.at[t, n], S2[n])

    def rs_start(t, acc):
        for n in range(4):
            dd_copy(t, acc, n).start()

    def rs_mid1(t, acc):
        for n in range(4):
            dd_copy(t, acc, n).wait_recv()
            fy, fx = ORDER[n]
            acc[blk(fy, fx, 0)] += rd[t, n]
            for k in ((0, 1), (2,), (3,), ())[n]:
                s1_copy(t, acc, k).start()

    def rs_mid2(t, acc):
        for n in range(4):
            s1_copy(t, acc, n).wait_recv()
            (fy, fx), h = IN1[n]
            acc[blk(fy, fx, 0), h * HALF:(h + 1) * HALF, :] += r1[t, n]
            if n < 2:
                s2_copy(t, acc, n).start()

    def rs_fin(t, acc, out):
        for n in range(2):
            s2_copy(t, acc, n).wait_recv()
            rows = slice(n * HALF, (n + 1) * HALF)
            out[rows, :] = (acc[me, rows, :] + r2[t, n]).astype(BF16)

    def rs_drain(t, acc):
        for n in range(4):
            dd_copy(t, acc, n).wait_send()
            s1_copy(t, acc, n).wait_send()
        for n in range(2):
            s2_copy(t, acc, n).wait_send()

    def fwd_group(g, _):
        gather_all(g, xs)

        def fwd(r, _):
            n = g * GRP + r * PAIR
            for k, (w13, w2) in enumerate(weights(n)):
                i = r * PAIR + k
                uv = nn(xe_s[i], w13).astype(BF16)
                uv_s[n + k] = uv
                a = act(uv.astype(F32))[3]
                put_rows(i, nn(a, w2))
            return 0

        lax.fori_loop(0, GRP // PAIR, fwd, 0)
        combine_y(g)

        @pl.when(g == 0)
        def _():
            ag_relay(1, dys, (0, 1, 2, 3))

        @pl.when(g == 1)
        def _():
            ag_relay(1, dys, (4, 5))

        @pl.when(g == 2)
        def _():
            ag_finish(1, dys)
            out_copies[3].start()
        return 0

    lax.fori_loop(0, ng, fwd_group, 0)

    def duv_copy(g):
        return pltpu.make_async_copy(uv_s.at[ds(g, GRP)], duv_hbm.at[ds(g, GRP)], osem.at[4])

    def a_copy(g):
        return pltpu.make_async_copy(a_s.at[lax.rem(g, 2)], a_hbm.at[ds(g, GRP)], osem.at[5])

    def bwd_group(g, _):
        gather_all(g, dys)
        slot = lax.rem(g, 2)

        @pl.when(g == 0)
        def _():
            rs_start(0, yacc)

        def bwd(r, _):
            n = g * GRP + r * PAIR
            for k, (w13, w2) in enumerate(weights(el + n)):
                i = r * PAIR + k
                e = n + k
                u, v, sg, a = act(uv_s[e].astype(F32))
                a_s[slot, i] = a
                of = nn(a, w2).astype(BF16).astype(F32)
                dyf = xe_s[i].astype(F32)
                dgc = jnp.sum(dyf * of, axis=1, keepdims=True)
                it = lax.broadcasted_iota(jnp.int32, (CAP, TOK), 0).astype(F32)
                for p in range(NP):
                    m = jnp.broadcast_to(cm[p, pl.ds(e, 1), :], (CAP, TOK)) == it
                    db = jnp.broadcast_to(dgc[p * CAP:(p + 1) * CAP], (CAP, TOK))
                    dgm[p, pl.ds(e, 1), :] = jnp.sum(jnp.where(m, db, 0.0), axis=0, keepdims=True)
                do = (gate_column(cm, gm, e) * dyf).astype(BF16)
                da = nt(do, w2)
                du = (da * v * sg * (1.0 + u * (1.0 - sg))).astype(BF16)
                dv = (da * u * sg).astype(BF16)
                duv = jnp.concatenate([du, dv], axis=1)
                uv_s[e] = duv
                put_rows(i, nt(duv, w13))
            return 0

        @pl.when(g > 0)
        def _():
            a_copy(g - 1).wait()
            duv_copy(g - 1).wait()

        lax.fori_loop(0, GRP // PAIR, bwd, 0)
        a_copy(g).start()
        duv_copy(g).start()
        combine_dx(g)

        @pl.when(g == 1)
        def _():
            rs_mid1(0, yacc)

        @pl.when(g == ng - 1)
        def _():
            rs_mid2(0, yacc)
        return 0

    lax.fori_loop(0, ng, bwd_group, 0)

    def spread_dg(p, _):
        rg = rgs[p]
        acc = jnp.zeros((top, TOK), F32)
        for e in range(el):
            ef = (e0 + e).astype(F32)
            acc = acc + jnp.where(rg[:top] == ef, jnp.broadcast_to(dgm[p, e:e + 1, :], (top, TOK)), 0.0)
        dgo[p] = acc
        return 0

    lax.fori_loop(0, NP, spread_dg, 0)
    rs_start(1, dxacc)
    rs_fin(0, yacc, y_ref)
    dg_copies = [remote(dgo.at[blk(*to)], dgr.at[n], dg_ss.at[n], dg_rs.at[n], to) for n, to in enumerate(peers)]
    for c in dg_copies:
        c.start()
    part_copies = []
    for n in range(4):
        dd_copy(1, dxacc, n).wait_recv()
        fy, fx = ORDER[n]
        b = blk(fy, fx, 0)
        dxacc[b] += rd[1, n]
        to_b = (sy_hbm.at[0], kb_hbm.at[0], sy_hbm.at[1], kb_hbm.at[1])[n]
        to_a = (sx_hbm.at[0], sx_hbm.at[1], ka_hbm.at[0], ka_hbm.at[1])[n]
        for h, to in enumerate((to_a, to_b)):
            c = pltpu.make_async_copy(half(dxacc, b, h), to, psem.at[n, h])
            c.start()
            part_copies.append(c)
    total = dgo[me]
    for n, c in enumerate(dg_copies):
        c.wait_recv()
        total = total + dgr[n]
    dg_ref[...] = total

    ag_drain(0, xs)
    ag_drain(1, dys)
    rs_drain(0, yacc)
    for n in range(4):
        dd_copy(1, dxacc, n).wait_send()
    for c in part_copies:
        c.wait()
    for c in rg_copies + dg_copies:
        c.wait_send()
    for c in out_copies:
        c.wait()
    a_copy(ng - 1).wait()
    duv_copy(ng - 1).wait()


def grad_kernel(first, count, eb, nprev, xa_hbm, dya_hbm, cm, gm, a_ref, duv_ref, *refs):
    gw1_ref, gw3_ref, gw2_ref, xs, dys, xe_s, dye_s, sem = refs[nprev:]
    s = pl.program_id(0)
    per = GRP // eb
    ff = a_ref.shape[2]

    @pl.when(s == 0)
    def _():
        cx = pltpu.make_async_copy(xa_hbm, xs, sem.at[0])
        cd = pltpu.make_async_copy(dya_hbm, dys, sem.at[1])
        cx.start()
        cd.start()
        cx.wait()
        cd.wait()

    @pl.when(s < count // eb)
    def _():
        g = lax.div(s, per)
        slot = lax.rem(g, 2)
        for k in range(NP // 2 // per):
            q = lax.rem(s, per) * (NP // 2 // per) + k
            for src, dst in ((xs, xe_s), (dys, dye_s)):
                def store(j, rows, val):
                    dst[slot, j, rows, :] = val
                gather_pair(cm, first // GRP + g, q, src, store)

    @pl.when(s >= per)
    def _():
        t = s - per
        g = lax.div(t, per)
        slot = lax.rem(g, 2)
        for k in range(eb):
            i = lax.rem(t, per) * eb + k
            e = first + g * GRP + i
            do = (gate_column(cm, gm, e) * dye_s[slot, i].astype(F32)).astype(BF16)
            gw2_ref[k] = tn(a_ref[k], do)
            g13 = tn(xe_s[slot, i], duv_ref[k])
            gw1_ref[k] = g13[:, :ff]
            gw3_ref[k] = g13[:, ff:]


def solution(mesh):
    grp = ('row', 'col')
    tspec = P(('dp', 'row', 'col'), None)
    wspec = P(grp, None, None)
    gspec = P(('dp', 'row', 'col'), None, None)

    def local(x, ridx, gates, w1, w3, w2, dy):
        tok, d = x.shape
        top = ridx.shape[1]
        el, _, ff = w1.shape
        anyspec = pl.BlockSpec(memory_space=pl.ANY)
        vm = pl.BlockSpec(memory_space=pltpu.VMEM)
        sds = jax.ShapeDtypeStruct
        rg = jnp.concatenate([ridx.T.astype(F32), gates.T], axis=0)
        dma = pltpu.SemaphoreType.DMA
        y, dg, sx, sy, ka, kb, xa, dya, cm, gm, duv, a = pl.pallas_call(
            functools.partial(main_kernel, el),
            in_specs=[anyspec, anyspec, vm, anyspec, anyspec, anyspec],
            out_specs=[vm, vm] + [anyspec] * 10,
            out_shape=[
                sds((tok, d), BF16), sds((top, tok), F32)] + [sds((2, tok // 2, d), F32)] * 4 + [
                sds((NP, tok, d), BF16), sds((NP, tok, d), BF16),
                sds((NP, el, tok), F32), sds((NP, el, tok), F32),
                sds((el, NROW, 2 * ff), BF16), sds((el, NROW, ff), BF16),
            ],
            scratch_shapes=[
                pltpu.VMEM((NP, tok, d), BF16),
                pltpu.VMEM((NP, tok, d), BF16),
                pltpu.VMEM((NP, 2 * top, tok), F32),
                pltpu.VMEM((GRP, NROW, d), BF16),
                pltpu.VMEM((GRP, NP * PAD, d), BF16),
                pltpu.VMEM((el, NROW, 2 * ff), BF16),
                pltpu.VMEM((2, GRP, NROW, ff), BF16),
                pltpu.VMEM((NP, tok, d), F32),
                pltpu.VMEM((NP, tok, d), F32),
                pltpu.VMEM((NP, el, tok), F32),
                pltpu.VMEM((NP, el, tok), F32),
                pltpu.VMEM((NP, el, tok), F32),
                pltpu.VMEM((NP, top, tok), F32),
                pltpu.VMEM((NP - 1, top, tok), F32),
                pltpu.VMEM((NBUF, d, ff), BF16),
                pltpu.VMEM((NBUF, d, ff), BF16),
                pltpu.VMEM((NBUF, ff, d), BF16),
                pltpu.VMEM((2, 4, tok, d), F32),
                pltpu.VMEM((1, 4, tok // 2, d), F32),
                pltpu.VMEM((1, 2, tok // 2, d), F32),
                dma((3, NBUF)), dma((2,)), dma((6,)), dma((4, 2)),
                dma((NP - 1,)), dma((NP - 1,)),
                dma((2, 14)), dma((2, 14)),
                dma((2, 4)), dma((2, 4)),
                dma((1, 4)), dma((1, 4)),
                dma((1, 2)), dma((1, 2)),
                dma((NP - 1,)), dma((NP - 1,)),
            ],
            compiler_params=pltpu.CompilerParams(
                collective_id=0, has_side_effects=True, vmem_limit_bytes=67_000_000),
            cost_estimate=pl.CostEstimate(flops=40_000_000_000, bytes_accessed=160_000_000, transcendentals=0),
        )(x, dy, rg, w1, w3, w2)

        def perm(fy, fx):
            out = []
            for p in range(NP):
                yy, xx, cc = p // 4, (p // 2) % 2, p % 2
                out.append((p, (yy ^ fy) * 4 + (xx ^ fx) * 2 + cc))
            return out

        eb = 2
        per = GRP // eb

        def grads(first, count, prev):
            steps = count // eb + per

            def eidx(s):
                return (first // eb + jnp.clip(s - per, 0, count // eb - 1), 0, 0)

            return pl.pallas_call(
                functools.partial(grad_kernel, first, count, eb, len(prev)),
                grid=(steps,),
                in_specs=[anyspec, anyspec, vm, vm, pl.BlockSpec((eb, NROW, ff), eidx), pl.BlockSpec((eb, NROW, 2 * ff), eidx)] + [anyspec] * len(prev),
                out_specs=[pl.BlockSpec((eb, d, ff), eidx), pl.BlockSpec((eb, d, ff), eidx), pl.BlockSpec((eb, ff, d), eidx)],
                out_shape=[sds((el, d, ff), F32), sds((el, d, ff), F32), sds((el, ff, d), F32)],
                input_output_aliases={6 + k: k for k in range(len(prev))},
                scratch_shapes=[
                    pltpu.VMEM((NP, tok, d), BF16),
                    pltpu.VMEM((NP, tok, d), BF16),
                    pltpu.VMEM((2, GRP, NROW, d), BF16),
                    pltpu.VMEM((2, GRP, NROW, d), BF16),
                    pltpu.SemaphoreType.DMA((2,)),
                ],
                compiler_params=pltpu.CompilerParams(
                    dimension_semantics=('arbitrary',), vmem_limit_bytes=60_000_000),
                cost_estimate=pl.CostEstimate(flops=20_000_000_000 * count // el, bytes_accessed=150_000_000 * count // el, transcendentals=0),
            )(xa, dya, cm, gm, a, duv, *prev)

        r1x = lax.ppermute(sx, grp, perm(0, 1))
        r1y = lax.ppermute(sy, grp, perm(1, 0))
        prev = grads(0, SPLIT, ())
        prev, r1x, r1y = lax.optimization_barrier((prev, r1x, r1y))
        r2a = lax.ppermute(ka[0] + r1x[0], grp, perm(1, 0))
        r2b = lax.ppermute(kb[0] + r1y[0], grp, perm(0, 1))
        gw1, gw3, gw2 = grads(SPLIT, el - SPLIT, tuple(prev))
        dx = jnp.concatenate([ka[1] + r1x[1] + r2a, kb[1] + r1y[1] + r2b], axis=0).astype(BF16)
        return y, dx, dg.T, gw1, gw3, gw2

    return jax.shard_map(local, mesh=mesh, in_specs=(tspec, tspec, tspec, wspec, wspec, wspec, tspec), out_specs=(tspec, tspec, tspec, gspec, gspec, gspec), check_vma=False)
```

```python
import functools

import jax
import jax.numpy as jnp
from jax import lax
from jax.experimental import pallas as pl
from jax.experimental.pallas import tpu as pltpu
from jax.sharding import PartitionSpec as P

F32 = jnp.float32
BF16 = jnp.bfloat16
MESH = pl.DeviceIdType.MESH
NP = 8
TOK = 256
HALF = TOK // 2
CAP = 24
PAD = 32
GRP = 8
NROW = NP * CAP
NBUF = 8
PAIR = 2
SPLIT = 24


def nt(a, b):
    return lax.dot_general(a, b, (((1,), (1,)), ((), ())), preferred_element_type=F32)


def nn(a, b):
    return lax.dot_general(a, b, (((1,), (0,)), ((), ())), preferred_element_type=F32)


def tn(a, b):
    return lax.dot_general(a, b, (((0,), (0,)), ((), ())), preferred_element_type=F32)


def onehot(rows, cap):
    n = rows.shape[0]
    it = lax.broadcasted_iota(jnp.int32, (cap, TOK), 0).astype(F32)
    return [jnp.broadcast_to(rows[k:k + 1], (cap, TOK)) == it for k in range(n)]


def ds(i, n):
    return pl.ds(pl.multiple_of(i * n, n), n)


def gather_pair(cm, g, q, src, store):
    res = []
    for h in range(2):
        p = q * 2 + h
        oh = onehot(cm[p, ds(g, GRP), :], CAP)
        oh = jnp.concatenate([jnp.where(m, 1.0, 0.0) for m in oh], axis=0).astype(BF16)
        res.append(nn(oh, src[p]))
    for k in range(GRP):
        blk = jnp.concatenate([r[k * CAP:(k + 1) * CAP] for r in res], axis=0)
        store(k, ds(q, 2 * CAP), blk.astype(BF16))


def gather_dy_pair(cm, gm, g, q, src, store, store_scaled):
    res, scaled = [], []
    for h in range(2):
        p = q * 2 + h
        oh = onehot(cm[p, ds(g, GRP), :], CAP)
        gr = gm[p, ds(g, GRP), :]
        col = jnp.concatenate(
            [jnp.sum(jnp.where(m, jnp.broadcast_to(gr[k:k + 1], (CAP, TOK)), 0.0), axis=1, keepdims=True)
             for k, m in enumerate(oh)], axis=0)
        oh = jnp.concatenate([jnp.where(m, 1.0, 0.0) for m in oh], axis=0).astype(BF16)
        r = nn(oh, src[p])
        res.append(r)
        scaled.append(col * r)
    for parts, put in ((res, store), (scaled, store_scaled)):
        for k in range(GRP):
            blk = jnp.concatenate([r[k * CAP:(k + 1) * CAP] for r in parts], axis=0)
            put(k, ds(q, 2 * CAP), blk.astype(BF16))


def gate_column(cm, gm, e):
    it = lax.broadcasted_iota(jnp.int32, (CAP, TOK), 0).astype(F32)
    cols = []
    for p in range(NP):
        m = jnp.broadcast_to(cm[p, pl.ds(e, 1), :], (CAP, TOK)) == it
        gb = jnp.broadcast_to(gm[p, pl.ds(e, 1), :], (CAP, TOK))
        cols.append(jnp.sum(jnp.where(m, gb, 0.0), axis=1, keepdims=True))
    return jnp.concatenate(cols, axis=0)


def main_kernel(el, x_hbm, dy_hbm, rg_ref, w1_hbm, w3_hbm, w2_hbm,
                y_ref, dg_ref, sx_hbm, sy_hbm, ka_hbm, kb_hbm, xa_hbm, dya_hbm, cm_hbm, gm_hbm, duv_hbm, a_hbm,
                xs, dys, rgs, xe_s, do_s, dgc_s, o_s, uv_s, a_s, yacc, dxacc, cm, gm, dgm, dgo, dgr,
                w1b, w3b, w2b, rd, r1, r2,
                wsem, lsem, osem, psem, credit, rg_ss, rg_rs, ag_ss, ag_rs, dd_ss, dd_rs, s1_ss, s1_rs, s2_ss, s2_rs, dg_ss, dg_rs):
    ng = el // GRP
    ff = w2b.shape[1]
    Z = lax.axis_index('dp')
    Y = lax.axis_index('row')
    col = lax.axis_index('col')
    X = lax.div(col, 2)
    C = lax.rem(col, 2)
    me = Y * 4 + col
    e0 = me * el

    def pos(fy, fx, fc):
        return (1 - Y if fy else Y), (1 - X if fx else X), (1 - C if fc else C)

    def blk(fy, fx, fc):
        yy, xx, cc = pos(fy, fx, fc)
        return yy * 4 + xx * 2 + cc

    def dev(fy, fx, fc):
        yy, xx, cc = pos(fy, fx, fc)
        return (Z, yy, xx * 2 + cc)

    peers = [(a, b, c) for a in range(2) for b in range(2) for c in range(2)][1:]

    def remote(src, dst, ss, rs, to):
        return pltpu.make_async_remote_copy(src_ref=src, dst_ref=dst, send_sem=ss, recv_sem=rs,
                                            device_id=dev(*to), device_id_type=MESH)

    lx = pltpu.make_async_copy(x_hbm, xs.at[me], lsem.at[0])
    ld = pltpu.make_async_copy(dy_hbm, dys.at[me], lsem.at[1])
    lx.start()
    ld.start()

    def wcopies(e):
        b = lax.rem(e, NBUF)
        k = lax.rem(e, el)
        return [pltpu.make_async_copy(h.at[k], v.at[b], wsem.at[n, b])
                for n, (h, v) in enumerate(((w1_hbm, w1b), (w3_hbm, w3b), (w2_hbm, w2b)))]

    for e in range(2 * PAIR):
        for c in wcopies(e):
            c.start()

    barrier = pltpu.get_barrier_semaphore()
    for to in peers:
        pl.semaphore_signal(barrier, inc=1, device_id=dev(*to), device_id_type=MESH)
    pl.semaphore_wait(barrier, len(peers))

    rgs[me] = rg_ref[...]
    rg_copies = [remote(rg_ref, rgs.at[me], rg_ss.at[n], rg_rs.at[n], to) for n, to in enumerate(peers)]
    for c in rg_copies:
        c.start()

    def half(buf, b, h):
        return buf.at[b, pl.ds(h * HALF, HALF), :]

    XN, YN, DN, PN = (0, 1, 0), (1, 0, 0), (1, 1, 0), (0, 0, 1)
    FIRST = [(0, (0, 0, 0), 0, XN), (1, (0, 0, 0), 1, YN), (2, (0, 0, 0), 1, XN), (3, (0, 0, 0), 0, YN)]
    OWN2 = [(6, (0, 0, 0), 0, PN), (7, (0, 0, 0), 1, PN)]
    FWD = [(4, XN, 0, YN), (5, YN, 1, XN)]
    ARR = {0: (XN, 0), 1: (YN, 1), 2: (XN, 1), 3: (YN, 0), 4: (DN, 0), 5: (DN, 1)}
    ONWARD = {0: 8, 1: 9, 2: 10, 3: 11, 4: 12, 5: 13}

    def ag_copy(t, buf, n, f, h, to):
        r = half(buf, blk(*f), h)
        return remote(r, r, ag_ss.at[t, n], ag_rs.at[t, n], to)

    def ag_recv(t, buf, n, f, h):
        r = half(buf, blk(*f), h)
        remote(r, r, ag_ss.at[t, n], ag_rs.at[t, n], PN).wait_recv()

    def ag_start(t, buf):
        for n, f, h, to in FIRST + OWN2:
            ag_copy(t, buf, n, f, h, to).start()

    def ag_relay(t, buf, ns):
        for n in ns:
            f, h = ARR[n]
            ag_recv(t, buf, n, f, h)
            if n < 2:
                k, ff_, hh, to = FWD[n]
                ag_copy(t, buf, k, ff_, hh, to).start()
            ag_copy(t, buf, ONWARD[n], f, h, PN).start()

    def ag_finish(t, buf):
        for n, h in ((6, 0), (7, 1)):
            ag_recv(t, buf, n, PN, h)
        for n, k in ONWARD.items():
            f, h = ARR[n]
            ag_recv(t, buf, k, (f[0], f[1], 1), h)

    def ag_drain(t, buf):
        for n, f, h, to in FIRST + OWN2 + FWD:
            ag_copy(t, buf, n, f, h, to).wait_send()
        for n, k in ONWARD.items():
            f, h = ARR[n]
            ag_copy(t, buf, k, f, h, PN).wait_send()

    lx.wait()
    ld.wait()
    ag_start(0, xs)

    def zero(p, _):
        yacc[p] = jnp.zeros(yacc.shape[1:], F32)
        dxacc[p] = jnp.zeros(dxacc.shape[1:], F32)
        return 0

    lax.fori_loop(0, NP, zero, 0)

    for n, to in enumerate(peers):
        remote(rgs.at[blk(*to)], rgs.at[blk(*to)], rg_ss.at[n], rg_rs.at[n], to).wait_recv()
    top = rgs.shape[1] // 2
    tr = lax.broadcasted_iota(jnp.int32, (TOK, TOK), 0)
    tc = lax.broadcasted_iota(jnp.int32, (TOK, TOK), 1)
    tri = jnp.where(tr < tc, 1.0, 0.0).astype(BF16)
    ee = (lax.broadcasted_iota(jnp.int32, (el, TOK), 0) + e0).astype(F32)

    def prep(p, _):
        rg = rgs[p]
        m = jnp.zeros((el, TOK), F32)
        gs = jnp.zeros((el, TOK), F32)
        for j in range(top):
            hit = jnp.broadcast_to(rg[j:j + 1], (el, TOK)) == ee
            m = jnp.where(hit, 1.0, m)
            gs = jnp.where(hit, jnp.broadcast_to(rg[top + j:top + j + 1], (el, TOK)), gs)
        rank = nn(m.astype(BF16), tri)
        cm[p] = jnp.where(m > 0.0, rank, -1.0)
        gm[p] = gs
        return 0

    lax.fori_loop(0, NP, prep, 0)

    ag_relay(0, xs, (0, 1, 2, 3))
    ag_start(1, dys)
    ag_relay(0, xs, (4, 5))
    ag_finish(0, xs)
    out_copies = [pltpu.make_async_copy(xs, xa_hbm, osem.at[0]),
                  pltpu.make_async_copy(cm, cm_hbm, osem.at[1]),
                  pltpu.make_async_copy(gm, gm_hbm, osem.at[2]),
                  pltpu.make_async_copy(dys, dya_hbm, osem.at[3])]
    for c in out_copies[:3]:
        c.start()

    def gather_all(g, src):
        def step(q, _):
            def store(k, rows, val):
                xe_s[k, rows, :] = val
            gather_pair(cm, g, q, src, store)
            return 0
        lax.fori_loop(0, NP // 2, step, 0, unroll=4)

    def gather_dy(g):
        def step(q, _):
            def store(k, rows, val):
                xe_s[k, rows, :] = val

            def store_scaled(k, rows, val):
                do_s[k, rows, :] = val
            gather_dy_pair(cm, gm, g, q, dys, store, store_scaled)
            return 0
        lax.fori_loop(0, NP // 2, step, 0, unroll=4)

    def put_rows(i, val):
        zero = jnp.zeros((PAD - CAP, val.shape[1]), F32)
        for p in range(NP):
            o_s[i, p * PAD:(p + 1) * PAD, :] = jnp.concatenate([val[p * CAP:(p + 1) * CAP], zero], axis=0).astype(BF16)

    def take_rows(p):
        return jnp.concatenate([o_s[k, ds(p, PAD), :] for k in range(GRP)], axis=0)

    def combine_y(g):
        def step(p, _):
            oh = onehot(cm[p, ds(g, GRP), :], PAD)
            gr = gm[p, ds(g, GRP), :]
            g1 = gr.astype(BF16).astype(F32)
            rest = gr - g1
            g2 = rest.astype(BF16).astype(F32)
            g3 = rest - g2
            ob = take_rows(p)

            def spread(part):
                return jnp.concatenate(
                    [jnp.where(oh[k], jnp.broadcast_to(part[k:k + 1], (PAD, TOK)), 0.0) for k in range(GRP)],
                    axis=0).astype(BF16)

            gs = jnp.concatenate([spread(g1), spread(g2), spread(g3)], axis=0)
            yacc[p] += tn(gs, jnp.concatenate([ob, ob, ob], axis=0))
            return 0
        lax.fori_loop(0, NP, step, 0, unroll=4)

    def combine_dx(g):
        def step(p, _):
            oh = onehot(cm[p, ds(g, GRP), :], PAD)
            one = jnp.concatenate([jnp.where(m, 1.0, 0.0) for m in oh], axis=0).astype(BF16)
            dxacc[p] += tn(one, take_rows(p))
            rows = []
            for k in range(GRP):
                db = jnp.broadcast_to(dgc_s[k, ds(p, CAP), :], (CAP, TOK))
                rows.append(jnp.sum(jnp.where(oh[k][:CAP], db, 0.0), axis=0, keepdims=True))
            dgm[p, ds(g, GRP), :] = jnp.concatenate(rows, axis=0)
            return 0
        lax.fori_loop(0, NP, step, 0, unroll=4)

    def fetch(n):
        for k in range(PAIR):
            for c in wcopies(n + k):
                c.wait()

        @pl.when(n + 2 * PAIR < 2 * el)
        def _():
            for k in range(PAIR):
                for c in wcopies(n + 2 * PAIR + k):
                    c.start()

    def w13_of(n):
        b = lax.rem(n, NBUF)
        return jnp.concatenate([w1b[b], w3b[b]], axis=1)

    def w2_of(n):
        return w2b[lax.rem(n, NBUF)]

    def skewed(g, first, base, second):
        npair = GRP // PAIR
        fetch(base)
        first(0)

        def step(r, _):
            fetch(base + r * PAIR)
            second(r - 1)
            first(r)
            return 0

        lax.fori_loop(1, npair, step, 0)
        second(npair - 1)

    def act(uv):
        u, v = uv[:, :ff], uv[:, ff:]
        sg = jax.nn.sigmoid(u)
        return u, v, sg, (u * sg * v).astype(BF16)

    ORDER = [(1, 1), (0, 1), (1, 0), (0, 0)]
    S1 = [((1, 1), 0, XN), ((1, 1), 1, YN), ((0, 1), 0, XN), ((1, 0), 1, YN)]
    IN1 = [((1, 0), 0), ((0, 1), 1), ((0, 0), 0), ((0, 0), 1)]
    S2 = [YN, XN]

    def dd_copy(t, acc, n):
        fy, fx = ORDER[n]
        return remote(acc.at[blk(fy, fx, 1)], rd.at[n], dd_ss.at[t, n], dd_rs.at[t, n], PN)

    def s1_copy(t, acc, n):
        (fy, fx), h, to = S1[n]
        return remote(half(acc, blk(fy, fx, 0), h), r1.at[t, n], s1_ss.at[t, n], s1_rs.at[t, n], to)

    def s2_copy(t, acc, n):
        (fy, fx), h = IN1[n]
        return remote(half(acc, blk(fy, fx, 0), h), r2.at[t, n], s2_ss.at[t, n], s2_rs.at[t, n], S2[n])

    def rs_start(t, acc):
        for n in range(4):
            dd_copy(t, acc, n).start()

    def rs_mid1(t, acc):
        for n in range(4):
            dd_copy(t, acc, n).wait_recv()
            fy, fx = ORDER[n]
            acc[blk(fy, fx, 0)] += rd[n]
            for k in ((0, 1), (2,), (3,), ())[n]:
                s1_copy(t, acc, k).start()

    def rs_mid2(t, acc):
        for n in range(4):
            s1_copy(t, acc, n).wait_recv()
            (fy, fx), h = IN1[n]
            acc[blk(fy, fx, 0), h * HALF:(h + 1) * HALF, :] += r1[t, n]
            if n < 2:
                s2_copy(t, acc, n).start()

    def rs_fin(t, acc, out):
        for n in range(2):
            s2_copy(t, acc, n).wait_recv()
            rows = slice(n * HALF, (n + 1) * HALF)
            out[rows, :] = (acc[me, rows, :] + r2[t, n]).astype(BF16)

    def rs_drain(t, acc):
        for n in range(4):
            dd_copy(t, acc, n).wait_send()
            s1_copy(t, acc, n).wait_send()
        for n in range(2):
            s2_copy(t, acc, n).wait_send()

    def fwd_group(g, _):
        gather_all(g, xs)

        def f1(r):
            for k in range(PAIR):
                i = r * PAIR + k
                uv_s[g * GRP + i] = nn(xe_s[i], w13_of(g * GRP + i)).astype(BF16)

        def f2(r):
            uvs = [uv_s[g * GRP + r * PAIR + k].astype(F32) for k in range(PAIR)]
            for k in range(PAIR):
                i = r * PAIR + k
                put_rows(i, nn(act(uvs[k])[3], w2_of(g * GRP + i)))

        skewed(g, f1, g * GRP, f2)
        combine_y(g)

        @pl.when(g == 0)
        def _():
            ag_relay(1, dys, (0, 1, 2, 3))

        @pl.when(g == 1)
        def _():
            ag_relay(1, dys, (4, 5))

        @pl.when(g == 2)
        def _():
            ag_finish(1, dys)
            out_copies[3].start()
        return 0

    lax.fori_loop(0, ng, fwd_group, 0)

    def duv_copy(g):
        return pltpu.make_async_copy(uv_s.at[ds(g, GRP)], duv_hbm.at[ds(g, GRP)], osem.at[4])

    def a_copy(g):
        return pltpu.make_async_copy(a_s, a_hbm.at[ds(g, GRP)], osem.at[5])

    def bwd_group(g, _):
        gather_dy(g)

        @pl.when(g == 0)
        def _():
            rs_start(0, yacc)

        def b1(r):
            uvs = [uv_s[g * GRP + r * PAIR + k] for k in range(PAIR)]
            for k in range(PAIR):
                i = r * PAIR + k
                e = g * GRP + i
                w2 = w2_of(el + e)
                da = nt(do_s[i], w2)
                u, v, sg, a = act(uvs[k].astype(F32))
                a_s[i] = a
                of = nn(a, w2).astype(BF16).astype(F32)
                dgc_s[i] = jnp.sum(xe_s[i].astype(F32) * of, axis=1, keepdims=True)
                du = (da * v * sg * (1.0 + u * (1.0 - sg))).astype(BF16)
                dv = (da * u * sg).astype(BF16)
                uv_s[e] = jnp.concatenate([du, dv], axis=1)

        def b2(r):
            duvs = [uv_s[g * GRP + r * PAIR + k] for k in range(PAIR)]
            for k in range(PAIR):
                i = r * PAIR + k
                put_rows(i, nt(duvs[k], w13_of(el + g * GRP + i)))

        @pl.when(g > 0)
        def _():
            a_copy(g - 1).wait()
            duv_copy(g - 1).wait()

        skewed(g, b1, el + g * GRP, b2)
        a_copy(g).start()
        duv_copy(g).start()
        combine_dx(g)

        @pl.when(g == 1)
        def _():
            rs_mid1(0, yacc)
            pl.semaphore_signal(credit, inc=1, device_id=dev(*PN), device_id_type=MESH)

        @pl.when(g == ng - 1)
        def _():
            rs_mid2(0, yacc)
        return 0

    lax.fori_loop(0, ng, bwd_group, 0)

    def spread_dg(p, _):
        rg = rgs[p]
        acc = jnp.zeros((top, TOK), F32)
        for e in range(el):
            ef = (e0 + e).astype(F32)
            acc = acc + jnp.where(rg[:top] == ef, jnp.broadcast_to(dgm[p, e:e + 1, :], (top, TOK)), 0.0)
        dgo[p] = acc
        return 0

    lax.fori_loop(0, NP, spread_dg, 0)
    pl.semaphore_wait(credit, 1)
    rs_start(1, dxacc)
    rs_fin(0, yacc, y_ref)
    dg_copies = [remote(dgo.at[blk(*to)], dgr.at[n], dg_ss.at[n], dg_rs.at[n], to) for n, to in enumerate(peers)]
    for c in dg_copies:
        c.start()
    part_copies = []
    for n in range(4):
        dd_copy(1, dxacc, n).wait_recv()
        fy, fx = ORDER[n]
        b = blk(fy, fx, 0)
        dxacc[b] += rd[n]
        to_b = (sy_hbm.at[0], kb_hbm.at[0], sy_hbm.at[1], kb_hbm.at[1])[n]
        to_a = (sx_hbm.at[0], sx_hbm.at[1], ka_hbm.at[0], ka_hbm.at[1])[n]
        for h, to in enumerate((to_a, to_b)):
            c = pltpu.make_async_copy(half(dxacc, b, h), to, psem.at[n, h])
            c.start()
            part_copies.append(c)
    total = dgo[me]
    for n, c in enumerate(dg_copies):
        c.wait_recv()
        total = total + dgr[n]
    dg_ref[...] = total

    ag_drain(0, xs)
    ag_drain(1, dys)
    rs_drain(0, yacc)
    for n in range(4):
        dd_copy(1, dxacc, n).wait_send()
    for c in part_copies:
        c.wait()
    for c in rg_copies + dg_copies:
        c.wait_send()
    for c in out_copies:
        c.wait()
    a_copy(ng - 1).wait()
    duv_copy(ng - 1).wait()


def grad_kernel(first, count, eb, nprev, xa_hbm, dya_hbm, cm, gm, a_ref, duv_ref, *refs):
    gw1_ref, gw3_ref, gw2_ref, xs, dys, xe_s, dye_s, sem = refs[nprev:]
    s = pl.program_id(0)
    per = GRP // eb
    ff = a_ref.shape[2]

    @pl.when(s == 0)
    def _():
        cx = pltpu.make_async_copy(xa_hbm, xs, sem.at[0])
        cd = pltpu.make_async_copy(dya_hbm, dys, sem.at[1])
        cx.start()
        cd.start()
        cx.wait()
        cd.wait()

    @pl.when(s < count // eb)
    def _():
        g = lax.div(s, per)
        slot = lax.rem(g, 2)
        for k in range(NP // 2 // per):
            q = lax.rem(s, per) * (NP // 2 // per) + k
            for src, dst in ((xs, xe_s), (dys, dye_s)):
                def store(j, rows, val):
                    dst[slot, j, rows, :] = val
                gather_pair(cm, first // GRP + g, q, src, store)

    @pl.when(s >= per)
    def _():
        t = s - per
        g = lax.div(t, per)
        slot = lax.rem(g, 2)
        for k in range(eb):
            i = lax.rem(t, per) * eb + k
            e = first + g * GRP + i
            do = (gate_column(cm, gm, e) * dye_s[slot, i].astype(F32)).astype(BF16)
            gw2_ref[k] = tn(a_ref[k], do)
            g13 = tn(xe_s[slot, i], duv_ref[k])
            gw1_ref[k] = g13[:, :ff]
            gw3_ref[k] = g13[:, ff:]


def solution(mesh):
    grp = ('row', 'col')
    tspec = P(('dp', 'row', 'col'), None)
    wspec = P(grp, None, None)
    gspec = P(('dp', 'row', 'col'), None, None)

    def local(x, ridx, gates, w1, w3, w2, dy):
        tok, d = x.shape
        top = ridx.shape[1]
        el, _, ff = w1.shape
        anyspec = pl.BlockSpec(memory_space=pl.ANY)
        vm = pl.BlockSpec(memory_space=pltpu.VMEM)
        sds = jax.ShapeDtypeStruct
        rg = jnp.concatenate([ridx.T.astype(F32), gates.T], axis=0)
        dma = pltpu.SemaphoreType.DMA
        y, dg, sx, sy, ka, kb, xa, dya, cm, gm, duv, a = pl.pallas_call(
            functools.partial(main_kernel, el),
            in_specs=[anyspec, anyspec, vm, anyspec, anyspec, anyspec],
            out_specs=[vm, vm] + [anyspec] * 10,
            out_shape=[
                sds((tok, d), BF16), sds((top, tok), F32)] + [sds((2, tok // 2, d), F32)] * 4 + [
                sds((NP, tok, d), BF16), sds((NP, tok, d), BF16),
                sds((NP, el, tok), F32), sds((NP, el, tok), F32),
                sds((el, NROW, 2 * ff), BF16), sds((el, NROW, ff), BF16),
            ],
            scratch_shapes=[
                pltpu.VMEM((NP, tok, d), BF16),
                pltpu.VMEM((NP, tok, d), BF16),
                pltpu.VMEM((NP, 2 * top, tok), F32),
                pltpu.VMEM((GRP, NROW, d), BF16),
                pltpu.VMEM((GRP, NROW, d), BF16),
                pltpu.VMEM((GRP, NROW, 1), F32),
                pltpu.VMEM((GRP, NP * PAD, d), BF16),
                pltpu.VMEM((el, NROW, 2 * ff), BF16),
                pltpu.VMEM((GRP, NROW, ff), BF16),
                pltpu.VMEM((NP, tok, d), F32),
                pltpu.VMEM((NP, tok, d), F32),
                pltpu.VMEM((NP, el, tok), F32),
                pltpu.VMEM((NP, el, tok), F32),
                pltpu.VMEM((NP, el, tok), F32),
                pltpu.VMEM((NP, top, tok), F32),
                pltpu.VMEM((NP - 1, top, tok), F32),
                pltpu.VMEM((NBUF, d, ff), BF16),
                pltpu.VMEM((NBUF, d, ff), BF16),
                pltpu.VMEM((NBUF, ff, d), BF16),
                pltpu.VMEM((4, tok, d), F32),
                pltpu.VMEM((1, 4, tok // 2, d), F32),
                pltpu.VMEM((1, 2, tok // 2, d), F32),
                dma((3, NBUF)), dma((2,)), dma((6,)), dma((4, 2)), pltpu.SemaphoreType.REGULAR,
                dma((NP - 1,)), dma((NP - 1,)),
                dma((2, 14)), dma((2, 14)),
                dma((2, 4)), dma((2, 4)),
                dma((1, 4)), dma((1, 4)),
                dma((1, 2)), dma((1, 2)),
                dma((NP - 1,)), dma((NP - 1,)),
            ],
            compiler_params=pltpu.CompilerParams(
                collective_id=0, has_side_effects=True, vmem_limit_bytes=67_000_000),
            cost_estimate=pl.CostEstimate(flops=40_000_000_000, bytes_accessed=160_000_000, transcendentals=0),
        )(x, dy, rg, w1, w3, w2)

        def perm(fy, fx):
            out = []
            for p in range(NP):
                yy, xx, cc = p // 4, (p // 2) % 2, p % 2
                out.append((p, (yy ^ fy) * 4 + (xx ^ fx) * 2 + cc))
            return out

        eb = 2
        per = GRP // eb

        def grads(first, count, prev):
            steps = count // eb + per

            def eidx(s):
                return (first // eb + jnp.clip(s - per, 0, count // eb - 1), 0, 0)

            return pl.pallas_call(
                functools.partial(grad_kernel, first, count, eb, len(prev)),
                grid=(steps,),
                in_specs=[anyspec, anyspec, vm, vm, pl.BlockSpec((eb, NROW, ff), eidx), pl.BlockSpec((eb, NROW, 2 * ff), eidx)] + [anyspec] * len(prev),
                out_specs=[pl.BlockSpec((eb, d, ff), eidx), pl.BlockSpec((eb, d, ff), eidx), pl.BlockSpec((eb, ff, d), eidx)],
                out_shape=[sds((el, d, ff), F32), sds((el, d, ff), F32), sds((el, ff, d), F32)],
                input_output_aliases={6 + k: k for k in range(len(prev))},
                scratch_shapes=[
                    pltpu.VMEM((NP, tok, d), BF16),
                    pltpu.VMEM((NP, tok, d), BF16),
                    pltpu.VMEM((2, GRP, NROW, d), BF16),
                    pltpu.VMEM((2, GRP, NROW, d), BF16),
                    pltpu.SemaphoreType.DMA((2,)),
                ],
                compiler_params=pltpu.CompilerParams(
                    dimension_semantics=('arbitrary',), vmem_limit_bytes=60_000_000),
                cost_estimate=pl.CostEstimate(flops=20_000_000_000 * count // el, bytes_accessed=150_000_000 * count // el, transcendentals=0),
            )(xa, dya, cm, gm, a, duv, *prev)

        r1x = lax.ppermute(sx, grp, perm(0, 1))
        r1y = lax.ppermute(sy, grp, perm(1, 0))
        prev = grads(0, SPLIT, ())
        prev, r1x, r1y = lax.optimization_barrier((prev, r1x, r1y))
        r2a = lax.ppermute(ka[0] + r1x[0], grp, perm(1, 0))
        r2b = lax.ppermute(kb[0] + r1y[0], grp, perm(0, 1))
        gw1, gw3, gw2 = grads(SPLIT, el - SPLIT, tuple(prev))
        dx = jnp.concatenate([ka[1] + r1x[1] + r2a, kb[1] + r1y[1] + r2b], axis=0).astype(BF16)
        return y, dx, dg.T, gw1, gw3, gw2

    return jax.shard_map(local, mesh=mesh, in_specs=(tspec, tspec, tspec, wspec, wspec, wspec, tspec), out_specs=(tspec, tspec, tspec, gspec, gspec, gspec), check_vma=False)
```

```python
import functools

import jax
import jax.numpy as jnp
from jax import lax
from jax.experimental import pallas as pl
from jax.experimental.pallas import tpu as pltpu
from jax.sharding import PartitionSpec as P

F32 = jnp.float32
BF16 = jnp.bfloat16
MESH = pl.DeviceIdType.MESH
NP = 8
TOK = 256
HALF = TOK // 2
CAP = 24
PAD = 32
GRP = 8
NROW = NP * CAP
NBUF = 8
PAIR = 2
SPLIT = 24


def nt(a, b):
    return lax.dot_general(a, b, (((1,), (1,)), ((), ())), preferred_element_type=F32)


def nn(a, b):
    return lax.dot_general(a, b, (((1,), (0,)), ((), ())), preferred_element_type=F32)


def tn(a, b):
    return lax.dot_general(a, b, (((0,), (0,)), ((), ())), preferred_element_type=F32)


def onehot(rows, cap):
    n = rows.shape[0]
    it = lax.broadcasted_iota(jnp.int32, (cap, TOK), 0).astype(F32)
    return [jnp.broadcast_to(rows[k:k + 1], (cap, TOK)) == it for k in range(n)]


def ds(i, n):
    return pl.ds(pl.multiple_of(i * n, n), n)


def gather_pair(cm, g, q, src, store):
    res = []
    for h in range(2):
        p = q * 2 + h
        oh = onehot(cm[p, ds(g, GRP), :], CAP)
        oh = jnp.concatenate([jnp.where(m, 1.0, 0.0) for m in oh], axis=0).astype(BF16)
        res.append(nn(oh, src[p]))
    for k in range(GRP):
        blk = jnp.concatenate([r[k * CAP:(k + 1) * CAP] for r in res], axis=0)
        store(k, ds(q, 2 * CAP), blk.astype(BF16))


def gather_dy_pair(cm, gm, g, q, src, store, store_scaled):
    res, scaled = [], []
    for h in range(2):
        p = q * 2 + h
        oh = onehot(cm[p, ds(g, GRP), :], CAP)
        gr = gm[p, ds(g, GRP), :]
        col = jnp.concatenate(
            [jnp.sum(jnp.where(m, jnp.broadcast_to(gr[k:k + 1], (CAP, TOK)), 0.0), axis=1, keepdims=True)
             for k, m in enumerate(oh)], axis=0)
        oh = jnp.concatenate([jnp.where(m, 1.0, 0.0) for m in oh], axis=0).astype(BF16)
        r = nn(oh, src[p])
        res.append(r)
        scaled.append(col * r)
    for parts, put in ((res, store), (scaled, store_scaled)):
        if put is None:
            continue
        for k in range(GRP):
            blk = jnp.concatenate([r[k * CAP:(k + 1) * CAP] for r in parts], axis=0)
            put(k, ds(q, 2 * CAP), blk.astype(BF16))


def main_kernel(el, x_hbm, dy_hbm, rg_ref, w1_hbm, w3_hbm, w2_hbm,
                y_ref, dg_ref, sx_hbm, sy_hbm, ka_hbm, kb_hbm, xa_hbm, dya_hbm, cm_hbm, gm_hbm, duv_hbm, a_hbm, xef_hbm, dof_hbm,
                xs, dys, rgs, xe_s, do_s, dgc_s, o_s, uv_s, a_s, yacc, dxacc, cm, gm, dgm, dgo, dgr,
                w1b, w3b, w2b, rd, r1, r2,
                wsem, lsem, osem, psem, credit, rg_ss, rg_rs, ag_ss, ag_rs, dd_ss, dd_rs, s1_ss, s1_rs, s2_ss, s2_rs, dg_ss, dg_rs):
    ng = el // GRP
    ff = w2b.shape[1]
    Z = lax.axis_index('dp')
    Y = lax.axis_index('row')
    col = lax.axis_index('col')
    X = lax.div(col, 2)
    C = lax.rem(col, 2)
    me = Y * 4 + col
    e0 = me * el

    def pos(fy, fx, fc):
        return (1 - Y if fy else Y), (1 - X if fx else X), (1 - C if fc else C)

    def blk(fy, fx, fc):
        yy, xx, cc = pos(fy, fx, fc)
        return yy * 4 + xx * 2 + cc

    def dev(fy, fx, fc):
        yy, xx, cc = pos(fy, fx, fc)
        return (Z, yy, xx * 2 + cc)

    peers = [(a, b, c) for a in range(2) for b in range(2) for c in range(2)][1:]

    def remote(src, dst, ss, rs, to):
        return pltpu.make_async_remote_copy(src_ref=src, dst_ref=dst, send_sem=ss, recv_sem=rs,
                                            device_id=dev(*to), device_id_type=MESH)

    lx = pltpu.make_async_copy(x_hbm, xs.at[me], lsem.at[0])
    ld = pltpu.make_async_copy(dy_hbm, dys.at[me], lsem.at[1])
    lx.start()
    ld.start()

    def wcopies(e):
        b = lax.rem(e, NBUF)
        k = lax.rem(e, el)
        return [pltpu.make_async_copy(h.at[k], v.at[b], wsem.at[n, b])
                for n, (h, v) in enumerate(((w1_hbm, w1b), (w3_hbm, w3b), (w2_hbm, w2b)))]

    for e in range(2 * PAIR):
        for c in wcopies(e):
            c.start()

    barrier = pltpu.get_barrier_semaphore()
    for to in peers:
        pl.semaphore_signal(barrier, inc=1, device_id=dev(*to), device_id_type=MESH)
    pl.semaphore_wait(barrier, len(peers))

    rgs[me] = rg_ref[...]
    rg_copies = [remote(rg_ref, rgs.at[me], rg_ss.at[n], rg_rs.at[n], to) for n, to in enumerate(peers)]
    for c in rg_copies:
        c.start()

    def half(buf, b, h):
        return buf.at[b, pl.ds(h * HALF, HALF), :]

    XN, YN, DN, PN = (0, 1, 0), (1, 0, 0), (1, 1, 0), (0, 0, 1)
    FIRST = [(0, (0, 0, 0), 0, XN), (1, (0, 0, 0), 1, YN), (2, (0, 0, 0), 1, XN), (3, (0, 0, 0), 0, YN)]
    OWN2 = [(6, (0, 0, 0), 0, PN), (7, (0, 0, 0), 1, PN)]
    FWD = [(4, XN, 0, YN), (5, YN, 1, XN)]
    ARR = {0: (XN, 0), 1: (YN, 1), 2: (XN, 1), 3: (YN, 0), 4: (DN, 0), 5: (DN, 1)}
    ONWARD = {0: 8, 1: 9, 2: 10, 3: 11, 4: 12, 5: 13}

    def ag_copy(t, buf, n, f, h, to):
        r = half(buf, blk(*f), h)
        return remote(r, r, ag_ss.at[t, n], ag_rs.at[t, n], to)

    def ag_recv(t, buf, n, f, h):
        r = half(buf, blk(*f), h)
        remote(r, r, ag_ss.at[t, n], ag_rs.at[t, n], PN).wait_recv()

    def ag_start(t, buf):
        for n, f, h, to in FIRST + OWN2:
            ag_copy(t, buf, n, f, h, to).start()

    def ag_relay(t, buf, ns):
        for n in ns:
            f, h = ARR[n]
            ag_recv(t, buf, n, f, h)
            if n < 2:
                k, ff_, hh, to = FWD[n]
                ag_copy(t, buf, k, ff_, hh, to).start()
            ag_copy(t, buf, ONWARD[n], f, h, PN).start()

    def ag_finish(t, buf):
        for n, h in ((6, 0), (7, 1)):
            ag_recv(t, buf, n, PN, h)
        for n, k in ONWARD.items():
            f, h = ARR[n]
            ag_recv(t, buf, k, (f[0], f[1], 1), h)

    def ag_drain(t, buf):
        for n, f, h, to in FIRST + OWN2 + FWD:
            ag_copy(t, buf, n, f, h, to).wait_send()
        for n, k in ONWARD.items():
            f, h = ARR[n]
            ag_copy(t, buf, k, f, h, PN).wait_send()

    lx.wait()
    ld.wait()
    ag_start(0, xs)

    def zero(p, _):
        yacc[p] = jnp.zeros(yacc.shape[1:], F32)
        dxacc[p] = jnp.zeros(dxacc.shape[1:], F32)
        return 0

    lax.fori_loop(0, NP, zero, 0)

    for n, to in enumerate(peers):
        remote(rgs.at[blk(*to)], rgs.at[blk(*to)], rg_ss.at[n], rg_rs.at[n], to).wait_recv()
    top = rgs.shape[1] // 2
    tr = lax.broadcasted_iota(jnp.int32, (TOK, TOK), 0)
    tc = lax.broadcasted_iota(jnp.int32, (TOK, TOK), 1)
    tri = jnp.where(tr < tc, 1.0, 0.0).astype(BF16)
    ee = (lax.broadcasted_iota(jnp.int32, (el, TOK), 0) + e0).astype(F32)

    def prep(p, _):
        rg = rgs[p]
        m = jnp.zeros((el, TOK), F32)
        gs = jnp.zeros((el, TOK), F32)
        for j in range(top):
            hit = jnp.broadcast_to(rg[j:j + 1], (el, TOK)) == ee
            m = jnp.where(hit, 1.0, m)
            gs = jnp.where(hit, jnp.broadcast_to(rg[top + j:top + j + 1], (el, TOK)), gs)
        rank = nn(m.astype(BF16), tri)
        cm[p] = jnp.where(m > 0.0, rank, -1.0)
        gm[p] = gs
        return 0

    lax.fori_loop(0, NP, prep, 0)

    ag_relay(0, xs, (0, 1, 2, 3))
    ag_start(1, dys)
    ag_relay(0, xs, (4, 5))
    ag_finish(0, xs)
    out_copies = [pltpu.make_async_copy(xs, xa_hbm, osem.at[0]),
                  pltpu.make_async_copy(cm, cm_hbm, osem.at[1]),
                  pltpu.make_async_copy(gm, gm_hbm, osem.at[2]),
                  pltpu.make_async_copy(dys, dya_hbm, osem.at[3])]
    for c in out_copies[:3]:
        c.start()

    def gather_all(g, src):
        def step(q, _):
            def store(k, rows, val):
                xe_s[k, rows, :] = val
            gather_pair(cm, g, q, src, store)
            return 0
        lax.fori_loop(0, NP // 2, step, 0, unroll=4)

    def gather_dy(g):
        def step(q, _):
            def store(k, rows, val):
                xe_s[k, rows, :] = val

            def store_scaled(k, rows, val):
                do_s[k, rows, :] = val
            gather_dy_pair(cm, gm, g, q, dys, store, store_scaled)
            return 0
        lax.fori_loop(0, NP // 2, step, 0, unroll=4)

    def put_rows(i, val):
        zero = jnp.zeros((PAD - CAP, val.shape[1]), F32)
        for p in range(NP):
            o_s[i, p * PAD:(p + 1) * PAD, :] = jnp.concatenate([val[p * CAP:(p + 1) * CAP], zero], axis=0).astype(BF16)

    def take_rows(p):
        return jnp.concatenate([o_s[k, ds(p, PAD), :] for k in range(GRP)], axis=0)

    def combine_y(g):
        def step(p, _):
            oh = onehot(cm[p, ds(g, GRP), :], PAD)
            gr = gm[p, ds(g, GRP), :]
            g1 = gr.astype(BF16).astype(F32)
            rest = gr - g1
            g2 = rest.astype(BF16).astype(F32)
            g3 = rest - g2
            ob = take_rows(p)

            def spread(part):
                return jnp.concatenate(
                    [jnp.where(oh[k], jnp.broadcast_to(part[k:k + 1], (PAD, TOK)), 0.0) for k in range(GRP)],
                    axis=0).astype(BF16)

            gs = jnp.concatenate([spread(g1), spread(g2), spread(g3)], axis=0)
            yacc[p] += tn(gs, jnp.concatenate([ob, ob, ob], axis=0))
            return 0
        lax.fori_loop(0, NP, step, 0, unroll=4)

    def combine_dx(g):
        def step(p, _):
            oh = onehot(cm[p, ds(g, GRP), :], PAD)
            one = jnp.concatenate([jnp.where(m, 1.0, 0.0) for m in oh], axis=0).astype(BF16)
            dxacc[p] += tn(one, take_rows(p))
            rows = []
            for k in range(GRP):
                db = jnp.broadcast_to(dgc_s[k, ds(p, CAP), :], (CAP, TOK))
                rows.append(jnp.sum(jnp.where(oh[k][:CAP], db, 0.0), axis=0, keepdims=True))
            dgm[p, ds(g, GRP), :] = jnp.concatenate(rows, axis=0)
            return 0
        lax.fori_loop(0, NP, step, 0, unroll=4)

    def fetch(n):
        for k in range(PAIR):
            for c in wcopies(n + k):
                c.wait()

        @pl.when(n + 2 * PAIR < 2 * el)
        def _():
            for k in range(PAIR):
                for c in wcopies(n + 2 * PAIR + k):
                    c.start()

    def w13_of(n):
        b = lax.rem(n, NBUF)
        return jnp.concatenate([w1b[b], w3b[b]], axis=1)

    def w2_of(n):
        return w2b[lax.rem(n, NBUF)]

    def skewed(g, first, base, second):
        npair = GRP // PAIR
        fetch(base)
        first(0)

        def step(r, _):
            fetch(base + r * PAIR)
            second(r - 1)
            first(r)
            return 0

        lax.fori_loop(1, npair, step, 0)
        second(npair - 1)

    def act(uv):
        u, v = uv[:, :ff], uv[:, ff:]
        sg = jax.nn.sigmoid(u)
        return u, v, sg, (u * sg * v).astype(BF16)

    ORDER = [(1, 1), (0, 1), (1, 0), (0, 0)]
    S1 = [((1, 1), 0, XN), ((1, 1), 1, YN), ((0, 1), 0, XN), ((1, 0), 1, YN)]
    IN1 = [((1, 0), 0), ((0, 1), 1), ((0, 0), 0), ((0, 0), 1)]
    S2 = [YN, XN]

    def dd_copy(t, acc, n):
        fy, fx = ORDER[n]
        return remote(acc.at[blk(fy, fx, 1)], rd.at[n], dd_ss.at[t, n], dd_rs.at[t, n], PN)

    def s1_copy(t, acc, n):
        (fy, fx), h, to = S1[n]
        return remote(half(acc, blk(fy, fx, 0), h), r1.at[t, n], s1_ss.at[t, n], s1_rs.at[t, n], to)

    def s2_copy(t, acc, n):
        (fy, fx), h = IN1[n]
        return remote(half(acc, blk(fy, fx, 0), h), r2.at[t, n], s2_ss.at[t, n], s2_rs.at[t, n], S2[n])

    def rs_start(t, acc):
        for n in range(4):
            dd_copy(t, acc, n).start()

    def rs_mid1(t, acc):
        for n in range(4):
            dd_copy(t, acc, n).wait_recv()
            fy, fx = ORDER[n]
            acc[blk(fy, fx, 0)] += rd[n]
            for k in ((0, 1), (2,), (3,), ())[n]:
                s1_copy(t, acc, k).start()

    def rs_mid2(t, acc):
        for n in range(4):
            s1_copy(t, acc, n).wait_recv()
            (fy, fx), h = IN1[n]
            acc[blk(fy, fx, 0), h * HALF:(h + 1) * HALF, :] += r1[t, n]
            if n < 2:
                s2_copy(t, acc, n).start()

    def rs_fin(t, acc, out):
        for n in range(2):
            s2_copy(t, acc, n).wait_recv()
            rows = slice(n * HALF, (n + 1) * HALF)
            out[rows, :] = (acc[me, rows, :] + r2[t, n]).astype(BF16)

    def rs_drain(t, acc):
        for n in range(4):
            dd_copy(t, acc, n).wait_send()
            s1_copy(t, acc, n).wait_send()
        for n in range(2):
            s2_copy(t, acc, n).wait_send()

    gs = SPLIT // GRP

    def xef_copy(g):
        return pltpu.make_async_copy(xe_s, xef_hbm.at[lax.div(g, gs)], osem.at[6])

    def dof_copy(g):
        return pltpu.make_async_copy(do_s, dof_hbm.at[lax.div(g, gs)], osem.at[7])

    def fwd_group(g, _):
        gather_all(g, xs)

        @pl.when(lax.rem(g, gs) == 0)
        def _():
            xef_copy(g).start()

        def f1(r):
            for k in range(PAIR):
                i = r * PAIR + k
                uv_s[g * GRP + i] = nn(xe_s[i], w13_of(g * GRP + i)).astype(BF16)

        def f2(r):
            uvs = [uv_s[g * GRP + r * PAIR + k].astype(F32) for k in range(PAIR)]
            for k in range(PAIR):
                i = r * PAIR + k
                put_rows(i, nn(act(uvs[k])[3], w2_of(g * GRP + i)))

        skewed(g, f1, g * GRP, f2)
        combine_y(g)

        @pl.when(lax.rem(g, gs) == 0)
        def _():
            xef_copy(g).wait()

        @pl.when(g == 0)
        def _():
            ag_relay(1, dys, (0, 1, 2, 3))

        @pl.when(g == 1)
        def _():
            ag_relay(1, dys, (4, 5))

        @pl.when(g == 2)
        def _():
            ag_finish(1, dys)
            out_copies[3].start()
        return 0

    lax.fori_loop(0, ng, fwd_group, 0)

    def duv_copy(g):
        return pltpu.make_async_copy(uv_s.at[ds(g, GRP)], duv_hbm.at[ds(g, GRP)], osem.at[4])

    def a_copy(g):
        return pltpu.make_async_copy(a_s, a_hbm.at[ds(g, GRP)], osem.at[5])

    def bwd_group(g, _):
        gather_dy(g)

        @pl.when(lax.rem(g, gs) == 0)
        def _():
            dof_copy(g).start()

        @pl.when(g == 0)
        def _():
            rs_start(0, yacc)

        def b1(r):
            uvs = [uv_s[g * GRP + r * PAIR + k] for k in range(PAIR)]
            for k in range(PAIR):
                i = r * PAIR + k
                e = g * GRP + i
                w2 = w2_of(el + e)
                da = nt(do_s[i], w2)
                u, v, sg, a = act(uvs[k].astype(F32))
                a_s[i] = a
                of = nn(a, w2).astype(BF16).astype(F32)
                dgc_s[i] = jnp.sum(xe_s[i].astype(F32) * of, axis=1, keepdims=True)
                du = (da * v * sg * (1.0 + u * (1.0 - sg))).astype(BF16)
                dv = (da * u * sg).astype(BF16)
                uv_s[e] = jnp.concatenate([du, dv], axis=1)

        def b2(r):
            duvs = [uv_s[g * GRP + r * PAIR + k] for k in range(PAIR)]
            for k in range(PAIR):
                i = r * PAIR + k
                put_rows(i, nt(duvs[k], w13_of(el + g * GRP + i)))

        @pl.when(g > 0)
        def _():
            a_copy(g - 1).wait()
            duv_copy(g - 1).wait()

        skewed(g, b1, el + g * GRP, b2)
        a_copy(g).start()
        duv_copy(g).start()
        combine_dx(g)

        @pl.when(lax.rem(g, gs) == 0)
        def _():
            dof_copy(g).wait()

        @pl.when(g == 1)
        def _():
            rs_mid1(0, yacc)
            pl.semaphore_signal(credit, inc=1, device_id=dev(*PN), device_id_type=MESH)

        @pl.when(g == ng - 1)
        def _():
            rs_mid2(0, yacc)
        return 0

    lax.fori_loop(0, ng, bwd_group, 0)

    def spread_dg(p, _):
        rg = rgs[p]
        acc = jnp.zeros((top, TOK), F32)
        for e in range(el):
            ef = (e0 + e).astype(F32)
            acc = acc + jnp.where(rg[:top] == ef, jnp.broadcast_to(dgm[p, e:e + 1, :], (top, TOK)), 0.0)
        dgo[p] = acc
        return 0

    lax.fori_loop(0, NP, spread_dg, 0)
    pl.semaphore_wait(credit, 1)
    rs_start(1, dxacc)
    rs_fin(0, yacc, y_ref)
    dg_copies = [remote(dgo.at[blk(*to)], dgr.at[n], dg_ss.at[n], dg_rs.at[n], to) for n, to in enumerate(peers)]
    for c in dg_copies:
        c.start()
    part_copies = []
    for n in range(4):
        dd_copy(1, dxacc, n).wait_recv()
        fy, fx = ORDER[n]
        b = blk(fy, fx, 0)
        dxacc[b] += rd[n]
        to_b = (sy_hbm.at[0], kb_hbm.at[0], sy_hbm.at[1], kb_hbm.at[1])[n]
        to_a = (sx_hbm.at[0], sx_hbm.at[1], ka_hbm.at[0], ka_hbm.at[1])[n]
        for h, to in enumerate((to_a, to_b)):
            c = pltpu.make_async_copy(half(dxacc, b, h), to, psem.at[n, h])
            c.start()
            part_copies.append(c)
    total = dgo[me]
    for n, c in enumerate(dg_copies):
        c.wait_recv()
        total = total + dgr[n]
    dg_ref[...] = total

    ag_drain(0, xs)
    ag_drain(1, dys)
    rs_drain(0, yacc)
    for n in range(4):
        dd_copy(1, dxacc, n).wait_send()
    for c in part_copies:
        c.wait()
    for c in rg_copies + dg_copies:
        c.wait_send()
    for c in out_copies:
        c.wait()
    a_copy(ng - 1).wait()
    duv_copy(ng - 1).wait()


def grad_kernel(first, count, eb, nprev, xa_hbm, dya_hbm, cm, gm, a_ref, duv_ref, xef_ref, dof_ref, *refs):
    gw1_ref, gw3_ref, gw2_ref, xs, dys, xe_s, do_s, sem = refs[nprev:]
    s = pl.program_id(0)
    per = GRP // eb
    ff = a_ref.shape[2]
    g = lax.div(s, per)
    i = lax.rem(s, per)
    loads = [pltpu.make_async_copy(xa_hbm, xs, sem.at[0]), pltpu.make_async_copy(dya_hbm, dys, sem.at[1])]

    @pl.when(s == 0)
    def _():
        for c in loads:
            c.start()

    @pl.when(s == 1)
    def _():
        for c in loads:
            c.wait()

    def gather(q):
        n = g + 1
        slot = lax.rem(n, 2)

        def store(j, rows, val):
            xe_s[slot, j, rows, :] = val

        def store_scaled(j, rows, val):
            do_s[slot, j, rows, :] = val
        gather_pair(cm, first // GRP + n, q, xs, store)
        gather_dy_pair(cm, gm, first // GRP + n, q, dys, None, store_scaled)

    more = g + 1 < count // GRP

    @pl.when(jnp.logical_and(more, i == 1))
    def _():
        gather(0)

    @pl.when(jnp.logical_and(more, i >= 1))
    def _():
        gather(i)

    def core(xe, do):
        for k in range(eb):
            g13 = tn(xe[k], duv_ref[k])
            gw1_ref[k] = g13[:, :ff]
            gw3_ref[k] = g13[:, ff:]
            gw2_ref[k] = tn(a_ref[k], do[k])

    @pl.when(g == 0)
    def _():
        core([xef_ref[0, k] for k in range(eb)], [dof_ref[0, k] for k in range(eb)])

    @pl.when(g > 0)
    def _():
        slot = lax.rem(g, 2)
        core([xe_s[slot, i * eb + k] for k in range(eb)], [do_s[slot, i * eb + k] for k in range(eb)])


def solution(mesh):
    grp = ('row', 'col')
    tspec = P(('dp', 'row', 'col'), None)
    wspec = P(grp, None, None)
    gspec = P(('dp', 'row', 'col'), None, None)

    def local(x, ridx, gates, w1, w3, w2, dy):
        tok, d = x.shape
        top = ridx.shape[1]
        el, _, ff = w1.shape
        anyspec = pl.BlockSpec(memory_space=pl.ANY)
        vm = pl.BlockSpec(memory_space=pltpu.VMEM)
        sds = jax.ShapeDtypeStruct
        rg = jnp.concatenate([ridx.T.astype(F32), gates.T], axis=0)
        dma = pltpu.SemaphoreType.DMA
        y, dg, sx, sy, ka, kb, xa, dya, cm, gm, duv, a, xef, dof = pl.pallas_call(
            functools.partial(main_kernel, el),
            in_specs=[anyspec, anyspec, vm, anyspec, anyspec, anyspec],
            out_specs=[vm, vm] + [anyspec] * 12,
            out_shape=[
                sds((tok, d), BF16), sds((top, tok), F32)] + [sds((2, tok // 2, d), F32)] * 4 + [
                sds((NP, tok, d), BF16), sds((NP, tok, d), BF16),
                sds((NP, el, tok), F32), sds((NP, el, tok), F32),
                sds((el, NROW, 2 * ff), BF16), sds((el, NROW, ff), BF16),
                sds((el // SPLIT, GRP, NROW, d), BF16), sds((el // SPLIT, GRP, NROW, d), BF16),
            ],
            scratch_shapes=[
                pltpu.VMEM((NP, tok, d), BF16),
                pltpu.VMEM((NP, tok, d), BF16),
                pltpu.VMEM((NP, 2 * top, tok), F32),
                pltpu.VMEM((GRP, NROW, d), BF16),
                pltpu.VMEM((GRP, NROW, d), BF16),
                pltpu.VMEM((GRP, NROW, 1), F32),
                pltpu.VMEM((GRP, NP * PAD, d), BF16),
                pltpu.VMEM((el, NROW, 2 * ff), BF16),
                pltpu.VMEM((GRP, NROW, ff), BF16),
                pltpu.VMEM((NP, tok, d), F32),
                pltpu.VMEM((NP, tok, d), F32),
                pltpu.VMEM((NP, el, tok), F32),
                pltpu.VMEM((NP, el, tok), F32),
                pltpu.VMEM((NP, el, tok), F32),
                pltpu.VMEM((NP, top, tok), F32),
                pltpu.VMEM((NP - 1, top, tok), F32),
                pltpu.VMEM((NBUF, d, ff), BF16),
                pltpu.VMEM((NBUF, d, ff), BF16),
                pltpu.VMEM((NBUF, ff, d), BF16),
                pltpu.VMEM((4, tok, d), F32),
                pltpu.VMEM((1, 4, tok // 2, d), F32),
                pltpu.VMEM((1, 2, tok // 2, d), F32),
                dma((3, NBUF)), dma((2,)), dma((8,)), dma((4, 2)), pltpu.SemaphoreType.REGULAR,
                dma((NP - 1,)), dma((NP - 1,)),
                dma((2, 14)), dma((2, 14)),
                dma((2, 4)), dma((2, 4)),
                dma((1, 4)), dma((1, 4)),
                dma((1, 2)), dma((1, 2)),
                dma((NP - 1,)), dma((NP - 1,)),
            ],
            compiler_params=pltpu.CompilerParams(
                collective_id=0, has_side_effects=True, vmem_limit_bytes=67_000_000),
            cost_estimate=pl.CostEstimate(flops=40_000_000_000, bytes_accessed=160_000_000, transcendentals=0),
        )(x, dy, rg, w1, w3, w2)

        def perm(fy, fx):
            out = []
            for p in range(NP):
                yy, xx, cc = p // 4, (p // 2) % 2, p % 2
                out.append((p, (yy ^ fy) * 4 + (xx ^ fx) * 2 + cc))
            return out

        eb = 2
        per = GRP // eb

        def grads(first, count, prev):
            def eidx(s):
                return (first // eb + s, 0, 0)

            head = pl.BlockSpec((1, eb, NROW, d), lambda s: (first // SPLIT, jnp.minimum(s, per - 1), 0, 0))
            return pl.pallas_call(
                functools.partial(grad_kernel, first, count, eb, len(prev)),
                grid=(count // eb,),
                in_specs=[anyspec, anyspec, vm, vm, pl.BlockSpec((eb, NROW, ff), eidx), pl.BlockSpec((eb, NROW, 2 * ff), eidx), head, head] + [anyspec] * len(prev),
                out_specs=[pl.BlockSpec((eb, d, ff), eidx), pl.BlockSpec((eb, d, ff), eidx), pl.BlockSpec((eb, ff, d), eidx)],
                out_shape=[sds((el, d, ff), F32), sds((el, d, ff), F32), sds((el, ff, d), F32)],
                input_output_aliases={8 + k: k for k in range(len(prev))},
                scratch_shapes=[
                    pltpu.VMEM((NP, tok, d), BF16),
                    pltpu.VMEM((NP, tok, d), BF16),
                    pltpu.VMEM((2, GRP, NROW, d), BF16),
                    pltpu.VMEM((2, GRP, NROW, d), BF16),
                    pltpu.SemaphoreType.DMA((2,)),
                ],
                compiler_params=pltpu.CompilerParams(
                    dimension_semantics=('arbitrary',), vmem_limit_bytes=60_000_000),
                cost_estimate=pl.CostEstimate(flops=20_000_000_000 * count // el, bytes_accessed=150_000_000 * count // el, transcendentals=0),
            )(xa, dya, cm, gm, a, duv, xef, dof, *prev)

        r1x = lax.ppermute(sx, grp, perm(0, 1))
        r1y = lax.ppermute(sy, grp, perm(1, 0))
        prev = grads(0, SPLIT, ())
        prev, r1x, r1y = lax.optimization_barrier((prev, r1x, r1y))
        r2a = lax.ppermute(ka[0] + r1x[0], grp, perm(1, 0))
        r2b = lax.ppermute(kb[0] + r1y[0], grp, perm(0, 1))
        gw1, gw3, gw2 = grads(SPLIT, el - SPLIT, tuple(prev))
        dx = jnp.concatenate([ka[1] + r1x[1] + r2a, kb[1] + r1y[1] + r2b], axis=0).astype(BF16)
        return y, dx, dg.T, gw1, gw3, gw2

    return jax.shard_map(local, mesh=mesh, in_specs=(tspec, tspec, tspec, wspec, wspec, wspec, tspec), out_specs=(tspec, tspec, tspec, gspec, gspec, gspec), check_vma=False)
```

```python
import functools

import jax
import jax.numpy as jnp
from jax import lax
from jax.experimental import pallas as pl
from jax.experimental.pallas import tpu as pltpu
from jax.sharding import PartitionSpec as P

F32 = jnp.float32
BF16 = jnp.bfloat16
MESH = pl.DeviceIdType.MESH
NP = 8
TOK = 256
HALF = TOK // 2
CAP = 24
PAD = 32
GRP = 8
NROW = NP * CAP
NBUF = 8
PAIR = 2


def nt(a, b):
    return lax.dot_general(a, b, (((1,), (1,)), ((), ())), preferred_element_type=F32)


def nn(a, b):
    return lax.dot_general(a, b, (((1,), (0,)), ((), ())), preferred_element_type=F32)


def tn(a, b):
    return lax.dot_general(a, b, (((0,), (0,)), ((), ())), preferred_element_type=F32)


def onehot(rows, cap):
    n = rows.shape[0]
    it = lax.broadcasted_iota(jnp.int32, (cap, TOK), 0).astype(F32)
    return [jnp.broadcast_to(rows[k:k + 1], (cap, TOK)) == it for k in range(n)]


def ds(i, n):
    return pl.ds(pl.multiple_of(i * n, n), n)


def gather_pair(cm, g, q, src, store):
    res = []
    for h in range(2):
        p = q * 2 + h
        oh = onehot(cm[p, ds(g, GRP), :], CAP)
        oh = jnp.concatenate([jnp.where(m, 1.0, 0.0) for m in oh], axis=0).astype(BF16)
        res.append(nn(oh, src[p]))
    for k in range(GRP):
        blk = jnp.concatenate([r[k * CAP:(k + 1) * CAP] for r in res], axis=0)
        store(k, ds(q, 2 * CAP), blk.astype(BF16))


def gather_dy_pair(cm, gm, g, q, src, store, store_scaled):
    res, scaled = [], []
    for h in range(2):
        p = q * 2 + h
        oh = onehot(cm[p, ds(g, GRP), :], CAP)
        gr = gm[p, ds(g, GRP), :]
        col = jnp.concatenate(
            [jnp.sum(jnp.where(m, jnp.broadcast_to(gr[k:k + 1], (CAP, TOK)), 0.0), axis=1, keepdims=True)
             for k, m in enumerate(oh)], axis=0)
        oh = jnp.concatenate([jnp.where(m, 1.0, 0.0) for m in oh], axis=0).astype(BF16)
        r = nn(oh, src[p])
        res.append(r)
        scaled.append(col * r)
    for parts, put in ((res, store), (scaled, store_scaled)):
        if put is None:
            continue
        for k in range(GRP):
            blk = jnp.concatenate([r[k * CAP:(k + 1) * CAP] for r in parts], axis=0)
            put(k, ds(q, 2 * CAP), blk.astype(BF16))


def main_kernel(el, x_hbm, dy_hbm, id_ref, gate_ref, w1_hbm, w3_hbm, w2_hbm,
                y_ref, dg_ref, sd_hbm, sx_hbm, sy_hbm, ka_hbm, xa_hbm, dya_hbm, cm_hbm, gm_hbm, duv_hbm, a_hbm, xef_hbm, dof_hbm,
                xs, dys, rgs, xe_s, do_s, dgc_s, o_s, uv_s, a_s, yacc, dxacc, cm, gm, dgm, dgo, dgr,
                w1b, w3b, w2b, rd, r1, r2,
                wsem, lsem, osem, psem, credit, rg_ss, rg_rs, ag_ss, ag_rs, dd_ss, dd_rs, s1_ss, s1_rs, s2_ss, s2_rs, dg_ss, dg_rs):
    ng = el // GRP
    ff = w2b.shape[1]
    Z = lax.axis_index('dp')
    Y = lax.axis_index('row')
    col = lax.axis_index('col')
    X = lax.div(col, 2)
    C = lax.rem(col, 2)
    me = Y * 4 + col
    e0 = me * el

    def pos(fy, fx, fc):
        return (1 - Y if fy else Y), (1 - X if fx else X), (1 - C if fc else C)

    def blk(fy, fx, fc):
        yy, xx, cc = pos(fy, fx, fc)
        return yy * 4 + xx * 2 + cc

    def dev(fy, fx, fc):
        yy, xx, cc = pos(fy, fx, fc)
        return (Z, yy, xx * 2 + cc)

    peers = [(a, b, c) for a in range(2) for b in range(2) for c in range(2)][1:]

    def remote(src, dst, ss, rs, to):
        return pltpu.make_async_remote_copy(src_ref=src, dst_ref=dst, send_sem=ss, recv_sem=rs,
                                            device_id=dev(*to), device_id_type=MESH)

    lx = pltpu.make_async_copy(x_hbm, xs.at[me], lsem.at[0])
    ld = pltpu.make_async_copy(dy_hbm, dys.at[me], lsem.at[1])
    lx.start()
    ld.start()

    def wcopies(e):
        b = lax.rem(e, NBUF)
        k = lax.rem(e, el)
        return [pltpu.make_async_copy(h.at[k], v.at[b], wsem.at[n, b])
                for n, (h, v) in enumerate(((w1_hbm, w1b), (w3_hbm, w3b), (w2_hbm, w2b)))]

    for e in range(2 * PAIR):
        for c in wcopies(e):
            c.start()

    rgs[me] = jnp.concatenate([id_ref[...].astype(F32), gate_ref[...]], axis=0)
    barrier = pltpu.get_barrier_semaphore()
    for to in peers:
        pl.semaphore_signal(barrier, inc=1, device_id=dev(*to), device_id_type=MESH)
    pl.semaphore_wait(barrier, len(peers))

    rg_copies = [remote(rgs.at[me], rgs.at[me], rg_ss.at[n], rg_rs.at[n], to) for n, to in enumerate(peers)]
    for c in rg_copies:
        c.start()

    def half(buf, b, h):
        return buf.at[b, pl.ds(h * HALF, HALF), :]

    XN, YN, DN, PN = (0, 1, 0), (1, 0, 0), (1, 1, 0), (0, 0, 1)
    FIRST = [(0, (0, 0, 0), 0, XN), (1, (0, 0, 0), 1, YN), (2, (0, 0, 0), 1, XN), (3, (0, 0, 0), 0, YN)]
    OWN2 = [(6, (0, 0, 0), 0, PN), (7, (0, 0, 0), 1, PN)]
    FWD = [(4, XN, 0, YN), (5, YN, 1, XN)]
    ARR = {0: (XN, 0), 1: (YN, 1), 2: (XN, 1), 3: (YN, 0), 4: (DN, 0), 5: (DN, 1)}
    ONWARD = {0: 8, 1: 9, 2: 10, 3: 11, 4: 12, 5: 13}

    def ag_copy(t, buf, n, f, h, to):
        r = half(buf, blk(*f), h)
        return remote(r, r, ag_ss.at[t, n], ag_rs.at[t, n], to)

    def ag_recv(t, buf, n, f, h):
        r = half(buf, blk(*f), h)
        remote(r, r, ag_ss.at[t, n], ag_rs.at[t, n], PN).wait_recv()

    def ag_start(t, buf):
        for n, f, h, to in FIRST + OWN2:
            ag_copy(t, buf, n, f, h, to).start()

    def ag_relay(t, buf, ns):
        for n in ns:
            f, h = ARR[n]
            ag_recv(t, buf, n, f, h)
            if n < 2:
                k, ff_, hh, to = FWD[n]
                ag_copy(t, buf, k, ff_, hh, to).start()
            ag_copy(t, buf, ONWARD[n], f, h, PN).start()

    def ag_finish(t, buf):
        for n, h in ((6, 0), (7, 1)):
            ag_recv(t, buf, n, PN, h)
        for n, k in ONWARD.items():
            f, h = ARR[n]
            ag_recv(t, buf, k, (f[0], f[1], 1), h)

    def ag_drain(t, buf):
        for n, f, h, to in FIRST + OWN2 + FWD:
            ag_copy(t, buf, n, f, h, to).wait_send()
        for n, k in ONWARD.items():
            f, h = ARR[n]
            ag_copy(t, buf, k, f, h, PN).wait_send()

    lx.wait()
    ld.wait()
    ag_start(0, xs)

    def zero(p, _):
        yacc[p] = jnp.zeros(yacc.shape[1:], F32)
        dxacc[p] = jnp.zeros(dxacc.shape[1:], F32)
        return 0

    lax.fori_loop(0, NP, zero, 0)

    for n, to in enumerate(peers):
        remote(rgs.at[blk(*to)], rgs.at[blk(*to)], rg_ss.at[n], rg_rs.at[n], to).wait_recv()
    top = rgs.shape[1] // 2
    tr = lax.broadcasted_iota(jnp.int32, (TOK, TOK), 0)
    tc = lax.broadcasted_iota(jnp.int32, (TOK, TOK), 1)
    tri = jnp.where(tr < tc, 1.0, 0.0).astype(BF16)
    ee = (lax.broadcasted_iota(jnp.int32, (el, TOK), 0) + e0).astype(F32)

    def prep(p, _):
        rg = rgs[p]
        m = jnp.zeros((el, TOK), F32)
        gs = jnp.zeros((el, TOK), F32)
        for j in range(top):
            hit = jnp.broadcast_to(rg[j:j + 1], (el, TOK)) == ee
            m = jnp.where(hit, 1.0, m)
            gs = jnp.where(hit, jnp.broadcast_to(rg[top + j:top + j + 1], (el, TOK)), gs)
        rank = nn(m.astype(BF16), tri)
        cm[p] = jnp.where(m > 0.0, rank, -1.0)
        gm[p] = gs
        return 0

    lax.fori_loop(0, NP, prep, 0)

    ag_relay(0, xs, (0, 1, 2, 3))
    ag_start(1, dys)
    ag_relay(0, xs, (4, 5))
    ag_finish(0, xs)
    out_copies = [pltpu.make_async_copy(xs, xa_hbm, osem.at[0]),
                  pltpu.make_async_copy(cm, cm_hbm, osem.at[1]),
                  pltpu.make_async_copy(gm, gm_hbm, osem.at[2]),
                  pltpu.make_async_copy(dys, dya_hbm, osem.at[3])]
    for c in out_copies[:3]:
        c.start()

    def gather_all(g, src):
        def step(q, _):
            def store(k, rows, val):
                xe_s[k, rows, :] = val
            gather_pair(cm, g, q, src, store)
            return 0
        lax.fori_loop(0, NP // 2, step, 0, unroll=4)

    def gather_dy(g):
        def step(q, _):
            def store(k, rows, val):
                xe_s[k, rows, :] = val

            def store_scaled(k, rows, val):
                do_s[k, rows, :] = val
            gather_dy_pair(cm, gm, g, q, dys, store, store_scaled)
            return 0
        lax.fori_loop(0, NP // 2, step, 0, unroll=4)

    def put_rows(i, val):
        zero = jnp.zeros((PAD - CAP, val.shape[1]), F32)
        for p in range(NP):
            o_s[i, p * PAD:(p + 1) * PAD, :] = jnp.concatenate([val[p * CAP:(p + 1) * CAP], zero], axis=0).astype(BF16)

    def take_rows(p):
        return jnp.concatenate([o_s[k, ds(p, PAD), :] for k in range(GRP)], axis=0)

    def combine_y(g):
        def step(p, _):
            oh = onehot(cm[p, ds(g, GRP), :], PAD)
            gr = gm[p, ds(g, GRP), :]
            g1 = gr.astype(BF16).astype(F32)
            rest = gr - g1
            g2 = rest.astype(BF16).astype(F32)
            g3 = rest - g2
            ob = take_rows(p)

            def spread(part):
                return jnp.concatenate(
                    [jnp.where(oh[k], jnp.broadcast_to(part[k:k + 1], (PAD, TOK)), 0.0) for k in range(GRP)],
                    axis=0).astype(BF16)

            gs = jnp.concatenate([spread(g1), spread(g2), spread(g3)], axis=0)
            yacc[p] += tn(gs, jnp.concatenate([ob, ob, ob], axis=0))
            return 0
        lax.fori_loop(0, NP, step, 0, unroll=4)

    def combine_dx(g, cc):
        for j in range(NP // 2):
            p = 2 * j + cc
            oh = onehot(cm[p, ds(g, GRP), :], PAD)
            one = jnp.concatenate([jnp.where(m, 1.0, 0.0) for m in oh], axis=0).astype(BF16)
            dxacc[p] += tn(one, take_rows(p))
            rows = []
            for k in range(GRP):
                db = jnp.broadcast_to(dgc_s[k, ds(p, CAP), :], (CAP, TOK))
                rows.append(jnp.sum(jnp.where(oh[k][:CAP], db, 0.0), axis=0, keepdims=True))
            dgm[p, ds(g, GRP), :] = jnp.concatenate(rows, axis=0)

    def fetch(n):
        for k in range(PAIR):
            for c in wcopies(n + k):
                c.wait()

        @pl.when(n + 2 * PAIR < 2 * el)
        def _():
            for k in range(PAIR):
                for c in wcopies(n + 2 * PAIR + k):
                    c.start()

    def w13_of(n):
        b = lax.rem(n, NBUF)
        return jnp.concatenate([w1b[b], w3b[b]], axis=1)

    def w2_of(n):
        return w2b[lax.rem(n, NBUF)]

    def skewed(g, first, base, second):
        npair = GRP // PAIR
        fetch(base)
        first(0)

        def step(r, _):
            fetch(base + r * PAIR)
            second(r - 1)
            first(r)
            return 0

        lax.fori_loop(1, npair, step, 0)
        second(npair - 1)

    def act(uv):
        u, v = uv[:, :ff], uv[:, ff:]
        sg = jax.nn.sigmoid(u)
        return u, v, sg, (u * sg * v).astype(BF16)

    ORDER = [(1, 1), (0, 1), (1, 0), (0, 0)]
    S1 = [((1, 1), 0, XN), ((1, 1), 1, YN), ((0, 1), 0, XN), ((1, 0), 1, YN)]
    IN1 = [((1, 0), 0), ((0, 1), 1), ((0, 0), 0), ((0, 0), 1)]
    S2 = [YN, XN]

    def dd_copy(t, acc, n):
        fy, fx = ORDER[n]
        return remote(acc.at[blk(fy, fx, 1)], rd.at[n], dd_ss.at[t, n], dd_rs.at[t, n], PN)

    def s1_copy(t, acc, n):
        (fy, fx), h, to = S1[n]
        return remote(half(acc, blk(fy, fx, 0), h), r1.at[t, n], s1_ss.at[t, n], s1_rs.at[t, n], to)

    def s2_copy(t, acc, n):
        (fy, fx), h = IN1[n]
        return remote(half(acc, blk(fy, fx, 0), h), r2.at[t, n], s2_ss.at[t, n], s2_rs.at[t, n], S2[n])

    def rs_start(t, acc):
        for n in range(4):
            dd_copy(t, acc, n).start()

    def rs_mid1(t, acc):
        for n in range(4):
            dd_copy(t, acc, n).wait_recv()
            fy, fx = ORDER[n]
            acc[blk(fy, fx, 0)] += rd[n]
            for k in ((0, 1), (2,), (3,), ())[n]:
                s1_copy(t, acc, k).start()

    def rs_mid2(t, acc):
        for n in range(4):
            s1_copy(t, acc, n).wait_recv()
            (fy, fx), h = IN1[n]
            acc[blk(fy, fx, 0), h * HALF:(h + 1) * HALF, :] += r1[t, n]
            if n < 2:
                s2_copy(t, acc, n).start()

    def rs_fin(t, acc, out):
        for n in range(2):
            s2_copy(t, acc, n).wait_recv()
            rows = slice(n * HALF, (n + 1) * HALF)
            out[rows, :] = (acc[me, rows, :] + r2[t, n]).astype(BF16)

    def rs_drain(t, acc):
        for n in range(4):
            dd_copy(t, acc, n).wait_send()
            s1_copy(t, acc, n).wait_send()
        for n in range(2):
            s2_copy(t, acc, n).wait_send()

    xef_copy = pltpu.make_async_copy(xe_s, xef_hbm, osem.at[6])
    dof_copy = pltpu.make_async_copy(do_s, dof_hbm, osem.at[7])

    def fwd_group(g, _):
        gather_all(g, xs)

        @pl.when(g == 0)
        def _():
            xef_copy.start()

        def f1(r):
            for k in range(PAIR):
                i = r * PAIR + k
                uv_s[g * GRP + i] = nn(xe_s[i], w13_of(g * GRP + i)).astype(BF16)

        def f2(r):
            uvs = [uv_s[g * GRP + r * PAIR + k].astype(F32) for k in range(PAIR)]
            for k in range(PAIR):
                i = r * PAIR + k
                put_rows(i, nn(act(uvs[k])[3], w2_of(g * GRP + i)))

        skewed(g, f1, g * GRP, f2)
        combine_y(g)

        @pl.when(g == 0)
        def _():
            xef_copy.wait()

        @pl.when(g == 0)
        def _():
            ag_relay(1, dys, (0, 1, 2, 3))

        @pl.when(g == 1)
        def _():
            ag_relay(1, dys, (4, 5))

        @pl.when(g == 2)
        def _():
            ag_finish(1, dys)
            out_copies[3].start()
        return 0

    lax.fori_loop(0, ng, fwd_group, 0)

    def duv_copy(g):
        return pltpu.make_async_copy(uv_s.at[ds(g, GRP)], duv_hbm.at[ds(g, GRP)], osem.at[4])

    def a_copy(g):
        return pltpu.make_async_copy(a_s, a_hbm.at[ds(g, GRP)], osem.at[5])

    def bwd_group(g, _):
        gather_dy(g)

        @pl.when(g == 0)
        def _():
            dof_copy.start()

        @pl.when(g == 0)
        def _():
            rs_start(0, yacc)

        def b1(r):
            uvs = [uv_s[g * GRP + r * PAIR + k] for k in range(PAIR)]
            for k in range(PAIR):
                i = r * PAIR + k
                e = g * GRP + i
                w2 = w2_of(el + e)
                da = nt(do_s[i], w2)
                u, v, sg, a = act(uvs[k].astype(F32))
                a_s[i] = a
                of = nn(a, w2).astype(BF16).astype(F32)
                dgc_s[i] = jnp.sum(xe_s[i].astype(F32) * of, axis=1, keepdims=True)
                du = (da * v * sg * (1.0 + u * (1.0 - sg))).astype(BF16)
                dv = (da * u * sg).astype(BF16)
                uv_s[e] = jnp.concatenate([du, dv], axis=1)

        def b2(r):
            duvs = [uv_s[g * GRP + r * PAIR + k] for k in range(PAIR)]
            for k in range(PAIR):
                i = r * PAIR + k
                put_rows(i, nt(duvs[k], w13_of(el + g * GRP + i)))

        @pl.when(g > 0)
        def _():
            a_copy(g - 1).wait()
            duv_copy(g - 1).wait()

        skewed(g, b1, el + g * GRP, b2)
        a_copy(g).start()
        duv_copy(g).start()
        combine_dx(g, 1 - C)

        @pl.when(g == ng - 1)
        def _():
            pl.semaphore_wait(credit, 1)
            rs_start(1, dxacc)
        combine_dx(g, C)

        @pl.when(g == 0)
        def _():
            dof_copy.wait()

        @pl.when(g == 1)
        def _():
            rs_mid1(0, yacc)
            pl.semaphore_signal(credit, inc=1, device_id=dev(*PN), device_id_type=MESH)

        @pl.when(g == ng - 1)
        def _():
            rs_mid2(0, yacc)
        return 0

    lax.fori_loop(0, ng, bwd_group, 0)

    def spread_dg(p, _):
        rg = rgs[p]
        acc = jnp.zeros((top, TOK), F32)
        for e in range(el):
            ef = (e0 + e).astype(F32)
            acc = acc + jnp.where(rg[:top] == ef, jnp.broadcast_to(dgm[p, e:e + 1, :], (top, TOK)), 0.0)
        dgo[p] = acc
        return 0

    lax.fori_loop(0, NP, spread_dg, 0)
    rs_fin(0, yacc, y_ref)
    dg_copies = [remote(dgo.at[blk(*to)], dgr.at[n], dg_ss.at[n], dg_rs.at[n], to) for n, to in enumerate(peers)]
    for c in dg_copies:
        c.start()
    part_copies = []
    for n in range(4):
        dd_copy(1, dxacc, n).wait_recv()
        b = blk(*ORDER[n], 0)
        dxacc[b] += rd[n]
        c = pltpu.make_async_copy(dxacc.at[b], (sd_hbm, sx_hbm, sy_hbm, ka_hbm)[n], psem.at[n])
        c.start()
        part_copies.append(c)
    total = dgo[me]
    for n, c in enumerate(dg_copies):
        c.wait_recv()
        total = total + dgr[n]
    dg_ref[...] = total

    ag_drain(0, xs)
    ag_drain(1, dys)
    rs_drain(0, yacc)
    for n in range(4):
        dd_copy(1, dxacc, n).wait_send()
    for c in part_copies:
        c.wait()
    for c in rg_copies + dg_copies:
        c.wait_send()
    for c in out_copies:
        c.wait()
    a_copy(ng - 1).wait()
    duv_copy(ng - 1).wait()


def grad_kernel(count, eb, y_ref, dg_ref, xa_hbm, dya_hbm, cm, gm, a_ref, duv_ref, xef_ref, dof_ref,
                yo_ref, dgo_ref, gw1_ref, gw3_ref, gw2_ref, xs, dys, xe_s, do_s, sem):
    s = pl.program_id(0)
    per = GRP // eb
    ff = a_ref.shape[2]
    g = lax.div(s, per)
    i = lax.rem(s, per)
    loads = [pltpu.make_async_copy(xa_hbm, xs, sem.at[0]), pltpu.make_async_copy(dya_hbm, dys, sem.at[1])]

    @pl.when(s == 0)
    def _():
        for c in loads:
            c.start()
        yo_ref[...] = y_ref[...]
        dgo_ref[...] = dg_ref[...]

    @pl.when(s == 1)
    def _():
        for c in loads:
            c.wait()

    def gather(q):
        n = g + 1
        slot = lax.rem(n, 2)

        def store(j, rows, val):
            xe_s[slot, j, rows, :] = val

        def store_scaled(j, rows, val):
            do_s[slot, j, rows, :] = val
        gather_pair(cm, n, q, xs, store)
        gather_dy_pair(cm, gm, n, q, dys, None, store_scaled)

    more = g + 1 < count // GRP

    @pl.when(jnp.logical_and(more, jnp.logical_and(i >= 1, i <= NP // 2)))
    def _():
        gather(i - 1)

    def core(xe, do):
        for k in range(eb):
            g13 = tn(xe[k], duv_ref[k])
            gw1_ref[k] = g13[:, :ff]
            gw3_ref[k] = g13[:, ff:]
            gw2_ref[k] = tn(a_ref[k], do[k])

    @pl.when(g == 0)
    def _():
        core([xef_ref[k] for k in range(eb)], [dof_ref[k] for k in range(eb)])

    @pl.when(g > 0)
    def _():
        slot = lax.rem(g, 2)
        core([xe_s[slot, i * eb + k] for k in range(eb)], [do_s[slot, i * eb + k] for k in range(eb)])


def solution(mesh):
    grp = ('row', 'col')
    tspec = P(('dp', 'row', 'col'), None)
    wspec = P(grp, None, None)
    gspec = P(('dp', 'row', 'col'), None, None)

    def local(x, ridx, gates, w1, w3, w2, dy):
        tok, d = x.shape
        top = ridx.shape[1]
        el, _, ff = w1.shape
        anyspec = pl.BlockSpec(memory_space=pl.ANY)
        vm = pl.BlockSpec(memory_space=pltpu.VMEM)
        sds = jax.ShapeDtypeStruct
        dma = pltpu.SemaphoreType.DMA
        y, dg, sd, sx, sy, ka, xa, dya, cm, gm, duv, a, xef, dof = pl.pallas_call(
            functools.partial(main_kernel, el),
            in_specs=[anyspec, anyspec, vm, vm, anyspec, anyspec, anyspec],
            out_specs=[vm, vm] + [anyspec] * 12,
            out_shape=[
                sds((tok, d), BF16), sds((top, tok), F32)] + [sds((tok, d), F32)] * 4 + [
                sds((NP, tok, d), BF16), sds((NP, tok, d), BF16),
                sds((NP, el, tok), F32), sds((NP, el, tok), F32),
                sds((el, NROW, 2 * ff), BF16), sds((el, NROW, ff), BF16),
                sds((GRP, NROW, d), BF16), sds((GRP, NROW, d), BF16),
            ],
            scratch_shapes=[
                pltpu.VMEM((NP, tok, d), BF16),
                pltpu.VMEM((NP, tok, d), BF16),
                pltpu.VMEM((NP, 2 * top, tok), F32),
                pltpu.VMEM((GRP, NROW, d), BF16),
                pltpu.VMEM((GRP, NROW, d), BF16),
                pltpu.VMEM((GRP, NROW, 1), F32),
                pltpu.VMEM((GRP, NP * PAD, d), BF16),
                pltpu.VMEM((el, NROW, 2 * ff), BF16),
                pltpu.VMEM((GRP, NROW, ff), BF16),
                pltpu.VMEM((NP, tok, d), F32),
                pltpu.VMEM((NP, tok, d), F32),
                pltpu.VMEM((NP, el, tok), F32),
                pltpu.VMEM((NP, el, tok), F32),
                pltpu.VMEM((NP, el, tok), F32),
                pltpu.VMEM((NP, top, tok), F32),
                pltpu.VMEM((NP - 1, top, tok), F32),
                pltpu.VMEM((NBUF, d, ff), BF16),
                pltpu.VMEM((NBUF, d, ff), BF16),
                pltpu.VMEM((NBUF, ff, d), BF16),
                pltpu.VMEM((4, tok, d), F32),
                pltpu.VMEM((1, 4, tok // 2, d), F32),
                pltpu.VMEM((1, 2, tok // 2, d), F32),
                dma((3, NBUF)), dma((2,)), dma((8,)), dma((4,)), pltpu.SemaphoreType.REGULAR,
                dma((NP - 1,)), dma((NP - 1,)),
                dma((2, 14)), dma((2, 14)),
                dma((2, 4)), dma((2, 4)),
                dma((1, 4)), dma((1, 4)),
                dma((1, 2)), dma((1, 2)),
                dma((NP - 1,)), dma((NP - 1,)),
            ],
            compiler_params=pltpu.CompilerParams(
                collective_id=0, has_side_effects=True, vmem_limit_bytes=67_000_000),
            cost_estimate=pl.CostEstimate(flops=40_000_000_000, bytes_accessed=160_000_000, transcendentals=0),
        )(x, dy, ridx.T, gates.T, w1, w3, w2)

        def perm(fy, fx):
            out = []
            for p in range(NP):
                yy, xx, cc = p // 4, (p // 2) % 2, p % 2
                out.append((p, (yy ^ fy) * 4 + (xx ^ fx) * 2 + cc))
            return out

        rd = lax.ppermute(sd, grp, perm(1, 1))
        rx = lax.ppermute(sx, grp, perm(0, 1))
        ry = lax.ppermute(sy, grp, perm(1, 0))
        eb = 1
        per = GRP // eb

        def eidx(s):
            return (s, 0, 0)

        head = pl.BlockSpec((eb, NROW, d), lambda s: (jnp.minimum(s, per - 1), 0, 0))
        y, dg, gw1, gw3, gw2 = pl.pallas_call(
            functools.partial(grad_kernel, el, eb),
            grid=(el // eb,),
            in_specs=[vm, vm, anyspec, anyspec, vm, vm, pl.BlockSpec((eb, NROW, ff), eidx), pl.BlockSpec((eb, NROW, 2 * ff), eidx), head, head],
            out_specs=[vm, vm, pl.BlockSpec((eb, d, ff), eidx), pl.BlockSpec((eb, d, ff), eidx), pl.BlockSpec((eb, ff, d), eidx)],
            out_shape=[sds((tok, d), BF16), sds((top, tok), F32), sds((el, d, ff), F32), sds((el, d, ff), F32), sds((el, ff, d), F32)],
            scratch_shapes=[
                pltpu.VMEM((NP, tok, d), BF16),
                pltpu.VMEM((NP, tok, d), BF16),
                pltpu.VMEM((2, GRP, NROW, d), BF16),
                pltpu.VMEM((2, GRP, NROW, d), BF16),
                pltpu.SemaphoreType.DMA((2,)),
            ],
            compiler_params=pltpu.CompilerParams(
                dimension_semantics=('arbitrary',), vmem_limit_bytes=56_000_000),
            cost_estimate=pl.CostEstimate(flops=40_000_000_000, bytes_accessed=160_000_000, transcendentals=0),
        )(y, dg, xa, dya, cm, gm, a, duv, xef, dof)
        dx = (ka + rx + ry + rd).astype(BF16)
        return y, dx, dg.T, gw1, gw3, gw2

    return jax.shard_map(local, mesh=mesh, in_specs=(tspec, tspec, tspec, wspec, wspec, wspec, tspec), out_specs=(tspec, tspec, tspec, gspec, gspec, gspec), check_vma=False)
```

```python
import functools

import jax
import jax.numpy as jnp
from jax import lax
from jax.experimental import pallas as pl
from jax.experimental.pallas import tpu as pltpu
from jax.sharding import PartitionSpec as P

F32 = jnp.float32
BF16 = jnp.bfloat16
MESH = pl.DeviceIdType.MESH
NP = 8
TOK = 256
HALF = TOK // 2
CAP = 24
PAD = 32
GRP = 8
NROW = NP * CAP
NBUF = 8
PAIR = 2
NOUT = 3


def nt(a, b):
    return lax.dot_general(a, b, (((1,), (1,)), ((), ())), preferred_element_type=F32)


def nn(a, b):
    return lax.dot_general(a, b, (((1,), (0,)), ((), ())), preferred_element_type=F32)


def tn(a, b):
    return lax.dot_general(a, b, (((0,), (0,)), ((), ())), preferred_element_type=F32)


def onehot(rows, cap):
    n = rows.shape[0]
    it = lax.broadcasted_iota(jnp.int32, (cap, TOK), 0).astype(F32)
    return [jnp.broadcast_to(rows[k:k + 1], (cap, TOK)) == it for k in range(n)]


def ds(i, n):
    return pl.ds(pl.multiple_of(i * n, n), n)


def gather_pair(cm, g, q, src, store):
    res = []
    for h in range(2):
        p = q * 2 + h
        oh = onehot(cm[p, ds(g, GRP), :], CAP)
        oh = jnp.concatenate([jnp.where(m, 1.0, 0.0) for m in oh], axis=0).astype(BF16)
        res.append(nn(oh, src[p]))
    for k in range(GRP):
        blk = jnp.concatenate([r[k * CAP:(k + 1) * CAP] for r in res], axis=0)
        store(k, ds(q, 2 * CAP), blk.astype(BF16))


def gather_dy_pair(cm, gm, g, q, src, store, store_scaled):
    res, scaled = [], []
    for h in range(2):
        p = q * 2 + h
        oh = onehot(cm[p, ds(g, GRP), :], CAP)
        gr = gm[p, ds(g, GRP), :]
        col = jnp.concatenate(
            [jnp.sum(jnp.where(m, jnp.broadcast_to(gr[k:k + 1], (CAP, TOK)), 0.0), axis=1, keepdims=True)
             for k, m in enumerate(oh)], axis=0)
        oh = jnp.concatenate([jnp.where(m, 1.0, 0.0) for m in oh], axis=0).astype(BF16)
        r = nn(oh, src[p])
        res.append(r)
        scaled.append(col * r)
    for parts, put in ((res, store), (scaled, store_scaled)):
        if put is None:
            continue
        for k in range(GRP):
            blk = jnp.concatenate([r[k * CAP:(k + 1) * CAP] for r in parts], axis=0)
            put(k, ds(q, 2 * CAP), blk.astype(BF16))


def main_kernel(el, x_hbm, dy_hbm, id_ref, gate_ref, w1_hbm, w3_hbm, w2_hbm,
                y_ref, dg_ref, sd_hbm, sx_hbm, sy_hbm, ka_hbm, xa_hbm, dya_hbm, cm_hbm, gm_hbm, duv_hbm, a_hbm, xef_hbm, dof_hbm,
                xs, dys, rgs, xe_s, do_s, dgc_s, o_s, uv_s, a_s, yacc, dxacc, cm, gm, dgm, dgo, dgr,
                w1b, w3b, w2b, rd, r1, r2,
                wsem, lsem, osem, psem, credit, rg_ss, rg_rs, ag_ss, ag_rs, dd_ss, dd_rs, s1_ss, s1_rs, s2_ss, s2_rs, dg_ss, dg_rs):
    ng = el // GRP
    ff = w2b.shape[1]
    Z = lax.axis_index('dp')
    Y = lax.axis_index('row')
    col = lax.axis_index('col')
    X = lax.div(col, 2)
    C = lax.rem(col, 2)
    me = Y * 4 + col
    e0 = me * el

    def pos(fy, fx, fc):
        return (1 - Y if fy else Y), (1 - X if fx else X), (1 - C if fc else C)

    def blk(fy, fx, fc):
        yy, xx, cc = pos(fy, fx, fc)
        return yy * 4 + xx * 2 + cc

    def dev(fy, fx, fc):
        yy, xx, cc = pos(fy, fx, fc)
        return (Z, yy, xx * 2 + cc)

    peers = [(a, b, c) for a in range(2) for b in range(2) for c in range(2)][1:]

    def remote(src, dst, ss, rs, to):
        return pltpu.make_async_remote_copy(src_ref=src, dst_ref=dst, send_sem=ss, recv_sem=rs,
                                            device_id=dev(*to), device_id_type=MESH)

    lx = pltpu.make_async_copy(x_hbm, xs.at[me], lsem.at[0])
    ld = pltpu.make_async_copy(dy_hbm, dys.at[me], lsem.at[1])
    lx.start()
    ld.start()

    def wcopies(e):
        b = lax.rem(e, NBUF)
        k = lax.rem(e, el)
        return [pltpu.make_async_copy(h.at[k], v.at[b], wsem.at[n, b])
                for n, (h, v) in enumerate(((w1_hbm, w1b), (w3_hbm, w3b), (w2_hbm, w2b)))]

    for e in range(2 * PAIR):
        for c in wcopies(e):
            c.start()

    rgs[me] = jnp.concatenate([id_ref[...].astype(F32), gate_ref[...]], axis=0)
    barrier = pltpu.get_barrier_semaphore()
    for to in peers:
        pl.semaphore_signal(barrier, inc=1, device_id=dev(*to), device_id_type=MESH)
    pl.semaphore_wait(barrier, len(peers))

    rg_copies = [remote(rgs.at[me], rgs.at[me], rg_ss.at[n], rg_rs.at[n], to) for n, to in enumerate(peers)]
    for c in rg_copies:
        c.start()

    def half(buf, b, h):
        return buf.at[b, pl.ds(h * HALF, HALF), :]

    XN, YN, DN, PN = (0, 1, 0), (1, 0, 0), (1, 1, 0), (0, 0, 1)
    FIRST = [(0, (0, 0, 0), 0, XN), (1, (0, 0, 0), 1, YN), (2, (0, 0, 0), 1, XN), (3, (0, 0, 0), 0, YN)]
    OWN2 = [(6, (0, 0, 0), 0, PN), (7, (0, 0, 0), 1, PN)]
    FWD = [(4, XN, 0, YN), (5, YN, 1, XN)]
    ARR = {0: (XN, 0), 1: (YN, 1), 2: (XN, 1), 3: (YN, 0), 4: (DN, 0), 5: (DN, 1)}
    ONWARD = {0: 8, 1: 9, 2: 10, 3: 11, 4: 12, 5: 13}

    def ag_copy(t, buf, n, f, h, to):
        r = half(buf, blk(*f), h)
        return remote(r, r, ag_ss.at[t, n], ag_rs.at[t, n], to)

    def ag_recv(t, buf, n, f, h):
        r = half(buf, blk(*f), h)
        remote(r, r, ag_ss.at[t, n], ag_rs.at[t, n], PN).wait_recv()

    def ag_start(t, buf):
        for n, f, h, to in FIRST + OWN2:
            ag_copy(t, buf, n, f, h, to).start()

    def ag_relay(t, buf, ns):
        for n in ns:
            f, h = ARR[n]
            ag_recv(t, buf, n, f, h)
            if n < 2:
                k, ff_, hh, to = FWD[n]
                ag_copy(t, buf, k, ff_, hh, to).start()
            ag_copy(t, buf, ONWARD[n], f, h, PN).start()

    def ag_finish(t, buf):
        for n, h in ((6, 0), (7, 1)):
            ag_recv(t, buf, n, PN, h)
        for n, k in ONWARD.items():
            f, h = ARR[n]
            ag_recv(t, buf, k, (f[0], f[1], 1), h)

    def ag_drain(t, buf):
        for n, f, h, to in FIRST + OWN2 + FWD:
            ag_copy(t, buf, n, f, h, to).wait_send()
        for n, k in ONWARD.items():
            f, h = ARR[n]
            ag_copy(t, buf, k, f, h, PN).wait_send()

    lx.wait()
    ld.wait()
    ag_start(0, xs)

    def zero(p, _):
        yacc[p] = jnp.zeros(yacc.shape[1:], F32)
        dxacc[p] = jnp.zeros(dxacc.shape[1:], F32)
        return 0

    lax.fori_loop(0, NP, zero, 0)

    for n, to in enumerate(peers):
        remote(rgs.at[blk(*to)], rgs.at[blk(*to)], rg_ss.at[n], rg_rs.at[n], to).wait_recv()
    top = rgs.shape[1] // 2
    tr = lax.broadcasted_iota(jnp.int32, (TOK, TOK), 0)
    tc = lax.broadcasted_iota(jnp.int32, (TOK, TOK), 1)
    tri = jnp.where(tr < tc, 1.0, 0.0).astype(BF16)
    ee = (lax.broadcasted_iota(jnp.int32, (el, TOK), 0) + e0).astype(F32)

    def prep(p, _):
        rg = rgs[p]
        m = jnp.zeros((el, TOK), F32)
        gs = jnp.zeros((el, TOK), F32)
        for j in range(top):
            hit = jnp.broadcast_to(rg[j:j + 1], (el, TOK)) == ee
            m = jnp.where(hit, 1.0, m)
            gs = jnp.where(hit, jnp.broadcast_to(rg[top + j:top + j + 1], (el, TOK)), gs)
        rank = nn(m.astype(BF16), tri)
        cm[p] = jnp.where(m > 0.0, rank, -1.0)
        gm[p] = gs
        return 0

    lax.fori_loop(0, NP, prep, 0)

    ag_relay(0, xs, (0, 1, 2, 3))
    ag_start(1, dys)
    ag_relay(0, xs, (4, 5))
    ag_finish(0, xs)
    out_copies = [pltpu.make_async_copy(xs, xa_hbm, osem.at[0]),
                  pltpu.make_async_copy(cm, cm_hbm, osem.at[1]),
                  pltpu.make_async_copy(gm, gm_hbm, osem.at[2]),
                  pltpu.make_async_copy(dys, dya_hbm, osem.at[3])]
    for c in out_copies[:3]:
        c.start()

    def gather_all(g, src):
        def step(q, _):
            def store(k, rows, val):
                xe_s[k, rows, :] = val
            gather_pair(cm, g, q, src, store)
            return 0
        lax.fori_loop(0, NP // 2, step, 0, unroll=4)

    def gather_dy(g):
        def step(q, _):
            def store(k, rows, val):
                xe_s[k, rows, :] = val

            def store_scaled(k, rows, val):
                do_s[k, rows, :] = val
            gather_dy_pair(cm, gm, g, q, dys, store, store_scaled)
            return 0
        lax.fori_loop(0, NP // 2, step, 0, unroll=4)

    def put_rows(i, val):
        zero = jnp.zeros((PAD - CAP, val.shape[1]), F32)
        for p in range(NP):
            o_s[i, p * PAD:(p + 1) * PAD, :] = jnp.concatenate([val[p * CAP:(p + 1) * CAP], zero], axis=0).astype(BF16)

    def take_rows(p):
        return jnp.concatenate([o_s[k, ds(p, PAD), :] for k in range(GRP)], axis=0)

    def combine_y(g):
        def step(p, _):
            oh = onehot(cm[p, ds(g, GRP), :], PAD)
            gr = gm[p, ds(g, GRP), :]
            g1 = gr.astype(BF16).astype(F32)
            rest = gr - g1
            g2 = rest.astype(BF16).astype(F32)
            g3 = rest - g2
            ob = take_rows(p)

            def spread(part):
                return jnp.concatenate(
                    [jnp.where(oh[k], jnp.broadcast_to(part[k:k + 1], (PAD, TOK)), 0.0) for k in range(GRP)],
                    axis=0).astype(BF16)

            gs = jnp.concatenate([spread(g1), spread(g2), spread(g3)], axis=0)
            yacc[p] += tn(gs, jnp.concatenate([ob, ob, ob], axis=0))
            return 0
        lax.fori_loop(0, NP, step, 0, unroll=4)

    def combine_dx(g, cc):
        for j in range(NP // 2):
            p = 2 * j + cc
            oh = onehot(cm[p, ds(g, GRP), :], PAD)
            one = jnp.concatenate([jnp.where(m, 1.0, 0.0) for m in oh], axis=0).astype(BF16)
            dxacc[p] += tn(one, take_rows(p))
            rows = []
            for k in range(GRP):
                db = jnp.broadcast_to(dgc_s[k, ds(p, CAP), :], (CAP, TOK))
                rows.append(jnp.sum(jnp.where(oh[k][:CAP], db, 0.0), axis=0, keepdims=True))
            dgm[p, ds(g, GRP), :] = jnp.concatenate(rows, axis=0)

    def fetch(n):
        for k in range(PAIR):
            for c in wcopies(n + k):
                c.wait()

        @pl.when(n + 2 * PAIR < 2 * el)
        def _():
            for k in range(PAIR):
                for c in wcopies(n + 2 * PAIR + k):
                    c.start()

    def w13_of(n):
        b = lax.rem(n, NBUF)
        return jnp.concatenate([w1b[b], w3b[b]], axis=1)

    def w2_of(n):
        return w2b[lax.rem(n, NBUF)]

    def skewed(g, first, base, second):
        npair = GRP // PAIR
        fetch(base)
        first(0)

        def step(r, _):
            fetch(base + r * PAIR)
            second(r - 1)
            first(r)
            return 0

        lax.fori_loop(1, npair, step, 0)
        second(npair - 1)

    def act(uv):
        u, v = uv[:, :ff], uv[:, ff:]
        sg = jax.nn.sigmoid(u)
        return u, v, sg, (u * sg * v).astype(BF16)

    ORDER = [(1, 1), (0, 1), (1, 0), (0, 0)]
    S1 = [((1, 1), 0, XN), ((1, 1), 1, YN), ((0, 1), 0, XN), ((1, 0), 1, YN)]
    IN1 = [((1, 0), 0), ((0, 1), 1), ((0, 0), 0), ((0, 0), 1)]
    S2 = [YN, XN]

    def dd_copy(t, acc, n):
        fy, fx = ORDER[n]
        return remote(acc.at[blk(fy, fx, 1)], rd.at[n], dd_ss.at[t, n], dd_rs.at[t, n], PN)

    def s1_copy(t, acc, n):
        (fy, fx), h, to = S1[n]
        return remote(half(acc, blk(fy, fx, 0), h), r1.at[t, n], s1_ss.at[t, n], s1_rs.at[t, n], to)

    def s2_copy(t, acc, n):
        (fy, fx), h = IN1[n]
        return remote(half(acc, blk(fy, fx, 0), h), r2.at[t, n], s2_ss.at[t, n], s2_rs.at[t, n], S2[n])

    def rs_start(t, acc):
        for n in range(4):
            dd_copy(t, acc, n).start()

    def rs_mid1(t, acc):
        for n in range(4):
            dd_copy(t, acc, n).wait_recv()
            fy, fx = ORDER[n]
            acc[blk(fy, fx, 0)] += rd[n]
            for k in ((0, 1), (2,), (3,), ())[n]:
                s1_copy(t, acc, k).start()

    def rs_mid2(t, acc):
        for n in range(4):
            s1_copy(t, acc, n).wait_recv()
            (fy, fx), h = IN1[n]
            acc[blk(fy, fx, 0), h * HALF:(h + 1) * HALF, :] += r1[t, n]
            if n < 2:
                s2_copy(t, acc, n).start()

    def rs_fin(t, acc, out):
        for n in range(2):
            s2_copy(t, acc, n).wait_recv()
            rows = slice(n * HALF, (n + 1) * HALF)
            out[rows, :] = (acc[me, rows, :] + r2[t, n]).astype(BF16)

    def rs_drain(t, acc):
        for n in range(4):
            dd_copy(t, acc, n).wait_send()
            s1_copy(t, acc, n).wait_send()
        for n in range(2):
            s2_copy(t, acc, n).wait_send()

    xef_copy = pltpu.make_async_copy(xe_s, xef_hbm, osem.at[6])
    dof_copy = pltpu.make_async_copy(do_s, dof_hbm, osem.at[7])

    def fwd_group(g, _):
        gather_all(g, xs)

        @pl.when(g == 0)
        def _():
            xef_copy.start()

        def f1(r):
            for k in range(PAIR):
                i = r * PAIR + k
                uv_s[g * GRP + i] = nn(xe_s[i], w13_of(g * GRP + i)).astype(BF16)

        def f2(r):
            uvs = [uv_s[g * GRP + r * PAIR + k].astype(F32) for k in range(PAIR)]
            for k in range(PAIR):
                i = r * PAIR + k
                put_rows(i, nn(act(uvs[k])[3], w2_of(g * GRP + i)))

        skewed(g, f1, g * GRP, f2)
        combine_y(g)

        @pl.when(g == 0)
        def _():
            xef_copy.wait()

        @pl.when(g == 0)
        def _():
            ag_relay(1, dys, (0, 1, 2, 3))

        @pl.when(g == 1)
        def _():
            ag_relay(1, dys, (4, 5))

        @pl.when(g == 2)
        def _():
            ag_finish(1, dys)
            out_copies[3].start()
        return 0

    lax.fori_loop(0, ng, fwd_group, 0)

    def duv_copy(g):
        return pltpu.make_async_copy(uv_s.at[ds(g, GRP)], duv_hbm.at[ds(g, GRP)], osem.at[4])

    def a_copy(g):
        return pltpu.make_async_copy(a_s, a_hbm.at[ds(g, GRP)], osem.at[5])

    def bwd_group(g, _):
        gather_dy(g)

        @pl.when(g == 0)
        def _():
            dof_copy.start()

        @pl.when(g == 0)
        def _():
            rs_start(0, yacc)

        def b1(r):
            uvs = [uv_s[g * GRP + r * PAIR + k] for k in range(PAIR)]
            for k in range(PAIR):
                i = r * PAIR + k
                e = g * GRP + i
                w2 = w2_of(el + e)
                da = nt(do_s[i], w2)
                u, v, sg, a = act(uvs[k].astype(F32))
                a_s[i] = a
                of = nn(a, w2).astype(BF16).astype(F32)
                dgc_s[i] = jnp.sum(xe_s[i].astype(F32) * of, axis=1, keepdims=True)
                du = (da * v * sg * (1.0 + u * (1.0 - sg))).astype(BF16)
                dv = (da * u * sg).astype(BF16)
                uv_s[e] = jnp.concatenate([du, dv], axis=1)

        def b2(r):
            duvs = [uv_s[g * GRP + r * PAIR + k] for k in range(PAIR)]
            for k in range(PAIR):
                i = r * PAIR + k
                put_rows(i, nt(duvs[k], w13_of(el + g * GRP + i)))

        @pl.when(g > 0)
        def _():
            a_copy(g - 1).wait()
            duv_copy(g - 1).wait()

        skewed(g, b1, el + g * GRP, b2)
        a_copy(g).start()
        duv_copy(g).start()
        combine_dx(g, 1 - C)

        @pl.when(g == ng - 1)
        def _():
            pl.semaphore_wait(credit, 1)
            rs_start(1, dxacc)
        combine_dx(g, C)

        @pl.when(g == 0)
        def _():
            dof_copy.wait()

        @pl.when(g == 1)
        def _():
            rs_mid1(0, yacc)
            pl.semaphore_signal(credit, inc=1, device_id=dev(*PN), device_id_type=MESH)

        @pl.when(g == ng - 1)
        def _():
            rs_mid2(0, yacc)
        return 0

    lax.fori_loop(0, ng, bwd_group, 0)

    def spread_dg(p, _):
        rg = rgs[p]
        acc = jnp.zeros((top, TOK), F32)
        for e in range(el):
            ef = (e0 + e).astype(F32)
            acc = acc + jnp.where(rg[:top] == ef, jnp.broadcast_to(dgm[p, e:e + 1, :], (top, TOK)), 0.0)
        dgo[p] = acc
        return 0

    lax.fori_loop(0, NP, spread_dg, 0)
    rs_fin(0, yacc, y_ref)
    dg_copies = [remote(dgo.at[blk(*to)], dgr.at[n], dg_ss.at[n], dg_rs.at[n], to) for n, to in enumerate(peers)]
    for c in dg_copies:
        c.start()
    part_copies = []
    for n in range(4):
        dd_copy(1, dxacc, n).wait_recv()
        b = blk(*ORDER[n], 0)
        dxacc[b] += rd[n]
        c = pltpu.make_async_copy(dxacc.at[b], (sd_hbm, sx_hbm, sy_hbm, ka_hbm)[n], psem.at[n])
        c.start()
        part_copies.append(c)
    total = dgo[me]
    for n, c in enumerate(dg_copies):
        c.wait_recv()
        total = total + dgr[n]
    dg_ref[...] = total

    ag_drain(0, xs)
    ag_drain(1, dys)
    rs_drain(0, yacc)
    for n in range(4):
        dd_copy(1, dxacc, n).wait_send()
    for c in part_copies:
        c.wait()
    for c in rg_copies + dg_copies:
        c.wait_send()
    for c in out_copies:
        c.wait()
    a_copy(ng - 1).wait()
    duv_copy(ng - 1).wait()


def grad_kernel(el, y_ref, dg_ref, xa_hbm, dya_hbm, cm, gm, a_hbm, duv_hbm, xef_hbm, dof_hbm,
                yo_ref, dgo_ref, gw1_hbm, gw3_hbm, gw2_hbm,
                xs, dys, xe_s, do_s, a_s, duv_s, g1b, g3b, g2b, lsem, isem, gsem):
    ng = el // GRP
    npair = GRP // PAIR
    ff = a_s.shape[3]

    def inputs(g):
        slot = lax.rem(g, 2)
        return [pltpu.make_async_copy(a_hbm.at[ds(g, GRP)], a_s.at[slot], isem.at[0, slot]),
                pltpu.make_async_copy(duv_hbm.at[ds(g, GRP)], duv_s.at[slot], isem.at[1, slot])]

    def outputs(m):
        slot = lax.rem(m, NOUT)
        return [pltpu.make_async_copy(v.at[slot], h.at[ds(m, PAIR)], gsem.at[n, slot])
                for n, (h, v) in enumerate(((gw1_hbm, g1b), (gw3_hbm, g3b), (gw2_hbm, g2b)))]

    heads = [pltpu.make_async_copy(xef_hbm, xe_s.at[0], lsem.at[2]), pltpu.make_async_copy(dof_hbm, do_s.at[0], lsem.at[3])]
    loads = [pltpu.make_async_copy(xa_hbm, xs, lsem.at[0]), pltpu.make_async_copy(dya_hbm, dys, lsem.at[1])]
    for c in heads + inputs(0) + loads:
        c.start()
    yo_ref[...] = y_ref[...]
    dgo_ref[...] = dg_ref[...]

    def gather(g, q):
        slot = lax.rem(g, 2)

        def store(j, rows, val):
            xe_s[slot, j, rows, :] = val

        def store_scaled(j, rows, val):
            do_s[slot, j, rows, :] = val
        gather_pair(cm, g, q, xs, store)
        gather_dy_pair(cm, gm, g, q, dys, None, store_scaled)

    def core(g, r):
        slot = lax.rem(g, 2)
        o = lax.rem(g * npair + r, NOUT)
        for k in range(PAIR):
            i = r * PAIR + k
            g13 = tn(xe_s[slot, i], duv_s[slot, i])
            g1b[o, k] = g13[:, :ff]
            g3b[o, k] = g13[:, ff:]
            g2b[o, k] = tn(a_s[slot, i], do_s[slot, i])

    def finish(g, r):
        for c in outputs(g * npair + r):
            c.start()

    for c in heads + inputs(0):
        c.wait()
    for c in inputs(1):
        c.start()
    for r in range(npair):
        if r == 1:
            for c in loads:
                c.wait()
        if r == NOUT:
            for c in outputs(0):
                c.wait()
        core(0, r)
        for q in ((), (0, 1), (2,), (3,))[r]:
            gather(1, q)
        finish(0, r)

    def group(g, _):
        for c in inputs(g):
            c.wait()

        @pl.when(g + 1 < ng)
        def _():
            for c in inputs(g + 1):
                c.start()

        def step(r, _):
            for c in outputs(g * npair + r - NOUT):
                c.wait()
            core(g, r)
            gather(g + 1, r)
            finish(g, r)
            return 0

        def last(r, _):
            for c in outputs(g * npair + r - NOUT):
                c.wait()
            core(g, r)
            finish(g, r)
            return 0

        @pl.when(g + 1 < ng)
        def _():
            lax.fori_loop(0, npair, step, 0)

        @pl.when(g + 1 == ng)
        def _():
            lax.fori_loop(0, npair, last, 0)
        return 0

    lax.fori_loop(1, ng, group, 0)
    for m in range(NOUT):
        for c in outputs(ng * npair - NOUT + m):
            c.wait()


def solution(mesh):
    grp = ('row', 'col')
    tspec = P(('dp', 'row', 'col'), None)
    wspec = P(grp, None, None)
    gspec = P(('dp', 'row', 'col'), None, None)

    def local(x, ridx, gates, w1, w3, w2, dy):
        tok, d = x.shape
        top = ridx.shape[1]
        el, _, ff = w1.shape
        anyspec = pl.BlockSpec(memory_space=pl.ANY)
        vm = pl.BlockSpec(memory_space=pltpu.VMEM)
        sds = jax.ShapeDtypeStruct
        dma = pltpu.SemaphoreType.DMA
        y, dg, sd, sx, sy, ka, xa, dya, cm, gm, duv, a, xef, dof = pl.pallas_call(
            functools.partial(main_kernel, el),
            in_specs=[anyspec, anyspec, vm, vm, anyspec, anyspec, anyspec],
            out_specs=[vm, vm] + [anyspec] * 12,
            out_shape=[
                sds((tok, d), BF16), sds((top, tok), F32)] + [sds((tok, d), F32)] * 4 + [
                sds((NP, tok, d), BF16), sds((NP, tok, d), BF16),
                sds((NP, el, tok), F32), sds((NP, el, tok), F32),
                sds((el, NROW, 2 * ff), BF16), sds((el, NROW, ff), BF16),
                sds((GRP, NROW, d), BF16), sds((GRP, NROW, d), BF16),
            ],
            scratch_shapes=[
                pltpu.VMEM((NP, tok, d), BF16),
                pltpu.VMEM((NP, tok, d), BF16),
                pltpu.VMEM((NP, 2 * top, tok), F32),
                pltpu.VMEM((GRP, NROW, d), BF16),
                pltpu.VMEM((GRP, NROW, d), BF16),
                pltpu.VMEM((GRP, NROW, 1), F32),
                pltpu.VMEM((GRP, NP * PAD, d), BF16),
                pltpu.VMEM((el, NROW, 2 * ff), BF16),
                pltpu.VMEM((GRP, NROW, ff), BF16),
                pltpu.VMEM((NP, tok, d), F32),
                pltpu.VMEM((NP, tok, d), F32),
                pltpu.VMEM((NP, el, tok), F32),
                pltpu.VMEM((NP, el, tok), F32),
                pltpu.VMEM((NP, el, tok), F32),
                pltpu.VMEM((NP, top, tok), F32),
                pltpu.VMEM((NP - 1, top, tok), F32),
                pltpu.VMEM((NBUF, d, ff), BF16),
                pltpu.VMEM((NBUF, d, ff), BF16),
                pltpu.VMEM((NBUF, ff, d), BF16),
                pltpu.VMEM((4, tok, d), F32),
                pltpu.VMEM((1, 4, tok // 2, d), F32),
                pltpu.VMEM((1, 2, tok // 2, d), F32),
                dma((3, NBUF)), dma((2,)), dma((8,)), dma((4,)), pltpu.SemaphoreType.REGULAR,
                dma((NP - 1,)), dma((NP - 1,)),
                dma((2, 14)), dma((2, 14)),
                dma((2, 4)), dma((2, 4)),
                dma((1, 4)), dma((1, 4)),
                dma((1, 2)), dma((1, 2)),
                dma((NP - 1,)), dma((NP - 1,)),
            ],
            compiler_params=pltpu.CompilerParams(
                collective_id=0, has_side_effects=True, vmem_limit_bytes=67_000_000),
            cost_estimate=pl.CostEstimate(flops=40_000_000_000, bytes_accessed=160_000_000, transcendentals=0),
        )(x, dy, ridx.T, gates.T, w1, w3, w2)

        def perm(fy, fx):
            out = []
            for p in range(NP):
                yy, xx, cc = p // 4, (p // 2) % 2, p % 2
                out.append((p, (yy ^ fy) * 4 + (xx ^ fx) * 2 + cc))
            return out

        rd = lax.ppermute(sd, grp, perm(1, 1))
        rx = lax.ppermute(sx, grp, perm(0, 1))
        ry = lax.ppermute(sy, grp, perm(1, 0))
        y, dg, gw1, gw3, gw2 = pl.pallas_call(
            functools.partial(grad_kernel, el),
            in_specs=[vm, vm, anyspec, anyspec, vm, vm] + [anyspec] * 4,
            out_specs=[vm, vm, anyspec, anyspec, anyspec],
            out_shape=[sds((tok, d), BF16), sds((top, tok), F32), sds((el, d, ff), F32), sds((el, d, ff), F32), sds((el, ff, d), F32)],
            scratch_shapes=[
                pltpu.VMEM((NP, tok, d), BF16),
                pltpu.VMEM((NP, tok, d), BF16),
                pltpu.VMEM((2, GRP, NROW, d), BF16),
                pltpu.VMEM((2, GRP, NROW, d), BF16),
                pltpu.VMEM((2, GRP, NROW, ff), BF16),
                pltpu.VMEM((2, GRP, NROW, 2 * ff), BF16),
                pltpu.VMEM((NOUT, PAIR, d, ff), F32),
                pltpu.VMEM((NOUT, PAIR, d, ff), F32),
                pltpu.VMEM((NOUT, PAIR, ff, d), F32),
                dma((4,)), dma((2, 2)), dma((3, NOUT)),
            ],
            compiler_params=pltpu.CompilerParams(vmem_limit_bytes=56_000_000),
            cost_estimate=pl.CostEstimate(flops=40_000_000_000, bytes_accessed=160_000_000, transcendentals=0),
        )(y, dg, xa, dya, cm, gm, a, duv, xef, dof)
        dx = (ka + rx + ry + rd).astype(BF16)
        return y, dx, dg.T, gw1, gw3, gw2

    return jax.shard_map(local, mesh=mesh, in_specs=(tspec, tspec, tspec, wspec, wspec, wspec, tspec), out_specs=(tspec, tspec, tspec, gspec, gspec, gspec), check_vma=False)
```

```python
import functools

import jax
import jax.numpy as jnp
from jax import lax
from jax.experimental import pallas as pl
from jax.experimental.pallas import tpu as pltpu
from jax.sharding import PartitionSpec as P

F32 = jnp.float32
BF16 = jnp.bfloat16
MESH = pl.DeviceIdType.MESH
NP = 8
TOK = 256
HALF = TOK // 2
CAP = 24
PAD = 32
GRP = 8
NROW = NP * CAP
NBUF = 8
PAIR = 2
NOUT = 3


def nt(a, b):
    return lax.dot_general(a, b, (((1,), (1,)), ((), ())), preferred_element_type=F32)


def nn(a, b):
    return lax.dot_general(a, b, (((1,), (0,)), ((), ())), preferred_element_type=F32)


def tn(a, b):
    return lax.dot_general(a, b, (((0,), (0,)), ((), ())), preferred_element_type=F32)


def onehot(rows, cap):
    n = rows.shape[0]
    it = lax.broadcasted_iota(jnp.int32, (cap, TOK), 0).astype(F32)
    return [jnp.broadcast_to(rows[k:k + 1], (cap, TOK)) == it for k in range(n)]


def ds(i, n):
    return pl.ds(pl.multiple_of(i * n, n), n)


def gather_pair(cm, g, q, src, store):
    res = []
    for h in range(2):
        p = q * 2 + h
        oh = onehot(cm[p, ds(g, GRP), :], CAP)
        oh = jnp.concatenate([jnp.where(m, 1.0, 0.0) for m in oh], axis=0).astype(BF16)
        res.append(nn(oh, src[p]))
    for k in range(GRP):
        blk = jnp.concatenate([r[k * CAP:(k + 1) * CAP] for r in res], axis=0)
        store(k, ds(q, 2 * CAP), blk.astype(BF16))


def gather_dy_pair(cm, gm, g, q, src, store, store_scaled):
    res, scaled = [], []
    for h in range(2):
        p = q * 2 + h
        oh = onehot(cm[p, ds(g, GRP), :], CAP)
        gr = gm[p, ds(g, GRP), :]
        col = jnp.concatenate(
            [jnp.sum(jnp.where(m, jnp.broadcast_to(gr[k:k + 1], (CAP, TOK)), 0.0), axis=1, keepdims=True)
             for k, m in enumerate(oh)], axis=0)
        oh = jnp.concatenate([jnp.where(m, 1.0, 0.0) for m in oh], axis=0).astype(BF16)
        r = nn(oh, src[p])
        res.append(r)
        scaled.append(col * r)
    for parts, put in ((res, store), (scaled, store_scaled)):
        if put is None:
            continue
        for k in range(GRP):
            blk = jnp.concatenate([r[k * CAP:(k + 1) * CAP] for r in parts], axis=0)
            put(k, ds(q, 2 * CAP), blk.astype(BF16))


def main_kernel(el, x_hbm, dy_hbm, id_ref, gate_ref, w1_hbm, w3_hbm, w2_hbm,
                y_ref, dg_ref, sd_hbm, sx_hbm, sy_hbm, ka_hbm, xa_hbm, dya_hbm, cm_hbm, gm_hbm, duv_hbm, a_hbm, xef_hbm, dof_hbm,
                xs, dys, rgs, xe_s, do_s, dgc_s, o_s, uv_s, a_s, yacc, dxacc, cm, gm, dgm, dgo, dgr,
                w1b, w3b, w2b, rd, r1, r2,
                wsem, lsem, osem, psem, credit, rg_ss, rg_rs, ag_ss, ag_rs, dd_ss, dd_rs, s1_ss, s1_rs, s2_ss, s2_rs, dg_ss, dg_rs):
    ng = el // GRP
    ff = w2b.shape[1]
    Z = lax.axis_index('dp')
    Y = lax.axis_index('row')
    col = lax.axis_index('col')
    X = lax.div(col, 2)
    C = lax.rem(col, 2)
    me = Y * 4 + col
    e0 = me * el

    def pos(fy, fx, fc):
        return (1 - Y if fy else Y), (1 - X if fx else X), (1 - C if fc else C)

    def blk(fy, fx, fc):
        yy, xx, cc = pos(fy, fx, fc)
        return yy * 4 + xx * 2 + cc

    def dev(fy, fx, fc):
        yy, xx, cc = pos(fy, fx, fc)
        return (Z, yy, xx * 2 + cc)

    peers = [(a, b, c) for a in range(2) for b in range(2) for c in range(2)][1:]

    def remote(src, dst, ss, rs, to):
        return pltpu.make_async_remote_copy(src_ref=src, dst_ref=dst, send_sem=ss, recv_sem=rs,
                                            device_id=dev(*to), device_id_type=MESH)

    lx = pltpu.make_async_copy(x_hbm, xs.at[me], lsem.at[0])
    ld = pltpu.make_async_copy(dy_hbm, dys.at[me], lsem.at[1])
    lx.start()
    ld.start()

    def wcopies(e):
        b = lax.rem(e, NBUF)
        k = lax.rem(e, el)
        return [pltpu.make_async_copy(h.at[k], v.at[b], wsem.at[n, b])
                for n, (h, v) in enumerate(((w1_hbm, w1b), (w3_hbm, w3b), (w2_hbm, w2b)))]

    for e in range(NBUF):
        for c in wcopies(e):
            c.start()

    rgs[me] = jnp.concatenate([id_ref[...].astype(F32), gate_ref[...]], axis=0)
    barrier = pltpu.get_barrier_semaphore()
    for to in peers:
        pl.semaphore_signal(barrier, inc=1, device_id=dev(*to), device_id_type=MESH)
    pl.semaphore_wait(barrier, len(peers))

    rg_copies = [remote(rgs.at[me], rgs.at[me], rg_ss.at[n], rg_rs.at[n], to) for n, to in enumerate(peers)]
    for c in rg_copies:
        c.start()

    def half(buf, b, h):
        return buf.at[b, pl.ds(h * HALF, HALF), :]

    XN, YN, DN, PN = (0, 1, 0), (1, 0, 0), (1, 1, 0), (0, 0, 1)
    FIRST = [(0, (0, 0, 0), 0, XN), (1, (0, 0, 0), 1, YN), (2, (0, 0, 0), 1, XN), (3, (0, 0, 0), 0, YN)]
    OWN2 = [(6, (0, 0, 0), 0, PN), (7, (0, 0, 0), 1, PN)]
    FWD = [(4, XN, 0, YN), (5, YN, 1, XN)]
    ARR = {0: (XN, 0), 1: (YN, 1), 2: (XN, 1), 3: (YN, 0), 4: (DN, 0), 5: (DN, 1)}
    ONWARD = {0: 8, 1: 9, 2: 10, 3: 11, 4: 12, 5: 13}

    def ag_copy(t, buf, n, f, h, to):
        r = half(buf, blk(*f), h)
        return remote(r, r, ag_ss.at[t, n], ag_rs.at[t, n], to)

    def ag_recv(t, buf, n, f, h):
        r = half(buf, blk(*f), h)
        remote(r, r, ag_ss.at[t, n], ag_rs.at[t, n], PN).wait_recv()

    def ag_start(t, buf):
        for n, f, h, to in FIRST + OWN2:
            ag_copy(t, buf, n, f, h, to).start()

    def ag_relay(t, buf, ns):
        for n in ns:
            f, h = ARR[n]
            ag_recv(t, buf, n, f, h)
            if n < 2:
                k, ff_, hh, to = FWD[n]
                ag_copy(t, buf, k, ff_, hh, to).start()
            ag_copy(t, buf, ONWARD[n], f, h, PN).start()

    def ag_finish(t, buf):
        for n, h in ((6, 0), (7, 1)):
            ag_recv(t, buf, n, PN, h)
        for n, k in ONWARD.items():
            f, h = ARR[n]
            ag_recv(t, buf, k, (f[0], f[1], 1), h)

    def ag_drain(t, buf):
        for n, f, h, to in FIRST + OWN2 + FWD:
            ag_copy(t, buf, n, f, h, to).wait_send()
        for n, k in ONWARD.items():
            f, h = ARR[n]
            ag_copy(t, buf, k, f, h, PN).wait_send()

    lx.wait()
    ld.wait()
    ag_start(0, xs)

    def zero(p, _):
        yacc[p] = jnp.zeros(yacc.shape[1:], F32)
        dxacc[p] = jnp.zeros(dxacc.shape[1:], F32)
        return 0

    lax.fori_loop(0, NP, zero, 0)

    for n, to in enumerate(peers):
        remote(rgs.at[blk(*to)], rgs.at[blk(*to)], rg_ss.at[n], rg_rs.at[n], to).wait_recv()
    top = rgs.shape[1] // 2
    tr = lax.broadcasted_iota(jnp.int32, (TOK, TOK), 0)
    tc = lax.broadcasted_iota(jnp.int32, (TOK, TOK), 1)
    tri = jnp.where(tr < tc, 1.0, 0.0).astype(BF16)
    ee = (lax.broadcasted_iota(jnp.int32, (el, TOK), 0) + e0).astype(F32)

    def prep(p, _):
        rg = rgs[p]
        m = jnp.zeros((el, TOK), F32)
        gs = jnp.zeros((el, TOK), F32)
        for j in range(top):
            hit = jnp.broadcast_to(rg[j:j + 1], (el, TOK)) == ee
            m = jnp.where(hit, 1.0, m)
            gs = jnp.where(hit, jnp.broadcast_to(rg[top + j:top + j + 1], (el, TOK)), gs)
        rank = nn(m.astype(BF16), tri)
        cm[p] = jnp.where(m > 0.0, rank, -1.0)
        gm[p] = gs
        return 0

    lax.fori_loop(0, NP, prep, 0)

    ag_relay(0, xs, (0, 1, 2, 3))
    ag_start(1, dys)
    ag_relay(0, xs, (4, 5))
    ag_finish(0, xs)
    out_copies = [pltpu.make_async_copy(xs, xa_hbm, osem.at[0]),
                  pltpu.make_async_copy(cm, cm_hbm, osem.at[1]),
                  pltpu.make_async_copy(gm, gm_hbm, osem.at[2]),
                  pltpu.make_async_copy(dys, dya_hbm, osem.at[3])]
    for c in out_copies[:3]:
        c.start()

    def gather_all(g, src):
        def step(q, _):
            def store(k, rows, val):
                xe_s[k, rows, :] = val
            gather_pair(cm, g, q, src, store)
            return 0
        lax.fori_loop(0, NP // 2, step, 0, unroll=4)

    def gather_dy(g):
        def step(q, _):
            def store(k, rows, val):
                xe_s[k, rows, :] = val

            def store_scaled(k, rows, val):
                do_s[k, rows, :] = val
            gather_dy_pair(cm, gm, g, q, dys, store, store_scaled)
            return 0
        lax.fori_loop(0, NP // 2, step, 0, unroll=4)

    def put_rows(i, val):
        zero = jnp.zeros((PAD - CAP, val.shape[1]), F32)
        for p in range(NP):
            o_s[i, p * PAD:(p + 1) * PAD, :] = jnp.concatenate([val[p * CAP:(p + 1) * CAP], zero], axis=0).astype(BF16)

    def take_rows(p):
        return jnp.concatenate([o_s[k, ds(p, PAD), :] for k in range(GRP)], axis=0)

    def combine_y(g):
        def step(p, _):
            oh = onehot(cm[p, ds(g, GRP), :], PAD)
            gr = gm[p, ds(g, GRP), :]
            g1 = gr.astype(BF16).astype(F32)
            rest = gr - g1
            g2 = rest.astype(BF16).astype(F32)
            g3 = rest - g2
            ob = take_rows(p)

            def spread(part):
                return jnp.concatenate(
                    [jnp.where(oh[k], jnp.broadcast_to(part[k:k + 1], (PAD, TOK)), 0.0) for k in range(GRP)],
                    axis=0).astype(BF16)

            gs = jnp.concatenate([spread(g1), spread(g2), spread(g3)], axis=0)
            yacc[p] += tn(gs, jnp.concatenate([ob, ob, ob], axis=0))
            return 0
        lax.fori_loop(0, NP, step, 0, unroll=4)

    def combine_dx(g, cc):
        for j in range(NP // 2):
            p = 2 * j + cc
            oh = onehot(cm[p, ds(g, GRP), :], PAD)
            one = jnp.concatenate([jnp.where(m, 1.0, 0.0) for m in oh], axis=0).astype(BF16)
            dxacc[p] += tn(one, take_rows(p))
            rows = []
            for k in range(GRP):
                db = jnp.broadcast_to(dgc_s[k, ds(p, CAP), :], (CAP, TOK))
                rows.append(jnp.sum(jnp.where(oh[k][:CAP], db, 0.0), axis=0, keepdims=True))
            dgm[p, ds(g, GRP), :] = jnp.concatenate(rows, axis=0)

    def fetch(n):
        for k in range(PAIR):
            for c in wcopies(n + k):
                c.wait()

    def release(n):
        @pl.when(n + NBUF < 2 * el)
        def _():
            for k in range(PAIR):
                for c in wcopies(n + NBUF + k):
                    c.start()

    def w13_of(n):
        b = lax.rem(n, NBUF)
        return jnp.concatenate([w1b[b], w3b[b]], axis=1)

    def w2_of(n):
        return w2b[lax.rem(n, NBUF)]

    def skewed(g, first, base, second):
        npair = GRP // PAIR
        fetch(base)
        first(0)

        def step(r, _):
            fetch(base + r * PAIR)
            second(r - 1)
            first(r)
            release(base + (r - 1) * PAIR)
            return 0

        lax.fori_loop(1, npair, step, 0)
        second(npair - 1)
        release(base + (npair - 1) * PAIR)

    def act(uv):
        u, v = uv[:, :ff], uv[:, ff:]
        sg = jax.nn.sigmoid(u)
        return u, v, sg, (u * sg * v).astype(BF16)

    ORDER = [(1, 1), (0, 1), (1, 0), (0, 0)]
    S1 = [((1, 1), 0, XN), ((1, 1), 1, YN), ((0, 1), 0, XN), ((1, 0), 1, YN)]
    IN1 = [((1, 0), 0), ((0, 1), 1), ((0, 0), 0), ((0, 0), 1)]
    S2 = [YN, XN]

    def dd_copy(t, acc, n):
        fy, fx = ORDER[n]
        return remote(acc.at[blk(fy, fx, 1)], rd.at[n], dd_ss.at[t, n], dd_rs.at[t, n], PN)

    def s1_copy(t, acc, n):
        (fy, fx), h, to = S1[n]
        return remote(half(acc, blk(fy, fx, 0), h), r1.at[t, n], s1_ss.at[t, n], s1_rs.at[t, n], to)

    def s2_copy(t, acc, n):
        (fy, fx), h = IN1[n]
        return remote(half(acc, blk(fy, fx, 0), h), r2.at[t, n], s2_ss.at[t, n], s2_rs.at[t, n], S2[n])

    def rs_start(t, acc):
        for n in range(4):
            dd_copy(t, acc, n).start()

    def rs_mid1(t, acc):
        for n in range(4):
            dd_copy(t, acc, n).wait_recv()
            fy, fx = ORDER[n]
            acc[blk(fy, fx, 0)] += rd[n]
            for k in ((0, 1), (2,), (3,), ())[n]:
                s1_copy(t, acc, k).start()

    def rs_mid2(t, acc):
        for n in range(4):
            s1_copy(t, acc, n).wait_recv()
            (fy, fx), h = IN1[n]
            acc[blk(fy, fx, 0), h * HALF:(h + 1) * HALF, :] += r1[t, n]
            if n < 2:
                s2_copy(t, acc, n).start()

    def rs_fin(t, acc, out):
        for n in range(2):
            s2_copy(t, acc, n).wait_recv()
            rows = slice(n * HALF, (n + 1) * HALF)
            out[rows, :] = (acc[me, rows, :] + r2[t, n]).astype(BF16)

    def rs_drain(t, acc):
        for n in range(4):
            dd_copy(t, acc, n).wait_send()
            s1_copy(t, acc, n).wait_send()
        for n in range(2):
            s2_copy(t, acc, n).wait_send()

    xef_copy = pltpu.make_async_copy(xe_s, xef_hbm, osem.at[6])
    dof_copy = pltpu.make_async_copy(do_s, dof_hbm, osem.at[7])

    def fwd_group(g, _):
        gather_all(g, xs)

        @pl.when(g == 0)
        def _():
            xef_copy.start()

        def f1(r):
            for k in range(PAIR):
                i = r * PAIR + k
                uv_s[g * GRP + i] = nn(xe_s[i], w13_of(g * GRP + i)).astype(BF16)

        def f2(r):
            uvs = [uv_s[g * GRP + r * PAIR + k].astype(F32) for k in range(PAIR)]
            for k in range(PAIR):
                i = r * PAIR + k
                put_rows(i, nn(act(uvs[k])[3], w2_of(g * GRP + i)))

        skewed(g, f1, g * GRP, f2)
        combine_y(g)

        @pl.when(g == 0)
        def _():
            xef_copy.wait()

        @pl.when(g == 0)
        def _():
            ag_relay(1, dys, (0, 1, 2, 3))

        @pl.when(g == 1)
        def _():
            ag_relay(1, dys, (4, 5))

        @pl.when(g == 2)
        def _():
            ag_finish(1, dys)
            out_copies[3].start()
        return 0

    lax.fori_loop(0, ng, fwd_group, 0)

    def duv_copy(g):
        return pltpu.make_async_copy(uv_s.at[ds(g, GRP)], duv_hbm.at[ds(g, GRP)], osem.at[4])

    def a_copy(g):
        return pltpu.make_async_copy(a_s, a_hbm.at[ds(g, GRP)], osem.at[5])

    def bwd_group(g, _):
        gather_dy(g)

        @pl.when(g == 0)
        def _():
            dof_copy.start()

        @pl.when(g == 0)
        def _():
            rs_start(0, yacc)

        def b1(r):
            uvs = [uv_s[g * GRP + r * PAIR + k] for k in range(PAIR)]
            for k in range(PAIR):
                i = r * PAIR + k
                e = g * GRP + i
                w2 = w2_of(el + e)
                da = nt(do_s[i], w2)
                u, v, sg, a = act(uvs[k].astype(F32))
                a_s[i] = a
                of = nn(a, w2).astype(BF16).astype(F32)
                dgc_s[i] = jnp.sum(xe_s[i].astype(F32) * of, axis=1, keepdims=True)
                du = (da * v * sg * (1.0 + u * (1.0 - sg))).astype(BF16)
                dv = (da * u * sg).astype(BF16)
                uv_s[e] = jnp.concatenate([du, dv], axis=1)

        def b2(r):
            duvs = [uv_s[g * GRP + r * PAIR + k] for k in range(PAIR)]
            for k in range(PAIR):
                i = r * PAIR + k
                put_rows(i, nt(duvs[k], w13_of(el + g * GRP + i)))

        @pl.when(g > 0)
        def _():
            a_copy(g - 1).wait()
            duv_copy(g - 1).wait()

        skewed(g, b1, el + g * GRP, b2)
        a_copy(g).start()
        duv_copy(g).start()
        combine_dx(g, 1 - C)

        @pl.when(g == ng - 1)
        def _():
            pl.semaphore_wait(credit, 1)
            rs_start(1, dxacc)
        combine_dx(g, C)

        @pl.when(g == 0)
        def _():
            dof_copy.wait()

        @pl.when(g == 1)
        def _():
            rs_mid1(0, yacc)
            pl.semaphore_signal(credit, inc=1, device_id=dev(*PN), device_id_type=MESH)

        @pl.when(g == ng - 1)
        def _():
            rs_mid2(0, yacc)
        return 0

    lax.fori_loop(0, ng, bwd_group, 0)

    def spread_dg(p, _):
        rg = rgs[p]
        acc = jnp.zeros((top, TOK), F32)
        for e in range(el):
            ef = (e0 + e).astype(F32)
            acc = acc + jnp.where(rg[:top] == ef, jnp.broadcast_to(dgm[p, e:e + 1, :], (top, TOK)), 0.0)
        dgo[p] = acc
        return 0

    lax.fori_loop(0, NP, spread_dg, 0)
    rs_fin(0, yacc, y_ref)
    dg_copies = [remote(dgo.at[blk(*to)], dgr.at[n], dg_ss.at[n], dg_rs.at[n], to) for n, to in enumerate(peers)]
    for c in dg_copies:
        c.start()
    part_copies = []
    for n in range(4):
        dd_copy(1, dxacc, n).wait_recv()
        b = blk(*ORDER[n], 0)
        dxacc[b] += rd[n]
        c = pltpu.make_async_copy(dxacc.at[b], (sd_hbm, sx_hbm, sy_hbm, ka_hbm)[n], psem.at[n])
        c.start()
        part_copies.append(c)
    total = dgo[me]
    for n, c in enumerate(dg_copies):
        c.wait_recv()
        total = total + dgr[n]
    dg_ref[...] = total

    ag_drain(0, xs)
    ag_drain(1, dys)
    rs_drain(0, yacc)
    for n in range(4):
        dd_copy(1, dxacc, n).wait_send()
    for c in part_copies:
        c.wait()
    for c in rg_copies + dg_copies:
        c.wait_send()
    for c in out_copies:
        c.wait()
    a_copy(ng - 1).wait()
    duv_copy(ng - 1).wait()


def grad_kernel(el, y_hbm, dg_hbm, xa_hbm, dya_hbm, cm_hbm, gm_hbm, a_hbm, duv_hbm, xef_hbm, dof_hbm,
                yo_ref, dgo_ref, gw1_hbm, gw3_hbm, gw2_hbm,
                xs, dys, cm, gm, xe_s, do_s, a_s, duv_s, g1b, g3b, g2b, lsem, isem, gsem):
    ng = el // GRP
    npair = GRP // PAIR
    ff = a_s.shape[3]

    def inputs(g):
        slot = lax.rem(g, 2)
        return [pltpu.make_async_copy(a_hbm.at[ds(g, GRP)], a_s.at[slot], isem.at[0, slot]),
                pltpu.make_async_copy(duv_hbm.at[ds(g, GRP)], duv_s.at[slot], isem.at[1, slot])]

    def outputs(m):
        slot = lax.rem(m, NOUT)
        return [pltpu.make_async_copy(v.at[slot], h.at[ds(m, PAIR)], gsem.at[n, slot])
                for n, (h, v) in enumerate(((gw1_hbm, g1b), (gw3_hbm, g3b), (gw2_hbm, g2b)))]

    heads = [pltpu.make_async_copy(xef_hbm, xe_s.at[0], lsem.at[2]), pltpu.make_async_copy(dof_hbm, do_s.at[0], lsem.at[3])]
    loads = [pltpu.make_async_copy(h, v, lsem.at[n]) for n, h, v in (
        (0, xa_hbm, xs), (1, dya_hbm, dys), (4, cm_hbm, cm), (5, gm_hbm, gm), (6, y_hbm, yo_ref), (7, dg_hbm, dgo_ref))]
    for c in heads + inputs(0) + loads:
        c.start()

    def gather(g, q):
        slot = lax.rem(g, 2)

        def store(j, rows, val):
            xe_s[slot, j, rows, :] = val

        def store_scaled(j, rows, val):
            do_s[slot, j, rows, :] = val
        gather_pair(cm, g, q, xs, store)
        gather_dy_pair(cm, gm, g, q, dys, None, store_scaled)

    def core(g, r):
        slot = lax.rem(g, 2)
        o = lax.rem(g * npair + r, NOUT)
        for k in range(PAIR):
            i = r * PAIR + k
            g13 = tn(xe_s[slot, i], duv_s[slot, i])
            g1b[o, k] = g13[:, :ff]
            g3b[o, k] = g13[:, ff:]
            g2b[o, k] = tn(a_s[slot, i], do_s[slot, i])

    def finish(g, r):
        for c in outputs(g * npair + r):
            c.start()

    for c in heads + inputs(0):
        c.wait()
    for c in inputs(1):
        c.start()
    for r in range(npair):
        if r == 1:
            for c in loads:
                c.wait()
        if r == NOUT:
            for c in outputs(0):
                c.wait()
        core(0, r)
        for q in ((), (0, 1), (2,), (3,))[r]:
            gather(1, q)
        finish(0, r)

    def group(g, _):
        for c in inputs(g):
            c.wait()

        @pl.when(g + 1 < ng)
        def _():
            for c in inputs(g + 1):
                c.start()

        def step(r, _):
            for c in outputs(g * npair + r - NOUT):
                c.wait()
            core(g, r)
            gather(g + 1, r)
            finish(g, r)
            return 0

        def last(r, _):
            for c in outputs(g * npair + r - NOUT):
                c.wait()
            core(g, r)
            finish(g, r)
            return 0

        @pl.when(g + 1 < ng)
        def _():
            lax.fori_loop(0, npair, step, 0)

        @pl.when(g + 1 == ng)
        def _():
            lax.fori_loop(0, npair, last, 0)
        return 0

    lax.fori_loop(1, ng, group, 0)
    for m in range(NOUT):
        for c in outputs(ng * npair - NOUT + m):
            c.wait()


def solution(mesh):
    grp = ('row', 'col')
    tspec = P(('dp', 'row', 'col'), None)
    wspec = P(grp, None, None)
    gspec = P(('dp', 'row', 'col'), None, None)

    def local(x, ridx, gates, w1, w3, w2, dy):
        tok, d = x.shape
        top = ridx.shape[1]
        el, _, ff = w1.shape
        anyspec = pl.BlockSpec(memory_space=pl.ANY)
        vm = pl.BlockSpec(memory_space=pltpu.VMEM)
        sds = jax.ShapeDtypeStruct
        dma = pltpu.SemaphoreType.DMA
        y, dg, sd, sx, sy, ka, xa, dya, cm, gm, duv, a, xef, dof = pl.pallas_call(
            functools.partial(main_kernel, el),
            in_specs=[anyspec, anyspec, vm, vm, anyspec, anyspec, anyspec],
            out_specs=[vm, vm] + [anyspec] * 12,
            out_shape=[
                sds((tok, d), BF16), sds((top, tok), F32)] + [sds((tok, d), F32)] * 4 + [
                sds((NP, tok, d), BF16), sds((NP, tok, d), BF16),
                sds((NP, el, tok), F32), sds((NP, el, tok), F32),
                sds((el, NROW, 2 * ff), BF16), sds((el, NROW, ff), BF16),
                sds((GRP, NROW, d), BF16), sds((GRP, NROW, d), BF16),
            ],
            scratch_shapes=[
                pltpu.VMEM((NP, tok, d), BF16),
                pltpu.VMEM((NP, tok, d), BF16),
                pltpu.VMEM((NP, 2 * top, tok), F32),
                pltpu.VMEM((GRP, NROW, d), BF16),
                pltpu.VMEM((GRP, NROW, d), BF16),
                pltpu.VMEM((GRP, NROW, 1), F32),
                pltpu.VMEM((GRP, NP * PAD, d), BF16),
                pltpu.VMEM((el, NROW, 2 * ff), BF16),
                pltpu.VMEM((GRP, NROW, ff), BF16),
                pltpu.VMEM((NP, tok, d), F32),
                pltpu.VMEM((NP, tok, d), F32),
                pltpu.VMEM((NP, el, tok), F32),
                pltpu.VMEM((NP, el, tok), F32),
                pltpu.VMEM((NP, el, tok), F32),
                pltpu.VMEM((NP, top, tok), F32),
                pltpu.VMEM((NP - 1, top, tok), F32),
                pltpu.VMEM((NBUF, d, ff), BF16),
                pltpu.VMEM((NBUF, d, ff), BF16),
                pltpu.VMEM((NBUF, ff, d), BF16),
                pltpu.VMEM((4, tok, d), F32),
                pltpu.VMEM((1, 4, tok // 2, d), F32),
                pltpu.VMEM((1, 2, tok // 2, d), F32),
                dma((3, NBUF)), dma((2,)), dma((8,)), dma((4,)), pltpu.SemaphoreType.REGULAR,
                dma((NP - 1,)), dma((NP - 1,)),
                dma((2, 14)), dma((2, 14)),
                dma((2, 4)), dma((2, 4)),
                dma((1, 4)), dma((1, 4)),
                dma((1, 2)), dma((1, 2)),
                dma((NP - 1,)), dma((NP - 1,)),
            ],
            compiler_params=pltpu.CompilerParams(
                collective_id=0, has_side_effects=True, vmem_limit_bytes=67_000_000),
            cost_estimate=pl.CostEstimate(flops=40_000_000_000, bytes_accessed=160_000_000, transcendentals=0),
        )(x, dy, ridx.T, gates.T, w1, w3, w2)

        def perm(fy, fx):
            out = []
            for p in range(NP):
                yy, xx, cc = p // 4, (p // 2) % 2, p % 2
                out.append((p, (yy ^ fy) * 4 + (xx ^ fx) * 2 + cc))
            return out

        rd = lax.ppermute(sd, grp, perm(1, 1))
        rx = lax.ppermute(sx, grp, perm(0, 1))
        ry = lax.ppermute(sy, grp, perm(1, 0))
        y, dg, gw1, gw3, gw2 = pl.pallas_call(
            functools.partial(grad_kernel, el),
            in_specs=[anyspec] * 10,
            out_specs=[vm, vm, anyspec, anyspec, anyspec],
            out_shape=[sds((tok, d), BF16), sds((top, tok), F32), sds((el, d, ff), F32), sds((el, d, ff), F32), sds((el, ff, d), F32)],
            scratch_shapes=[
                pltpu.VMEM((NP, tok, d), BF16),
                pltpu.VMEM((NP, tok, d), BF16),
                pltpu.VMEM((NP, el, tok), F32),
                pltpu.VMEM((NP, el, tok), F32),
                pltpu.VMEM((2, GRP, NROW, d), BF16),
                pltpu.VMEM((2, GRP, NROW, d), BF16),
                pltpu.VMEM((2, GRP, NROW, ff), BF16),
                pltpu.VMEM((2, GRP, NROW, 2 * ff), BF16),
                pltpu.VMEM((NOUT, PAIR, d, ff), F32),
                pltpu.VMEM((NOUT, PAIR, d, ff), F32),
                pltpu.VMEM((NOUT, PAIR, ff, d), F32),
                dma((8,)), dma((2, 2)), dma((3, NOUT)),
            ],
            compiler_params=pltpu.CompilerParams(vmem_limit_bytes=56_000_000),
            cost_estimate=pl.CostEstimate(flops=40_000_000_000, bytes_accessed=160_000_000, transcendentals=0),
        )(y, dg, xa, dya, cm, gm, a, duv, xef, dof)
        dx = (ka + rx + ry + rd).astype(BF16)
        return y, dx, dg.T, gw1, gw3, gw2

    return jax.shard_map(local, mesh=mesh, in_specs=(tspec, tspec, tspec, wspec, wspec, wspec, tspec), out_specs=(tspec, tspec, tspec, gspec, gspec, gspec), check_vma=False)
```

```python
import functools

import jax
import jax.numpy as jnp
from jax import lax
from jax.experimental import pallas as pl
from jax.experimental.pallas import tpu as pltpu
from jax.sharding import PartitionSpec as P

F32 = jnp.float32
BF16 = jnp.bfloat16
MESH = pl.DeviceIdType.MESH
NP = 8
TOK = 256
HALF = TOK // 2
CAP = 24
PAD = 32
GRP = 8
NROW = NP * CAP
NBUF = 8
PAIR = 2
NOUT = 3


def nt(a, b):
    return lax.dot_general(a, b, (((1,), (1,)), ((), ())), preferred_element_type=F32)


def nn(a, b):
    return lax.dot_general(a, b, (((1,), (0,)), ((), ())), preferred_element_type=F32)


def tn(a, b):
    return lax.dot_general(a, b, (((0,), (0,)), ((), ())), preferred_element_type=F32)


def onehot(rows, cap):
    n = rows.shape[0]
    it = lax.broadcasted_iota(jnp.int32, (cap, TOK), 0).astype(F32)
    return [jnp.broadcast_to(rows[k:k + 1], (cap, TOK)) == it for k in range(n)]


def ds(i, n):
    return pl.ds(pl.multiple_of(i * n, n), n)


def gather_pair(cm, g, q, src, store):
    res = []
    for h in range(2):
        p = q * 2 + h
        oh = onehot(cm[p, ds(g, GRP), :], CAP)
        oh = jnp.concatenate([jnp.where(m, 1.0, 0.0) for m in oh], axis=0).astype(BF16)
        res.append(nn(oh, src[p]))
    for k in range(GRP):
        blk = jnp.concatenate([r[k * CAP:(k + 1) * CAP] for r in res], axis=0)
        store(k, ds(q, 2 * CAP), blk.astype(BF16))


def gather_dy_pair(cm, gm, g, q, src, store, store_scaled):
    res, scaled = [], []
    for h in range(2):
        p = q * 2 + h
        oh = onehot(cm[p, ds(g, GRP), :], CAP)
        gr = gm[p, ds(g, GRP), :]
        col = jnp.concatenate(
            [jnp.sum(jnp.where(m, jnp.broadcast_to(gr[k:k + 1], (CAP, TOK)), 0.0), axis=1, keepdims=True)
             for k, m in enumerate(oh)], axis=0)
        oh = jnp.concatenate([jnp.where(m, 1.0, 0.0) for m in oh], axis=0).astype(BF16)
        r = nn(oh, src[p])
        res.append(r)
        scaled.append(col * r)
    for parts, put in ((res, store), (scaled, store_scaled)):
        if put is None:
            continue
        for k in range(GRP):
            blk = jnp.concatenate([r[k * CAP:(k + 1) * CAP] for r in parts], axis=0)
            put(k, ds(q, 2 * CAP), blk.astype(BF16))


def main_kernel(el, x_hbm, dy_hbm, id_ref, gate_ref, w1_hbm, w3_hbm, w2_hbm,
                y_ref, dg_ref, sd_hbm, sx_hbm, sy_hbm, ka_hbm, xa_hbm, dya_hbm, cm_hbm, gm_hbm, duv_hbm, a_hbm, xef_hbm, dof_hbm,
                xs, dys, rgs, xe_s, do_s, dgc_s, o_s, uv_s, a_s, yacc, dxacc, cm, gm, dgm, dgo, dgr,
                w1b, w3b, w2b, rd, r1, r2,
                wsem, lsem, osem, psem, credit, rg_ss, rg_rs, ag_ss, ag_rs, dd_ss, dd_rs, s1_ss, s1_rs, s2_ss, s2_rs, dg_ss, dg_rs):
    ng = el // GRP
    ff = w2b.shape[1]
    Z = lax.axis_index('dp')
    Y = lax.axis_index('row')
    col = lax.axis_index('col')
    X = lax.div(col, 2)
    C = lax.rem(col, 2)
    me = Y * 4 + col
    e0 = me * el

    def pos(fy, fx, fc):
        return (1 - Y if fy else Y), (1 - X if fx else X), (1 - C if fc else C)

    def blk(fy, fx, fc):
        yy, xx, cc = pos(fy, fx, fc)
        return yy * 4 + xx * 2 + cc

    def dev(fy, fx, fc):
        yy, xx, cc = pos(fy, fx, fc)
        return (Z, yy, xx * 2 + cc)

    peers = [(a, b, c) for a in range(2) for b in range(2) for c in range(2)][1:]

    def remote(src, dst, ss, rs, to):
        return pltpu.make_async_remote_copy(src_ref=src, dst_ref=dst, send_sem=ss, recv_sem=rs,
                                            device_id=dev(*to), device_id_type=MESH)

    lx = pltpu.make_async_copy(x_hbm, xs.at[me], lsem.at[0])
    ld = pltpu.make_async_copy(dy_hbm, dys.at[me], lsem.at[1])
    lx.start()
    ld.start()

    def wcopies(e):
        b = lax.rem(e, NBUF)
        k = lax.rem(e, el)
        return [pltpu.make_async_copy(h.at[k], v.at[b], wsem.at[n, b])
                for n, (h, v) in enumerate(((w1_hbm, w1b), (w3_hbm, w3b), (w2_hbm, w2b)))]

    for e in range(NBUF):
        for c in wcopies(e):
            c.start()

    rgs[me] = jnp.concatenate([id_ref[...].astype(F32), gate_ref[...]], axis=0)
    barrier = pltpu.get_barrier_semaphore()
    for to in peers:
        pl.semaphore_signal(barrier, inc=1, device_id=dev(*to), device_id_type=MESH)
    pl.semaphore_wait(barrier, len(peers))

    rg_copies = [remote(rgs.at[me], rgs.at[me], rg_ss.at[n], rg_rs.at[n], to) for n, to in enumerate(peers)]
    for c in rg_copies:
        c.start()

    def half(buf, b, h):
        return buf.at[b, pl.ds(h * HALF, HALF), :]

    XN, YN, DN, PN = (0, 1, 0), (1, 0, 0), (1, 1, 0), (0, 0, 1)
    FIRST = [(0, (0, 0, 0), 0, XN), (1, (0, 0, 0), 1, YN), (2, (0, 0, 0), 1, XN), (3, (0, 0, 0), 0, YN)]
    OWN2 = [(6, (0, 0, 0), 0, PN), (7, (0, 0, 0), 1, PN)]
    FWD = [(4, XN, 0, YN), (5, YN, 1, XN)]
    ARR = {0: (XN, 0), 1: (YN, 1), 2: (XN, 1), 3: (YN, 0), 4: (DN, 0), 5: (DN, 1)}
    ONWARD = {0: 8, 1: 9, 2: 10, 3: 11, 4: 12, 5: 13}

    def ag_copy(t, buf, n, f, h, to):
        r = half(buf, blk(*f), h)
        return remote(r, r, ag_ss.at[t, n], ag_rs.at[t, n], to)

    def ag_recv(t, buf, n, f, h):
        r = half(buf, blk(*f), h)
        remote(r, r, ag_ss.at[t, n], ag_rs.at[t, n], PN).wait_recv()

    def ag_start(t, buf):
        for n, f, h, to in FIRST + OWN2:
            ag_copy(t, buf, n, f, h, to).start()

    def ag_relay(t, buf, ns):
        for n in ns:
            f, h = ARR[n]
            ag_recv(t, buf, n, f, h)
            if n < 2:
                k, ff_, hh, to = FWD[n]
                ag_copy(t, buf, k, ff_, hh, to).start()
            ag_copy(t, buf, ONWARD[n], f, h, PN).start()

    def ag_finish(t, buf):
        for n, h in ((6, 0), (7, 1)):
            ag_recv(t, buf, n, PN, h)
        for n, k in ONWARD.items():
            f, h = ARR[n]
            ag_recv(t, buf, k, (f[0], f[1], 1), h)

    def ag_drain(t, buf):
        for n, f, h, to in FIRST + OWN2 + FWD:
            ag_copy(t, buf, n, f, h, to).wait_send()
        for n, k in ONWARD.items():
            f, h = ARR[n]
            ag_copy(t, buf, k, f, h, PN).wait_send()

    lx.wait()
    ld.wait()
    ag_start(0, xs)

    def zero(p, _):
        yacc[p] = jnp.zeros(yacc.shape[1:], F32)
        dxacc[p] = jnp.zeros(dxacc.shape[1:], F32)
        return 0

    lax.fori_loop(0, NP, zero, 0)

    for n, to in enumerate(peers):
        remote(rgs.at[blk(*to)], rgs.at[blk(*to)], rg_ss.at[n], rg_rs.at[n], to).wait_recv()
    top = rgs.shape[1] // 2
    tr = lax.broadcasted_iota(jnp.int32, (TOK, TOK), 0)
    tc = lax.broadcasted_iota(jnp.int32, (TOK, TOK), 1)
    tri = jnp.where(tr < tc, 1.0, 0.0).astype(BF16)
    ee = (lax.broadcasted_iota(jnp.int32, (el, TOK), 0) + e0).astype(F32)

    def prep(p, _):
        rg = rgs[p]
        m = jnp.zeros((el, TOK), F32)
        gs = jnp.zeros((el, TOK), F32)
        for j in range(top):
            hit = jnp.broadcast_to(rg[j:j + 1], (el, TOK)) == ee
            m = jnp.where(hit, 1.0, m)
            gs = jnp.where(hit, jnp.broadcast_to(rg[top + j:top + j + 1], (el, TOK)), gs)
        rank = nn(m.astype(BF16), tri)
        cm[p] = jnp.where(m > 0.0, rank, -1.0)
        gm[p] = gs
        return 0

    lax.fori_loop(0, NP, prep, 0)

    ag_relay(0, xs, (0, 1, 2, 3))
    ag_start(1, dys)
    ag_relay(0, xs, (4, 5))
    ag_finish(0, xs)
    out_copies = [pltpu.make_async_copy(xs, xa_hbm, osem.at[0]),
                  pltpu.make_async_copy(cm, cm_hbm, osem.at[1]),
                  pltpu.make_async_copy(gm, gm_hbm, osem.at[2]),
                  pltpu.make_async_copy(dys, dya_hbm, osem.at[3])]
    for c in out_copies[:3]:
        c.start()

    def gather_all(g, src):
        def step(q, _):
            def store(k, rows, val):
                xe_s[k, rows, :] = val
            gather_pair(cm, g, q, src, store)
            return 0
        lax.fori_loop(0, NP // 2, step, 0, unroll=4)

    def gather_dy(g):
        def step(q, _):
            def store(k, rows, val):
                xe_s[k, rows, :] = val

            def store_scaled(k, rows, val):
                do_s[k, rows, :] = val
            gather_dy_pair(cm, gm, g, q, dys, store, store_scaled)
            return 0
        lax.fori_loop(0, NP // 2, step, 0, unroll=4)

    def put_rows(i, val):
        zero = jnp.zeros((PAD - CAP, val.shape[1]), F32)
        for p in range(NP):
            o_s[i, p * PAD:(p + 1) * PAD, :] = jnp.concatenate([val[p * CAP:(p + 1) * CAP], zero], axis=0).astype(BF16)

    def take_rows(p):
        return jnp.concatenate([o_s[k, ds(p, PAD), :] for k in range(GRP)], axis=0)

    def combine_y(g):
        def step(p, _):
            oh = onehot(cm[p, ds(g, GRP), :], PAD)
            gr = gm[p, ds(g, GRP), :]
            g1 = gr.astype(BF16).astype(F32)
            rest = gr - g1
            g2 = rest.astype(BF16).astype(F32)
            g3 = rest - g2
            ob = take_rows(p)

            def spread(part):
                return jnp.concatenate(
                    [jnp.where(oh[k], jnp.broadcast_to(part[k:k + 1], (PAD, TOK)), 0.0) for k in range(GRP)],
                    axis=0).astype(BF16)

            gs = jnp.concatenate([spread(g1), spread(g2), spread(g3)], axis=0)
            yacc[p] += tn(gs, jnp.concatenate([ob, ob, ob], axis=0))
            return 0
        lax.fori_loop(0, NP, step, 0, unroll=4)

    def combine_dx(g, cc):
        for j in range(NP // 2):
            p = 2 * j + cc
            oh = onehot(cm[p, ds(g, GRP), :], PAD)
            one = jnp.concatenate([jnp.where(m, 1.0, 0.0) for m in oh], axis=0).astype(BF16)
            dxacc[p] += tn(one, take_rows(p))
            rows = []
            for k in range(GRP):
                db = jnp.broadcast_to(dgc_s[k, ds(p, CAP), :], (CAP, TOK))
                rows.append(jnp.sum(jnp.where(oh[k][:CAP], db, 0.0), axis=0, keepdims=True))
            dgm[p, ds(g, GRP), :] = jnp.concatenate(rows, axis=0)

    def fetch(n):
        for k in range(PAIR):
            for c in wcopies(n + k):
                c.wait()

    def release(n):
        @pl.when(n + NBUF < 2 * el)
        def _():
            for k in range(PAIR):
                for c in wcopies(n + NBUF + k):
                    c.start()

    def w13_of(n):
        b = lax.rem(n, NBUF)
        return jnp.concatenate([w1b[b], w3b[b]], axis=1)

    def w2_of(n):
        return w2b[lax.rem(n, NBUF)]

    def skewed(g, first, base, second):
        npair = GRP // PAIR
        first(0)

        def step(r, _):
            fetch(base + r * PAIR)
            second(r - 1)
            first(r)
            release(base + (r - 1) * PAIR)
            return 0

        lax.fori_loop(1, npair, step, 0)
        second(npair - 1)

    def act(uv):
        u, v = uv[:, :ff], uv[:, ff:]
        sg = jax.nn.sigmoid(u)
        return u, v, sg, (u * sg * v).astype(BF16)

    ORDER = [(1, 1), (0, 1), (1, 0), (0, 0)]
    S1 = [((1, 1), 0, XN), ((1, 1), 1, YN), ((0, 1), 0, XN), ((1, 0), 1, YN)]
    IN1 = [((1, 0), 0), ((0, 1), 1), ((0, 0), 0), ((0, 0), 1)]
    S2 = [YN, XN]

    def dd_copy(t, acc, n):
        fy, fx = ORDER[n]
        return remote(acc.at[blk(fy, fx, 1)], rd.at[n], dd_ss.at[t, n], dd_rs.at[t, n], PN)

    def s1_copy(t, acc, n):
        (fy, fx), h, to = S1[n]
        return remote(half(acc, blk(fy, fx, 0), h), r1.at[t, n], s1_ss.at[t, n], s1_rs.at[t, n], to)

    def s2_copy(t, acc, n):
        (fy, fx), h = IN1[n]
        return remote(half(acc, blk(fy, fx, 0), h), r2.at[t, n], s2_ss.at[t, n], s2_rs.at[t, n], S2[n])

    def rs_start(t, acc):
        for n in range(4):
            dd_copy(t, acc, n).start()

    def rs_mid1(t, acc):
        for n in range(4):
            dd_copy(t, acc, n).wait_recv()
            fy, fx = ORDER[n]
            acc[blk(fy, fx, 0)] += rd[n]
            for k in ((0, 1), (2,), (3,), ())[n]:
                s1_copy(t, acc, k).start()

    def rs_mid2(t, acc):
        for n in range(4):
            s1_copy(t, acc, n).wait_recv()
            (fy, fx), h = IN1[n]
            acc[blk(fy, fx, 0), h * HALF:(h + 1) * HALF, :] += r1[t, n]
            if n < 2:
                s2_copy(t, acc, n).start()

    def rs_fin(t, acc, out):
        for n in range(2):
            s2_copy(t, acc, n).wait_recv()
            rows = slice(n * HALF, (n + 1) * HALF)
            out[rows, :] = (acc[me, rows, :] + r2[t, n]).astype(BF16)

    def rs_drain(t, acc):
        for n in range(4):
            dd_copy(t, acc, n).wait_send()
            s1_copy(t, acc, n).wait_send()
        for n in range(2):
            s2_copy(t, acc, n).wait_send()

    xef_copy = pltpu.make_async_copy(xe_s, xef_hbm, osem.at[6])
    dof_copy = pltpu.make_async_copy(do_s, dof_hbm, osem.at[7])

    def fwd_group(g, _):
        fetch(g * GRP)
        gather_all(g, xs)

        def f1(r):
            for k in range(PAIR):
                i = r * PAIR + k
                uv_s[g * GRP + i] = nn(xe_s[i], w13_of(g * GRP + i)).astype(BF16)

        def f2(r):
            uvs = [uv_s[g * GRP + r * PAIR + k].astype(F32) for k in range(PAIR)]
            for k in range(PAIR):
                i = r * PAIR + k
                put_rows(i, nn(act(uvs[k])[3], w2_of(g * GRP + i)))

        skewed(g, f1, g * GRP, f2)

        @pl.when(g == 0)
        def _():
            xef_copy.start()
        combine_y(g)
        release(g * GRP + GRP - PAIR)

        @pl.when(g == 0)
        def _():
            xef_copy.wait()

        @pl.when(g == 0)
        def _():
            ag_relay(1, dys, (0, 1, 2, 3))

        @pl.when(g == 1)
        def _():
            ag_relay(1, dys, (4, 5))

        @pl.when(g == 2)
        def _():
            ag_finish(1, dys)
            out_copies[3].start()
        return 0

    lax.fori_loop(0, ng, fwd_group, 0)

    def duv_copy(g):
        return pltpu.make_async_copy(uv_s.at[ds(g, GRP)], duv_hbm.at[ds(g, GRP)], osem.at[4])

    def a_copy(g):
        return pltpu.make_async_copy(a_s, a_hbm.at[ds(g, GRP)], osem.at[5])

    def bwd_group(g, _):
        @pl.when(g > 0)
        def _():
            a_copy(g - 1).wait()
            duv_copy(g - 1).wait()
        fetch(el + g * GRP)
        gather_dy(g)

        def b1(r):
            uvs = [uv_s[g * GRP + r * PAIR + k] for k in range(PAIR)]
            for k in range(PAIR):
                i = r * PAIR + k
                e = g * GRP + i
                w2 = w2_of(el + e)
                da = nt(do_s[i], w2)
                u, v, sg, a = act(uvs[k].astype(F32))
                a_s[i] = a
                of = nn(a, w2).astype(BF16).astype(F32)
                dgc_s[i] = jnp.sum(xe_s[i].astype(F32) * of, axis=1, keepdims=True)
                du = (da * v * sg * (1.0 + u * (1.0 - sg))).astype(BF16)
                dv = (da * u * sg).astype(BF16)
                uv_s[e] = jnp.concatenate([du, dv], axis=1)

        def b2(r):
            duvs = [uv_s[g * GRP + r * PAIR + k] for k in range(PAIR)]
            for k in range(PAIR):
                i = r * PAIR + k
                put_rows(i, nt(duvs[k], w13_of(el + g * GRP + i)))

        skewed(g, b1, el + g * GRP, b2)
        a_copy(g).start()
        duv_copy(g).start()
        combine_dx(g, 1 - C)

        @pl.when(g == ng - 1)
        def _():
            pl.semaphore_wait(credit, 1)
            rs_start(1, dxacc)
        combine_dx(g, C)
        release(el + g * GRP + GRP - PAIR)

        @pl.when(g == 0)
        def _():
            dof_copy.start()
            rs_start(0, yacc)
            dof_copy.wait()

        @pl.when(g == 1)
        def _():
            rs_mid1(0, yacc)
            pl.semaphore_signal(credit, inc=1, device_id=dev(*PN), device_id_type=MESH)

        @pl.when(g == ng - 1)
        def _():
            rs_mid2(0, yacc)
        return 0

    lax.fori_loop(0, ng, bwd_group, 0)

    def spread_dg(p, _):
        rg = rgs[p]
        acc = jnp.zeros((top, TOK), F32)
        for e in range(el):
            ef = (e0 + e).astype(F32)
            acc = acc + jnp.where(rg[:top] == ef, jnp.broadcast_to(dgm[p, e:e + 1, :], (top, TOK)), 0.0)
        dgo[p] = acc
        return 0

    lax.fori_loop(0, NP, spread_dg, 0)
    rs_fin(0, yacc, y_ref)
    dg_copies = [remote(dgo.at[blk(*to)], dgr.at[n], dg_ss.at[n], dg_rs.at[n], to) for n, to in enumerate(peers)]
    for c in dg_copies:
        c.start()
    part_copies = []
    for n in range(4):
        dd_copy(1, dxacc, n).wait_recv()
        b = blk(*ORDER[n], 0)
        dxacc[b] += rd[n]
        c = pltpu.make_async_copy(dxacc.at[b], (sd_hbm, sx_hbm, sy_hbm, ka_hbm)[n], psem.at[n])
        c.start()
        part_copies.append(c)
    total = dgo[me]
    for n, c in enumerate(dg_copies):
        c.wait_recv()
        total = total + dgr[n]
    dg_ref[...] = total

    ag_drain(0, xs)
    ag_drain(1, dys)
    rs_drain(0, yacc)
    for n in range(4):
        dd_copy(1, dxacc, n).wait_send()
    for c in part_copies:
        c.wait()
    for c in rg_copies + dg_copies:
        c.wait_send()
    for c in out_copies:
        c.wait()
    a_copy(ng - 1).wait()
    duv_copy(ng - 1).wait()


def grad_kernel(el, y_hbm, dg_hbm, xa_hbm, dya_hbm, cm_hbm, gm_hbm, a_hbm, duv_hbm, xef_hbm, dof_hbm,
                yo_ref, dgo_ref, gw1_hbm, gw3_hbm, gw2_hbm,
                xs, dys, cm, gm, xe_s, do_s, a_s, duv_s, g1b, g3b, g2b, lsem, isem, gsem):
    ng = el // GRP
    npair = GRP // PAIR
    ff = a_s.shape[3]

    def inputs(g):
        slot = lax.rem(g, 2)
        return [pltpu.make_async_copy(a_hbm.at[ds(g, GRP)], a_s.at[slot], isem.at[0, slot]),
                pltpu.make_async_copy(duv_hbm.at[ds(g, GRP)], duv_s.at[slot], isem.at[1, slot])]

    def outputs(m):
        slot = lax.rem(m, NOUT)
        return [pltpu.make_async_copy(v.at[slot], h.at[ds(m, PAIR)], gsem.at[n, slot])
                for n, (h, v) in enumerate(((gw1_hbm, g1b), (gw3_hbm, g3b), (gw2_hbm, g2b)))]

    heads = [pltpu.make_async_copy(xef_hbm, xe_s.at[0], lsem.at[2]), pltpu.make_async_copy(dof_hbm, do_s.at[0], lsem.at[3])]
    loads = [pltpu.make_async_copy(h, v, lsem.at[n]) for n, h, v in (
        (0, xa_hbm, xs), (1, dya_hbm, dys), (4, cm_hbm, cm), (5, gm_hbm, gm), (6, y_hbm, yo_ref), (7, dg_hbm, dgo_ref))]
    for c in heads + inputs(0) + loads:
        c.start()

    def gather(g, q):
        slot = lax.rem(g, 2)

        def store(j, rows, val):
            xe_s[slot, j, rows, :] = val

        def store_scaled(j, rows, val):
            do_s[slot, j, rows, :] = val
        gather_pair(cm, g, q, xs, store)
        gather_dy_pair(cm, gm, g, q, dys, None, store_scaled)

    def core(g, r):
        slot = lax.rem(g, 2)
        o = lax.rem(g * npair + r, NOUT)
        for k in range(PAIR):
            i = r * PAIR + k
            g13 = tn(xe_s[slot, i], duv_s[slot, i])
            g1b[o, k] = g13[:, :ff]
            g3b[o, k] = g13[:, ff:]
            g2b[o, k] = tn(a_s[slot, i], do_s[slot, i])

    def finish(g, r):
        for c in outputs(g * npair + r):
            c.start()

    for c in heads + inputs(0):
        c.wait()
    for c in inputs(1):
        c.start()
    for r in range(npair):
        if r == 1:
            for c in loads:
                c.wait()
        if r == NOUT:
            for c in outputs(0):
                c.wait()
        core(0, r)
        for q in ((), (0, 1), (2,), (3,))[r]:
            gather(1, q)
        finish(0, r)

    def group(g, _):
        for c in inputs(g):
            c.wait()

        @pl.when(g + 1 < ng)
        def _():
            for c in inputs(g + 1):
                c.start()

        def step(r, _):
            for c in outputs(g * npair + r - NOUT):
                c.wait()
            core(g, r)
            gather(g + 1, r)
            finish(g, r)
            return 0

        def last(r, _):
            for c in outputs(g * npair + r - NOUT):
                c.wait()
            core(g, r)
            finish(g, r)
            return 0

        @pl.when(g + 1 < ng)
        def _():
            lax.fori_loop(0, npair, step, 0)

        @pl.when(g + 1 == ng)
        def _():
            lax.fori_loop(0, npair, last, 0)
        return 0

    lax.fori_loop(1, ng, group, 0)
    for m in range(NOUT):
        for c in outputs(ng * npair - NOUT + m):
            c.wait()


def solution(mesh):
    grp = ('row', 'col')
    tspec = P(('dp', 'row', 'col'), None)
    wspec = P(grp, None, None)
    gspec = P(('dp', 'row', 'col'), None, None)

    def local(x, ridx, gates, w1, w3, w2, dy):
        tok, d = x.shape
        top = ridx.shape[1]
        el, _, ff = w1.shape
        anyspec = pl.BlockSpec(memory_space=pl.ANY)
        vm = pl.BlockSpec(memory_space=pltpu.VMEM)
        sds = jax.ShapeDtypeStruct
        dma = pltpu.SemaphoreType.DMA
        y, dg, sd, sx, sy, ka, xa, dya, cm, gm, duv, a, xef, dof = pl.pallas_call(
            functools.partial(main_kernel, el),
            in_specs=[anyspec, anyspec, vm, vm, anyspec, anyspec, anyspec],
            out_specs=[vm, vm] + [anyspec] * 12,
            out_shape=[
                sds((tok, d), BF16), sds((top, tok), F32)] + [sds((tok, d), F32)] * 4 + [
                sds((NP, tok, d), BF16), sds((NP, tok, d), BF16),
                sds((NP, el, tok), F32), sds((NP, el, tok), F32),
                sds((el, NROW, 2 * ff), BF16), sds((el, NROW, ff), BF16),
                sds((GRP, NROW, d), BF16), sds((GRP, NROW, d), BF16),
            ],
            scratch_shapes=[
                pltpu.VMEM((NP, tok, d), BF16),
                pltpu.VMEM((NP, tok, d), BF16),
                pltpu.VMEM((NP, 2 * top, tok), F32),
                pltpu.VMEM((GRP, NROW, d), BF16),
                pltpu.VMEM((GRP, NROW, d), BF16),
                pltpu.VMEM((GRP, NROW, 1), F32),
                pltpu.VMEM((GRP, NP * PAD, d), BF16),
                pltpu.VMEM((el, NROW, 2 * ff), BF16),
                pltpu.VMEM((GRP, NROW, ff), BF16),
                pltpu.VMEM((NP, tok, d), F32),
                pltpu.VMEM((NP, tok, d), F32),
                pltpu.VMEM((NP, el, tok), F32),
                pltpu.VMEM((NP, el, tok), F32),
                pltpu.VMEM((NP, el, tok), F32),
                pltpu.VMEM((NP, top, tok), F32),
                pltpu.VMEM((NP - 1, top, tok), F32),
                pltpu.VMEM((NBUF, d, ff), BF16),
                pltpu.VMEM((NBUF, d, ff), BF16),
                pltpu.VMEM((NBUF, ff, d), BF16),
                pltpu.VMEM((4, tok, d), F32),
                pltpu.VMEM((1, 4, tok // 2, d), F32),
                pltpu.VMEM((1, 2, tok // 2, d), F32),
                dma((3, NBUF)), dma((2,)), dma((8,)), dma((4,)), pltpu.SemaphoreType.REGULAR,
                dma((NP - 1,)), dma((NP - 1,)),
                dma((2, 14)), dma((2, 14)),
                dma((2, 4)), dma((2, 4)),
                dma((1, 4)), dma((1, 4)),
                dma((1, 2)), dma((1, 2)),
                dma((NP - 1,)), dma((NP - 1,)),
            ],
            compiler_params=pltpu.CompilerParams(
                collective_id=0, has_side_effects=True, vmem_limit_bytes=67_000_000),
            cost_estimate=pl.CostEstimate(flops=40_000_000_000, bytes_accessed=160_000_000, transcendentals=0),
        )(x, dy, ridx.T, gates.T, w1, w3, w2)

        def perm(fy, fx):
            out = []
            for p in range(NP):
                yy, xx, cc = p // 4, (p // 2) % 2, p % 2
                out.append((p, (yy ^ fy) * 4 + (xx ^ fx) * 2 + cc))
            return out

        rd = lax.ppermute(sd, grp, perm(1, 1))
        rx = lax.ppermute(sx, grp, perm(0, 1))
        ry = lax.ppermute(sy, grp, perm(1, 0))
        y, dg, gw1, gw3, gw2 = pl.pallas_call(
            functools.partial(grad_kernel, el),
            in_specs=[pl.BlockSpec(memory_space=pltpu.HBM)] * 10,
            out_specs=[vm, vm, anyspec, anyspec, anyspec],
            out_shape=[sds((tok, d), BF16), sds((top, tok), F32), sds((el, d, ff), F32), sds((el, d, ff), F32), sds((el, ff, d), F32)],
            scratch_shapes=[
                pltpu.VMEM((NP, tok, d), BF16),
                pltpu.VMEM((NP, tok, d), BF16),
                pltpu.VMEM((NP, el, tok), F32),
                pltpu.VMEM((NP, el, tok), F32),
                pltpu.VMEM((2, GRP, NROW, d), BF16),
                pltpu.VMEM((2, GRP, NROW, d), BF16),
                pltpu.VMEM((2, GRP, NROW, ff), BF16),
                pltpu.VMEM((2, GRP, NROW, 2 * ff), BF16),
                pltpu.VMEM((NOUT, PAIR, d, ff), F32),
                pltpu.VMEM((NOUT, PAIR, d, ff), F32),
                pltpu.VMEM((NOUT, PAIR, ff, d), F32),
                dma((8,)), dma((2, 2)), dma((3, NOUT)),
            ],
            compiler_params=pltpu.CompilerParams(vmem_limit_bytes=67_000_000),
            cost_estimate=pl.CostEstimate(flops=40_000_000_000, bytes_accessed=160_000_000, transcendentals=0),
        )(y, dg, xa, dya, cm, gm, a, duv, xef, dof)
        dx = (ka + rx + ry + rd).astype(BF16)
        return y, dx, dg.T, gw1, gw3, gw2

    return jax.shard_map(local, mesh=mesh, in_specs=(tspec, tspec, tspec, wspec, wspec, wspec, tspec), out_specs=(tspec, tspec, tspec, gspec, gspec, gspec), check_vma=False)
```

```python
import functools

import jax
import jax.numpy as jnp
from jax import lax
from jax.experimental import pallas as pl
from jax.experimental.pallas import tpu as pltpu
from jax.sharding import PartitionSpec as P

F32 = jnp.float32
BF16 = jnp.bfloat16
MESH = pl.DeviceIdType.MESH
NP = 8
TOK = 256
HALF = TOK // 2
CAP = 24
PAD = 32
GRP = 8
NROW = NP * CAP
NBUF = 8
PAIR = 2
NOUT = 3


def nt(a, b):
    return lax.dot_general(a, b, (((1,), (1,)), ((), ())), preferred_element_type=F32)


def nn(a, b):
    return lax.dot_general(a, b, (((1,), (0,)), ((), ())), preferred_element_type=F32)


def tn(a, b):
    return lax.dot_general(a, b, (((0,), (0,)), ((), ())), preferred_element_type=F32)


def onehot(rows, cap):
    n = rows.shape[0]
    it = lax.broadcasted_iota(jnp.int32, (cap, TOK), 0).astype(F32)
    return [jnp.broadcast_to(rows[k:k + 1], (cap, TOK)) == it for k in range(n)]


def ds(i, n):
    return pl.ds(pl.multiple_of(i * n, n), n)


def gather_pair(cm, g, q, src, store):
    res = []
    for h in range(2):
        p = q * 2 + h
        oh = onehot(cm[p, ds(g, GRP), :], CAP)
        oh = jnp.concatenate([jnp.where(m, 1.0, 0.0) for m in oh], axis=0).astype(BF16)
        res.append(nn(oh, src[p]))
    for k in range(GRP):
        blk = jnp.concatenate([r[k * CAP:(k + 1) * CAP] for r in res], axis=0)
        store(k, ds(q, 2 * CAP), blk.astype(BF16))


def gather_dy_pair(cm, gm, g, q, src, store, store_scaled):
    res, scaled = [], []
    for h in range(2):
        p = q * 2 + h
        oh = onehot(cm[p, ds(g, GRP), :], CAP)
        gr = gm[p, ds(g, GRP), :]
        col = jnp.concatenate(
            [jnp.sum(jnp.where(m, jnp.broadcast_to(gr[k:k + 1], (CAP, TOK)), 0.0), axis=1, keepdims=True)
             for k, m in enumerate(oh)], axis=0)
        oh = jnp.concatenate([jnp.where(m, 1.0, 0.0) for m in oh], axis=0).astype(BF16)
        r = nn(oh, src[p])
        res.append(r)
        scaled.append(col * r)
    for parts, put in ((res, store), (scaled, store_scaled)):
        if put is None:
            continue
        for k in range(GRP):
            blk = jnp.concatenate([r[k * CAP:(k + 1) * CAP] for r in parts], axis=0)
            put(k, ds(q, 2 * CAP), blk.astype(BF16))


def main_kernel(el, x_hbm, dy_hbm, id_ref, gate_ref, w1_hbm, w3_hbm, w2_hbm,
                y_ref, dg_ref, sd_hbm, sx_hbm, sy_hbm, ka_hbm, xa_hbm, dya_hbm, cm_hbm, gm_hbm, duv_hbm, a_hbm, xef_hbm, dof_hbm,
                xs, dys, rgs, xe_s, do_s, dgc_s, o_s, uv_s, a_s, yacc, dxacc, cm, gm, dgm, dgo, dgr,
                w1b, w3b, w2b, rd, r1, r2,
                wsem, lsem, osem, psem, credit, rg_ss, rg_rs, ag_ss, ag_rs, dd_ss, dd_rs, s1_ss, s1_rs, s2_ss, s2_rs, dg_ss, dg_rs):
    ng = el // GRP
    ff = w2b.shape[1]
    Z = lax.axis_index('dp')
    Y = lax.axis_index('row')
    col = lax.axis_index('col')
    X = lax.div(col, 2)
    C = lax.rem(col, 2)
    me = Y * 4 + col
    e0 = me * el

    def pos(fy, fx, fc):
        return (1 - Y if fy else Y), (1 - X if fx else X), (1 - C if fc else C)

    def blk(fy, fx, fc):
        yy, xx, cc = pos(fy, fx, fc)
        return yy * 4 + xx * 2 + cc

    def dev(fy, fx, fc):
        yy, xx, cc = pos(fy, fx, fc)
        return (Z, yy, xx * 2 + cc)

    peers = [(a, b, c) for a in range(2) for b in range(2) for c in range(2)][1:]

    def remote(src, dst, ss, rs, to):
        return pltpu.make_async_remote_copy(src_ref=src, dst_ref=dst, send_sem=ss, recv_sem=rs,
                                            device_id=dev(*to), device_id_type=MESH)

    lx = pltpu.make_async_copy(x_hbm, xs.at[me], lsem.at[0])
    ld = pltpu.make_async_copy(dy_hbm, dys.at[me], lsem.at[1])
    lx.start()
    ld.start()

    def wcopies(e):
        b = lax.rem(e, NBUF)
        k = lax.rem(e, el)
        return [pltpu.make_async_copy(h.at[k], v.at[b], wsem.at[n, b])
                for n, (h, v) in enumerate(((w1_hbm, w1b), (w3_hbm, w3b), (w2_hbm, w2b)))]

    for e in range(NBUF):
        for c in wcopies(e):
            c.start()

    rgs[me] = jnp.concatenate([id_ref[...].astype(F32), gate_ref[...]], axis=0)
    barrier = pltpu.get_barrier_semaphore()
    for to in peers:
        pl.semaphore_signal(barrier, inc=1, device_id=dev(*to), device_id_type=MESH)
    pl.semaphore_wait(barrier, len(peers))

    rg_copies = [remote(rgs.at[me], rgs.at[me], rg_ss.at[n], rg_rs.at[n], to) for n, to in enumerate(peers)]
    for c in rg_copies:
        c.start()

    def half(buf, b, h):
        return buf.at[b, pl.ds(h * HALF, HALF), :]

    XN, YN, DN, PN = (0, 1, 0), (1, 0, 0), (1, 1, 0), (0, 0, 1)
    FIRST = [(0, (0, 0, 0), 0, XN), (1, (0, 0, 0), 1, YN), (2, (0, 0, 0), 1, XN), (3, (0, 0, 0), 0, YN)]
    OWN2 = [(6, (0, 0, 0), 0, PN), (7, (0, 0, 0), 1, PN)]
    FWD = [(4, XN, 0, YN), (5, YN, 1, XN)]
    ARR = {0: (XN, 0), 1: (YN, 1), 2: (XN, 1), 3: (YN, 0), 4: (DN, 0), 5: (DN, 1)}
    ONWARD = {0: 8, 1: 9, 2: 10, 3: 11, 4: 12, 5: 13}

    def ag_copy(t, buf, n, f, h, to):
        r = half(buf, blk(*f), h)
        return remote(r, r, ag_ss.at[t, n], ag_rs.at[t, n], to)

    def ag_recv(t, buf, n, f, h):
        r = half(buf, blk(*f), h)
        remote(r, r, ag_ss.at[t, n], ag_rs.at[t, n], PN).wait_recv()

    def ag_start(t, buf):
        for n, f, h, to in FIRST + OWN2:
            ag_copy(t, buf, n, f, h, to).start()

    def ag_relay(t, buf, ns):
        for n in ns:
            f, h = ARR[n]
            ag_recv(t, buf, n, f, h)
            if n < 2:
                k, ff_, hh, to = FWD[n]
                ag_copy(t, buf, k, ff_, hh, to).start()
            ag_copy(t, buf, ONWARD[n], f, h, PN).start()

    def ag_finish(t, buf):
        for n, h in ((6, 0), (7, 1)):
            ag_recv(t, buf, n, PN, h)
        for n, k in ONWARD.items():
            f, h = ARR[n]
            ag_recv(t, buf, k, (f[0], f[1], 1), h)

    def ag_drain(t, buf):
        for n, f, h, to in FIRST + OWN2 + FWD:
            ag_copy(t, buf, n, f, h, to).wait_send()
        for n, k in ONWARD.items():
            f, h = ARR[n]
            ag_copy(t, buf, k, f, h, PN).wait_send()

    lx.wait()
    ld.wait()
    ag_start(0, xs)

    def zero(p, _):
        yacc[p] = jnp.zeros(yacc.shape[1:], F32)
        dxacc[p] = jnp.zeros(dxacc.shape[1:], F32)
        return 0

    lax.fori_loop(0, NP, zero, 0)

    for n, to in enumerate(peers):
        remote(rgs.at[blk(*to)], rgs.at[blk(*to)], rg_ss.at[n], rg_rs.at[n], to).wait_recv()
    top = rgs.shape[1] // 2
    tr = lax.broadcasted_iota(jnp.int32, (TOK, TOK), 0)
    tc = lax.broadcasted_iota(jnp.int32, (TOK, TOK), 1)
    tri = jnp.where(tr < tc, 1.0, 0.0).astype(BF16)
    ee = (lax.broadcasted_iota(jnp.int32, (el, TOK), 0) + e0).astype(F32)

    def prep(p, _):
        rg = rgs[p]
        m = jnp.zeros((el, TOK), F32)
        gs = jnp.zeros((el, TOK), F32)
        for j in range(top):
            hit = jnp.broadcast_to(rg[j:j + 1], (el, TOK)) == ee
            m = jnp.where(hit, 1.0, m)
            gs = jnp.where(hit, jnp.broadcast_to(rg[top + j:top + j + 1], (el, TOK)), gs)
        rank = nn(m.astype(BF16), tri)
        cm[p] = jnp.where(m > 0.0, rank, -1.0)
        gm[p] = gs
        return 0

    lax.fori_loop(0, NP, prep, 0)

    ag_relay(0, xs, (0, 1, 2, 3))
    ag_start(1, dys)
    ag_relay(0, xs, (4, 5))
    ag_finish(0, xs)
    out_copies = [pltpu.make_async_copy(xs, xa_hbm, osem.at[0]),
                  pltpu.make_async_copy(cm, cm_hbm, osem.at[1]),
                  pltpu.make_async_copy(gm, gm_hbm, osem.at[2]),
                  pltpu.make_async_copy(dys, dya_hbm, osem.at[3])]
    for c in out_copies[:3]:
        c.start()

    def gather_all(g, src):
        def step(q, _):
            def store(k, rows, val):
                xe_s[k, rows, :] = val
            gather_pair(cm, g, q, src, store)
            return 0
        lax.fori_loop(0, NP // 2, step, 0, unroll=4)

    def gather_dy(g):
        def step(q, _):
            def store(k, rows, val):
                xe_s[k, rows, :] = val

            def store_scaled(k, rows, val):
                do_s[k, rows, :] = val
            gather_dy_pair(cm, gm, g, q, dys, store, store_scaled)
            return 0
        lax.fori_loop(0, NP // 2, step, 0, unroll=4)

    def put_rows(i, val):
        zero = jnp.zeros((PAD - CAP, val.shape[1]), F32)
        for p in range(NP):
            o_s[i, p * PAD:(p + 1) * PAD, :] = jnp.concatenate([val[p * CAP:(p + 1) * CAP], zero], axis=0).astype(BF16)

    def take_rows(p):
        return jnp.concatenate([o_s[k, ds(p, PAD), :] for k in range(GRP)], axis=0)

    def combine_y(g):
        def step(p, _):
            oh = onehot(cm[p, ds(g, GRP), :], PAD)
            gr = gm[p, ds(g, GRP), :]
            g1 = gr.astype(BF16).astype(F32)
            rest = gr - g1
            g2 = rest.astype(BF16).astype(F32)
            g3 = rest - g2
            ob = take_rows(p)

            def spread(part):
                return jnp.concatenate(
                    [jnp.where(oh[k], jnp.broadcast_to(part[k:k + 1], (PAD, TOK)), 0.0) for k in range(GRP)],
                    axis=0).astype(BF16)

            gs = jnp.concatenate([spread(g1), spread(g2), spread(g3)], axis=0)
            yacc[p] += tn(gs, jnp.concatenate([ob, ob, ob], axis=0))
            return 0
        lax.fori_loop(0, NP, step, 0, unroll=4)

    def combine_dx(g, cc):
        for j in range(NP // 2):
            p = 2 * j + cc
            oh = onehot(cm[p, ds(g, GRP), :], PAD)
            one = jnp.concatenate([jnp.where(m, 1.0, 0.0) for m in oh], axis=0).astype(BF16)
            dxacc[p] += tn(one, take_rows(p))
            rows = []
            for k in range(GRP):
                db = jnp.broadcast_to(dgc_s[k, ds(p, CAP), :], (CAP, TOK))
                rows.append(jnp.sum(jnp.where(oh[k][:CAP], db, 0.0), axis=0, keepdims=True))
            dgm[p, ds(g, GRP), :] = jnp.concatenate(rows, axis=0)

    def fetch(n):
        for k in range(PAIR):
            for c in wcopies(n + k):
                c.wait()

    def release(n):
        @pl.when(n + NBUF < 2 * el)
        def _():
            for k in range(PAIR):
                for c in wcopies(n + NBUF + k):
                    c.start()

    def w13_of(n):
        b = lax.rem(n, NBUF)
        return jnp.concatenate([w1b[b], w3b[b]], axis=1)

    def w2_of(n):
        return w2b[lax.rem(n, NBUF)]

    def skewed(g, first, base, second):
        npair = GRP // PAIR
        first(0)

        def step(r, _):
            fetch(base + r * PAIR)
            second(r - 1)
            first(r)
            release(base + (r - 1) * PAIR)
            return 0

        lax.fori_loop(1, npair, step, 0)
        second(npair - 1)

    def act(uv):
        u, v = uv[:, :ff], uv[:, ff:]
        sg = jax.nn.sigmoid(u)
        return u, v, sg, (u * sg * v).astype(BF16)

    ORDER = [(1, 1), (0, 1), (1, 0), (0, 0)]
    S1 = [((1, 1), 0, XN), ((1, 1), 1, YN), ((0, 1), 0, XN), ((1, 0), 1, YN)]
    IN1 = [((1, 0), 0), ((0, 1), 1), ((0, 0), 0), ((0, 0), 1)]
    S2 = [YN, XN]

    def dd_copy(t, acc, n):
        fy, fx = ORDER[n]
        return remote(acc.at[blk(fy, fx, 1)], rd.at[n], dd_ss.at[t, n], dd_rs.at[t, n], PN)

    def s1_copy(t, acc, n):
        (fy, fx), h, to = S1[n]
        return remote(half(acc, blk(fy, fx, 0), h), r1.at[t, n], s1_ss.at[t, n], s1_rs.at[t, n], to)

    def s2_copy(t, acc, n):
        (fy, fx), h = IN1[n]
        return remote(half(acc, blk(fy, fx, 0), h), r2.at[t, n], s2_ss.at[t, n], s2_rs.at[t, n], S2[n])

    def rs_start(t, acc):
        for n in range(4):
            dd_copy(t, acc, n).start()

    def rs_mid1(t, acc):
        for n in range(4):
            dd_copy(t, acc, n).wait_recv()
            fy, fx = ORDER[n]
            acc[blk(fy, fx, 0)] += rd[n]
            for k in ((0, 1), (2,), (3,), ())[n]:
                s1_copy(t, acc, k).start()

    def rs_mid2(t, acc):
        for n in range(4):
            s1_copy(t, acc, n).wait_recv()
            (fy, fx), h = IN1[n]
            acc[blk(fy, fx, 0), h * HALF:(h + 1) * HALF, :] += r1[t, n]
            if n < 2:
                s2_copy(t, acc, n).start()

    def rs_fin(t, acc, out):
        for n in range(2):
            s2_copy(t, acc, n).wait_recv()
            rows = slice(n * HALF, (n + 1) * HALF)
            out[rows, :] = (acc[me, rows, :] + r2[t, n]).astype(BF16)

    def rs_drain(t, acc):
        for n in range(4):
            dd_copy(t, acc, n).wait_send()
            s1_copy(t, acc, n).wait_send()
        for n in range(2):
            s2_copy(t, acc, n).wait_send()

    xef_copy = pltpu.make_async_copy(xe_s, xef_hbm, osem.at[6])
    dof_copy = pltpu.make_async_copy(do_s, dof_hbm, osem.at[7])

    def fwd_group(g, _):
        fetch(g * GRP)
        gather_all(g, xs)

        def f1(r):
            for k in range(PAIR):
                i = r * PAIR + k
                uv_s[g * GRP + i] = nn(xe_s[i], w13_of(g * GRP + i)).astype(BF16)

        def f2(r):
            uvs = [uv_s[g * GRP + r * PAIR + k].astype(F32) for k in range(PAIR)]
            for k in range(PAIR):
                i = r * PAIR + k
                put_rows(i, nn(act(uvs[k])[3], w2_of(g * GRP + i)))

        skewed(g, f1, g * GRP, f2)
        release(g * GRP + GRP - PAIR)

        @pl.when(g == 0)
        def _():
            xef_copy.start()
        combine_y(g)

        @pl.when(g == 0)
        def _():
            xef_copy.wait()

        @pl.when(g == 0)
        def _():
            ag_relay(1, dys, (0, 1, 2, 3))

        @pl.when(g == 1)
        def _():
            ag_relay(1, dys, (4, 5))

        @pl.when(g == 2)
        def _():
            ag_finish(1, dys)
            out_copies[3].start()
        return 0

    lax.fori_loop(0, ng, fwd_group, 0)

    def duv_copy(g):
        return pltpu.make_async_copy(uv_s.at[ds(g, GRP)], duv_hbm.at[ds(g, GRP)], osem.at[4])

    def a_copy(g):
        return pltpu.make_async_copy(a_s, a_hbm.at[ds(g, GRP)], osem.at[5])

    def bwd_group(g, _):
        @pl.when(g > 0)
        def _():
            a_copy(g - 1).wait()
            duv_copy(g - 1).wait()
        fetch(el + g * GRP)
        gather_dy(g)

        def b1(r):
            uvs = [uv_s[g * GRP + r * PAIR + k] for k in range(PAIR)]
            for k in range(PAIR):
                i = r * PAIR + k
                e = g * GRP + i
                w2 = w2_of(el + e)
                da = nt(do_s[i], w2)
                u, v, sg, a = act(uvs[k].astype(F32))
                a_s[i] = a
                of = nn(a, w2).astype(BF16).astype(F32)
                dgc_s[i] = jnp.sum(xe_s[i].astype(F32) * of, axis=1, keepdims=True)
                du = (da * v * sg * (1.0 + u * (1.0 - sg))).astype(BF16)
                dv = (da * u * sg).astype(BF16)
                uv_s[e] = jnp.concatenate([du, dv], axis=1)

        def b2(r):
            duvs = [uv_s[g * GRP + r * PAIR + k] for k in range(PAIR)]
            for k in range(PAIR):
                i = r * PAIR + k
                put_rows(i, nt(duvs[k], w13_of(el + g * GRP + i)))

        skewed(g, b1, el + g * GRP, b2)
        a_copy(g).start()
        duv_copy(g).start()
        combine_dx(g, 1 - C)

        @pl.when(g == ng - 1)
        def _():
            pl.semaphore_wait(credit, 1)
            rs_start(1, dxacc)
        combine_dx(g, C)
        release(el + g * GRP + GRP - PAIR)

        @pl.when(g == 0)
        def _():
            dof_copy.start()
            rs_start(0, yacc)
            dof_copy.wait()

        @pl.when(g == 1)
        def _():
            rs_mid1(0, yacc)
            pl.semaphore_signal(credit, inc=1, device_id=dev(*PN), device_id_type=MESH)

        @pl.when(g == ng - 1)
        def _():
            rs_mid2(0, yacc)
        return 0

    lax.fori_loop(0, ng, bwd_group, 0)

    def spread_dg(p, _):
        rg = rgs[p]
        acc = jnp.zeros((top, TOK), F32)
        for e in range(el):
            ef = (e0 + e).astype(F32)
            acc = acc + jnp.where(rg[:top] == ef, jnp.broadcast_to(dgm[p, e:e + 1, :], (top, TOK)), 0.0)
        dgo[p] = acc
        return 0

    lax.fori_loop(0, NP, spread_dg, 0)
    rs_fin(0, yacc, y_ref)
    dg_copies = [remote(dgo.at[blk(*to)], dgr.at[n], dg_ss.at[n], dg_rs.at[n], to) for n, to in enumerate(peers)]
    for c in dg_copies:
        c.start()
    part_copies = []
    for n in range(4):
        dd_copy(1, dxacc, n).wait_recv()
        b = blk(*ORDER[n], 0)
        dxacc[b] += rd[n]
        c = pltpu.make_async_copy(dxacc.at[b], (sd_hbm, sx_hbm, sy_hbm, ka_hbm)[n], psem.at[n])
        c.start()
        part_copies.append(c)
    total = dgo[me]
    for n, c in enumerate(dg_copies):
        c.wait_recv()
        total = total + dgr[n]
    dg_ref[...] = total

    ag_drain(0, xs)
    ag_drain(1, dys)
    rs_drain(0, yacc)
    for n in range(4):
        dd_copy(1, dxacc, n).wait_send()
    for c in part_copies:
        c.wait()
    for c in rg_copies + dg_copies:
        c.wait_send()
    for c in out_copies:
        c.wait()
    a_copy(ng - 1).wait()
    duv_copy(ng - 1).wait()


def grad_kernel(el, y_hbm, dg_hbm, xa_hbm, dya_hbm, cm_hbm, gm_hbm, a_hbm, duv_hbm, xef_hbm, dof_hbm,
                yo_ref, dgo_ref, gw1_hbm, gw3_hbm, gw2_hbm,
                xs, dys, cm, gm, xe_s, do_s, a_s, duv_s, g1b, g3b, g2b, lsem, isem, gsem):
    ng = el // GRP
    npair = GRP // PAIR
    ff = a_s.shape[3]

    def inputs(g):
        slot = lax.rem(g, 2)
        return [pltpu.make_async_copy(a_hbm.at[ds(g, GRP)], a_s.at[slot], isem.at[0, slot]),
                pltpu.make_async_copy(duv_hbm.at[ds(g, GRP)], duv_s.at[slot], isem.at[1, slot])]

    def outputs(m):
        slot = lax.rem(m, NOUT)
        return [pltpu.make_async_copy(v.at[slot], h.at[ds(m, PAIR)], gsem.at[n, slot])
                for n, (h, v) in enumerate(((gw1_hbm, g1b), (gw3_hbm, g3b), (gw2_hbm, g2b)))]

    heads = [pltpu.make_async_copy(xef_hbm, xe_s.at[0], lsem.at[2]), pltpu.make_async_copy(dof_hbm, do_s.at[0], lsem.at[3])]
    loads = [pltpu.make_async_copy(h, v, lsem.at[n]) for n, h, v in (
        (0, xa_hbm, xs), (1, dya_hbm, dys), (4, cm_hbm, cm), (5, gm_hbm, gm), (6, y_hbm, yo_ref), (7, dg_hbm, dgo_ref))]
    for c in heads + inputs(0) + loads:
        c.start()

    def gather(g, q):
        slot = lax.rem(g, 2)

        def store(j, rows, val):
            xe_s[slot, j, rows, :] = val

        def store_scaled(j, rows, val):
            do_s[slot, j, rows, :] = val
        gather_pair(cm, g, q, xs, store)
        gather_dy_pair(cm, gm, g, q, dys, None, store_scaled)

    def core(g, r):
        slot = lax.rem(g, 2)
        o = lax.rem(g * npair + r, NOUT)
        for k in range(PAIR):
            i = r * PAIR + k
            g13 = tn(xe_s[slot, i], duv_s[slot, i])
            g1b[o, k] = g13[:, :ff]
            g3b[o, k] = g13[:, ff:]
            g2b[o, k] = tn(a_s[slot, i], do_s[slot, i])

    def finish(g, r):
        for c in outputs(g * npair + r):
            c.start()

    for c in heads + inputs(0):
        c.wait()
    for c in inputs(1):
        c.start()
    for r in range(npair):
        if r == 1:
            for c in loads:
                c.wait()
        if r == NOUT:
            for c in outputs(0):
                c.wait()
        core(0, r)
        for q in ((), (0, 1), (2,), (3,))[r]:
            gather(1, q)
        finish(0, r)

    def group(g, _):
        for c in inputs(g):
            c.wait()

        @pl.when(g + 1 < ng)
        def _():
            for c in inputs(g + 1):
                c.start()

        def step(r, _):
            for c in outputs(g * npair + r - NOUT):
                c.wait()
            core(g, r)
            gather(g + 1, r)
            finish(g, r)
            return 0

        def last(r, _):
            for c in outputs(g * npair + r - NOUT):
                c.wait()
            core(g, r)
            finish(g, r)
            return 0

        @pl.when(g + 1 < ng)
        def _():
            lax.fori_loop(0, npair, step, 0)

        @pl.when(g + 1 == ng)
        def _():
            lax.fori_loop(0, npair, last, 0)
        return 0

    lax.fori_loop(1, ng, group, 0)
    for m in range(NOUT):
        for c in outputs(ng * npair - NOUT + m):
            c.wait()


def solution(mesh):
    grp = ('row', 'col')
    tspec = P(('dp', 'row', 'col'), None)
    wspec = P(grp, None, None)
    gspec = P(('dp', 'row', 'col'), None, None)

    def local(x, ridx, gates, w1, w3, w2, dy):
        tok, d = x.shape
        top = ridx.shape[1]
        el, _, ff = w1.shape
        anyspec = pl.BlockSpec(memory_space=pl.ANY)
        vm = pl.BlockSpec(memory_space=pltpu.VMEM)
        sds = jax.ShapeDtypeStruct
        dma = pltpu.SemaphoreType.DMA
        y, dg, sd, sx, sy, ka, xa, dya, cm, gm, duv, a, xef, dof = pl.pallas_call(
            functools.partial(main_kernel, el),
            in_specs=[anyspec, anyspec, vm, vm, anyspec, anyspec, anyspec],
            out_specs=[vm, vm] + [anyspec] * 12,
            out_shape=[
                sds((tok, d), BF16), sds((top, tok), F32)] + [sds((tok, d), F32)] * 4 + [
                sds((NP, tok, d), BF16), sds((NP, tok, d), BF16),
                sds((NP, el, tok), F32), sds((NP, el, tok), F32),
                sds((el, NROW, 2 * ff), BF16), sds((el, NROW, ff), BF16),
                sds((GRP, NROW, d), BF16), sds((GRP, NROW, d), BF16),
            ],
            scratch_shapes=[
                pltpu.VMEM((NP, tok, d), BF16),
                pltpu.VMEM((NP, tok, d), BF16),
                pltpu.VMEM((NP, 2 * top, tok), F32),
                pltpu.VMEM((GRP, NROW, d), BF16),
                pltpu.VMEM((GRP, NROW, d), BF16),
                pltpu.VMEM((GRP, NROW, 1), F32),
                pltpu.VMEM((GRP, NP * PAD, d), BF16),
                pltpu.VMEM((el, NROW, 2 * ff), BF16),
                pltpu.VMEM((GRP, NROW, ff), BF16),
                pltpu.VMEM((NP, tok, d), F32),
                pltpu.VMEM((NP, tok, d), F32),
                pltpu.VMEM((NP, el, tok), F32),
                pltpu.VMEM((NP, el, tok), F32),
                pltpu.VMEM((NP, el, tok), F32),
                pltpu.VMEM((NP, top, tok), F32),
                pltpu.VMEM((NP - 1, top, tok), F32),
                pltpu.VMEM((NBUF, d, ff), BF16),
                pltpu.VMEM((NBUF, d, ff), BF16),
                pltpu.VMEM((NBUF, ff, d), BF16),
                pltpu.VMEM((4, tok, d), F32),
                pltpu.VMEM((1, 4, tok // 2, d), F32),
                pltpu.VMEM((1, 2, tok // 2, d), F32),
                dma((3, NBUF)), dma((2,)), dma((8,)), dma((4,)), pltpu.SemaphoreType.REGULAR,
                dma((NP - 1,)), dma((NP - 1,)),
                dma((2, 14)), dma((2, 14)),
                dma((2, 4)), dma((2, 4)),
                dma((1, 4)), dma((1, 4)),
                dma((1, 2)), dma((1, 2)),
                dma((NP - 1,)), dma((NP - 1,)),
            ],
            compiler_params=pltpu.CompilerParams(
                collective_id=0, has_side_effects=True, vmem_limit_bytes=67_000_000),
            cost_estimate=pl.CostEstimate(flops=40_000_000_000, bytes_accessed=160_000_000, transcendentals=0),
        )(x, dy, ridx.T, gates.T, w1, w3, w2)

        def perm(fy, fx):
            out = []
            for p in range(NP):
                yy, xx, cc = p // 4, (p // 2) % 2, p % 2
                out.append((p, (yy ^ fy) * 4 + (xx ^ fx) * 2 + cc))
            return out

        rd = lax.ppermute(sd, grp, perm(1, 1))
        rx = lax.ppermute(sx, grp, perm(0, 1))
        ry = lax.ppermute(sy, grp, perm(1, 0))
        y, dg, gw1, gw3, gw2 = pl.pallas_call(
            functools.partial(grad_kernel, el),
            in_specs=[pl.BlockSpec(memory_space=pltpu.HBM)] * 10,
            out_specs=[vm, vm, anyspec, anyspec, anyspec],
            out_shape=[sds((tok, d), BF16), sds((top, tok), F32), sds((el, d, ff), F32), sds((el, d, ff), F32), sds((el, ff, d), F32)],
            scratch_shapes=[
                pltpu.VMEM((NP, tok, d), BF16),
                pltpu.VMEM((NP, tok, d), BF16),
                pltpu.VMEM((NP, el, tok), F32),
                pltpu.VMEM((NP, el, tok), F32),
                pltpu.VMEM((2, GRP, NROW, d), BF16),
                pltpu.VMEM((2, GRP, NROW, d), BF16),
                pltpu.VMEM((2, GRP, NROW, ff), BF16),
                pltpu.VMEM((2, GRP, NROW, 2 * ff), BF16),
                pltpu.VMEM((NOUT, PAIR, d, ff), F32),
                pltpu.VMEM((NOUT, PAIR, d, ff), F32),
                pltpu.VMEM((NOUT, PAIR, ff, d), F32),
                dma((8,)), dma((2, 2)), dma((3, NOUT)),
            ],
            compiler_params=pltpu.CompilerParams(vmem_limit_bytes=56_000_000),
            cost_estimate=pl.CostEstimate(flops=40_000_000_000, bytes_accessed=160_000_000, transcendentals=0),
        )(y, dg, xa, dya, cm, gm, a, duv, xef, dof)
        dx = (ka + rx + ry + rd).astype(BF16)
        return y, dx, dg.T, gw1, gw3, gw2

    return jax.shard_map(local, mesh=mesh, in_specs=(tspec, tspec, tspec, wspec, wspec, wspec, tspec), out_specs=(tspec, tspec, tspec, gspec, gspec, gspec), check_vma=False)
```
